32 devices in a mesh: dp: 4 (over y, x), ctx: 2 (over core), tensor: 4 (over z).
Axes of the slice: x: 2, y: 2, z: 4, core: 2. Of those that a mesh axis runs over, the one named last changes fastest.
Arguments:
- tokens: bfloat16 [12, 2048, 768], P('dp', ('ctx', 'tensor')), may hold values from -6 to 6
- cotangent: bfloat16 [12, 2048, 768], P('dp', ('ctx', 'tensor')), may hold values from -6 to 6
- lengths: int32 [12], P('dp'), may hold values from 512 to 2048, as said below
- w_query: bfloat16 [768, 768], P(('dp', 'ctx'), 'tensor'), may hold values from -0.21875 to 0.21875
- w_key: bfloat16 [768, 768], P(('dp', 'ctx'), 'tensor'), may hold values from -0.21875 to 0.21875
- w_value: bfloat16 [768, 768], P(('dp', 'ctx'), 'tensor'), may hold values from -0.21875 to 0.21875
- w_output: bfloat16 [768, 768], P('tensor', ('dp', 'ctx')), may hold values from -3.5 to 3.5
- w_in: bfloat16 [768, 3072], P(('dp', 'ctx'), 'tensor'), may hold values from -0.21875 to 0.21875
- w_out: bfloat16 [3072, 768], P('tensor', ('dp', 'ctx')), may hold values from -0.109375 to 0.109375
- bias_query: bfloat16 [768], P(('dp', 'ctx')), may hold values from -3 to 3
- bias_value: bfloat16 [768], P(('dp', 'ctx')), may hold values from -0.1796875 to 0.1796875
- bias_output: bfloat16 [768], P(('dp', 'ctx')), may hold values from -3 to 3
- gain_first: bfloat16 [768], P(('dp', 'ctx')), may hold values from 0.5 to 1.5
- shift_first: bfloat16 [768], P(('dp', 'ctx')), may hold values from -3 to 3
- gain_second: bfloat16 [768], P(('dp', 'ctx')), may hold values from 0.5 to 1.5
- shift_second: bfloat16 [768], P(('dp', 'ctx')), may hold values from -3 to 3
- bias_out: bfloat16 [768], P(('dp', 'ctx')), may hold values from -3 to 3
- bias_in: bfloat16 [3072], P(('dp', 'ctx')), may hold values from -3 to 3
Outputs:
- output: bfloat16 [12, 2048, 768], P('dp', ('ctx', 'tensor'))
- grad_tokens: bfloat16 [12, 2048, 768], P('dp', ('ctx', 'tensor'))
- grad_w_query: float32 [768, 768], P(('dp', 'ctx'), 'tensor')
- grad_w_key: float32 [768, 768], P(('dp', 'ctx'), 'tensor')
- grad_w_value: float32 [768, 768], P(('dp', 'ctx'), 'tensor')
- grad_w_output: float32 [768, 768], P('tensor', ('dp', 'ctx'))
- grad_w_in: float32 [768, 3072], P(('dp', 'ctx'), 'tensor')
- grad_w_out: float32 [3072, 768], P('tensor', ('dp', 'ctx'))
- grad_bias_query: float32 [768], P(('dp', 'ctx'))
- grad_bias_value: float32 [768], P(('dp', 'ctx'))
- grad_bias_output: float32 [768], P(('dp', 'ctx'))
- grad_gain_first: float32 [768], P(('dp', 'ctx'))
- grad_shift_first: float32 [768], P(('dp', 'ctx'))
- grad_gain_second: float32 [768], P(('dp', 'ctx'))
- grad_shift_second: float32 [768], P(('dp', 'ctx'))
- grad_bias_out: float32 [768], P(('dp', 'ctx'))
- grad_bias_in: float32 [3072], P(('dp', 'ctx'))
The draws below stay inside these ranges and needn't reach their ends.
Inputs may be any that keep to these rules, and one draw needn't show every extreme that they name: Sequence s has valid tokens at positions below lengths[s] and padding after; in every draw some sequence has 2048 valid tokens and some has 512.
All inputs are finite; a program needn't handle non-finite values.
Results may differ from the reference program's by a relative error of at most 0.02.
Values may be sent and summed in bfloat16 or wider, within the bound.
A program may use at most 192 MiB of HBM per device.

```python
import jax
import jax.numpy as jnp
from jax import lax

D = 768
HD = 64
FF = 3072
SEQ = 2048
MIN_LEN = 512
SEQS = 12


def draw_lengths(key, part):
    key_lengths, key_first, key_step = jax.random.split(jax.random.fold_in(key, 17), 3)
    drawn = jax.random.randint(key_lengths, (SEQS,), MIN_LEN, SEQ + 1)
    first_index = jax.random.randint(key_first, (), 0, SEQS)
    offset = jax.random.randint(key_step, (), 1, SEQS)
    second_index = (first_index + offset) % SEQS
    places = jnp.arange(SEQS, dtype=jnp.int32)
    drawn = jnp.where(places == first_index, SEQ, jnp.where(places == second_index, MIN_LEN, drawn))
    return drawn.astype(jnp.int32)


def block_scale(stream_key, shape, cuts, low, top_value):
    def one(position, blocks):
        steps = jax.random.uniform(jax.random.fold_in(jax.random.fold_in(stream_key, 6), position), (blocks,), jnp.float32, low / len(cuts), top_value / len(cuts))
        return jnp.repeat(jnp.exp(steps), shape[position] // blocks).reshape((-1,) + (1,) * (len(shape) - position - 1))

    level = one(*cuts[0])
    for cut in cuts[1:]:
        level = level * one(*cut)
    return level


def normal_values(own_key, dims, scale, most, cuts=(), held_as=jnp.bfloat16):
    array = jax.random.normal(own_key, dims, jnp.float32) * scale
    if len(cuts) > 0:
        array = block_scale(own_key, dims, cuts, -0.22, 0.18) * array
    return jnp.clip(array, min=-most, max=most).astype(held_as)


def setup_inputs(seed: int = 0) -> dict:
    streams_of = jax.random.split(jax.random.key(seed), 19)
    tokens = normal_values(streams_of[0], (SEQS, SEQ, D), 1.0, 6.0, ((0, 4), (1, 8)))
    cotangent = normal_values(streams_of[1], (SEQS, SEQ, D), 1.0, 6.0, ((0, 4), (1, 8)))
    lengths = draw_lengths(jax.random.fold_in(streams_of[18], 71), 0)
    w_query = normal_values(streams_of[3], (D, D), D ** -0.5, 0.21875, ((0, 8), (1, 4)))
    w_key = normal_values(streams_of[4], (D, D), D ** -0.5, 0.21875, ((0, 8), (1, 4)))
    w_value = normal_values(streams_of[5], (D, D), D ** -0.5, 0.21875, ((0, 8), (1, 4)))
    w_output = normal_values(streams_of[6], (D, D), 3 ** -0.5, 3.5, ((0, 4), (1, 8)))
    w_in = normal_values(streams_of[7], (D, FF), D ** -0.5, 0.21875, ((0, 8), (1, 4)))
    w_out = normal_values(streams_of[8], (FF, D), FF ** -0.5, 0.109375, ((0, 4), (1, 8)))
    bias_query = normal_values(streams_of[9], (D,), 0.5, 3.0, ((0, 8),))
    bias_value = normal_values(streams_of[10], (D,), 0.03, 0.1796875, ((0, 8),))
    bias_output = normal_values(streams_of[11], (D,), 0.5, 3.0, ((0, 8),))
    gain_first = jnp.clip(1.0 + 0.1 * jax.random.normal(streams_of[12], (D,), jnp.float32), 0.5, 1.5).astype(jnp.bfloat16)
    shift_first = normal_values(streams_of[13], (D,), 0.5, 3.0, ((0, 8),))
    gain_second = jnp.clip(1.0 + 0.1 * jax.random.normal(streams_of[14], (D,), jnp.float32), 0.5, 1.5).astype(jnp.bfloat16)
    shift_second = normal_values(streams_of[15], (D,), 0.5, 3.0, ((0, 8),))
    bias_out = normal_values(streams_of[16], (D,), 0.5, 3.0, ((0, 8),))
    bias_in = normal_values(streams_of[17], (FF,), 0.5, 3.0, ((0, 8),))
    return dict(tokens=tokens, cotangent=cotangent, lengths=lengths, w_query=w_query, w_key=w_key, w_value=w_value, w_output=w_output, w_in=w_in, w_out=w_out, bias_query=bias_query, bias_value=bias_value, bias_output=bias_output, gain_first=gain_first, shift_first=shift_first, gain_second=gain_second, shift_second=shift_second, bias_out=bias_out, bias_in=bias_in)


@jax.custom_vjp
def low(v):
    return lax.optimization_barrier(v.astype(jnp.bfloat16)).astype(jnp.float32)

@jax.custom_vjp
def low_back(v):
    return v

def low_keep(v):
    return (low(v), None)

def low_pass(kept, grad):
    return (grad,)

def back_keep(v):
    return (v, None)

def back_low(kept, grad):
    return (low(grad),)
low.defvjp(low_keep, low_pass)
low_back.defvjp(back_keep, back_low)
epsilon = 1e-05
masked_value = -1e+30

def layer_norm(hidden, gain, shift):
    centre = hidden - lax.optimization_barrier(jnp.mean(hidden, axis=-1, keepdims=True))
    spread = lax.optimization_barrier(jnp.mean(centre * centre, axis=-1, keepdims=True))
    return centre * lax.rsqrt(spread + epsilon) * gain + shift

def matmul(left, right):
    return jnp.dot(left, right, precision=lax.Precision.HIGHEST, preferred_element_type=jnp.float32)

def one_sequence(inputs, params, key_valid):
    query_w, key_w, value_w, output_w, first_w, second_w, bias_query, bias_value, bias_output, gain_first, shift_first, gain_second, shift_second, bias_out, bias_in = params
    heads = D // HD
    scale = HD ** (-0.5)
    block_rows = min(512, SEQ)
    queries = low_back(low(matmul(inputs, query_w) + bias_query))
    keys_heads = low_back(low(matmul(inputs, key_w))).reshape(SEQ, heads, HD)
    values_heads = low_back(low(matmul(inputs, value_w) + bias_value)).reshape(SEQ, heads, HD)
    query_blocks = queries.reshape(SEQ // block_rows, block_rows, heads, HD)

    def attend(query_block):
        raw = jnp.einsum('qhd,khd->hqk', query_block, keys_heads, precision=lax.Precision.HIGHEST) * scale
        scores = jnp.where(key_valid, low_back(raw), masked_value)
        top = lax.optimization_barrier(jnp.max(scores, axis=-1, keepdims=True))
        weights = jnp.exp(scores - top)
        probs = weights / lax.optimization_barrier(jnp.sum(weights, axis=-1, keepdims=True))
        return jnp.einsum('hqk,khd->qhd', low(probs), values_heads, precision=lax.Precision.HIGHEST)
    mixed = lax.map(jax.checkpoint(attend), query_blocks).reshape(SEQ, D)
    attended = low_back(low(mixed))
    branch = low_back(matmul(attended, output_w)) + bias_output
    first = layer_norm(inputs + branch, gain_first, shift_first)
    hidden_pre = low_back(matmul(low(first), first_w) + bias_in)
    activated = low(jax.nn.gelu(hidden_pre, approximate=False))
    second = first + low_back(matmul(activated, second_w)) + bias_out
    return layer_norm(second, gain_second, shift_second)

def reference(tokens, cotangent, lengths, w_query, w_key, w_value, w_output, w_in, w_out, bias_query, bias_value, bias_output, gain_first, shift_first, gain_second, shift_second, bias_out, bias_in):
    params = tuple((value.astype(jnp.float32) for value in (w_query, w_key, w_value, w_output, w_in, w_out, bias_query, bias_value, bias_output, gain_first, shift_first, gain_second, shift_second, bias_out, bias_in)))
    positions = jnp.arange(SEQ, dtype=jnp.int32)

    def step(totals, item):
        seq_tokens, seq_cot, length = item
        key_valid = positions < length.astype(jnp.int32)
        upstream = seq_cot.astype(jnp.float32) * key_valid.astype(jnp.float32)[:, None]

        def forward(inputs_now, params_now):
            return one_sequence(inputs_now, params_now, key_valid)
        result, pullback = jax.vjp(forward, seq_tokens.astype(jnp.float32), params)
        d_inputs, d_params = pullback(upstream)
        totals = jax.tree.map(jnp.add, totals, d_params)
        return (totals, (result.astype(jnp.bfloat16), d_inputs.astype(jnp.bfloat16)))
    zeros = tuple((jnp.zeros_like(value) for value in params))
    totals, (outputs, grads_in) = lax.scan(step, zeros, (tokens, cotangent, lengths))
    return (outputs, grads_in, totals[0], totals[1], totals[2], totals[3], totals[4], totals[5], totals[6], totals[7], totals[8], totals[9], totals[10], totals[11], totals[12], totals[13], totals[14])
```

```python
import jax
import jax.numpy as jnp
from jax import lax
from jax.sharding import PartitionSpec as P

HD = 64
epsilon = 1e-05
masked_value = -1e30
ALL = ("dp", "ctx", "tensor")
SEQ_AXES = ("ctx", "tensor")


def exact_gelu(value):
    return jax.nn.gelu(value, approximate=False)


def mm(left, right):
    return jnp.dot(left, right, preferred_element_type=jnp.float32)


def mm_tn(left, right):
    return lax.dot_general(left, right, (((0,), (0,)), ((), ())), preferred_element_type=jnp.float32)


def mm_nt(left, right):
    return lax.dot_general(left, right, (((1,), (1,)), ((), ())), preferred_element_type=jnp.float32)


def ln_forward(hidden, gain, shift):
    mean = jnp.mean(hidden, axis=-1, keepdims=True)
    centre = hidden - mean
    var = jnp.mean(centre * centre, axis=-1, keepdims=True)
    inv = lax.rsqrt(var + epsilon)
    normed = centre * inv
    return normed * gain + shift, normed, inv


def ln_backward(grad_out, normed, inv, gain):
    d_normed = grad_out * gain
    width = normed.shape[-1]
    mean_d = jnp.sum(d_normed, axis=-1, keepdims=True) / width
    mean_dn = jnp.sum(d_normed * normed, axis=-1, keepdims=True) / width
    d_in = inv * (d_normed - mean_d - normed * mean_dn)
    d_gain = jnp.sum(grad_out * normed, axis=0)
    d_shift = jnp.sum(grad_out, axis=0)
    return d_in, d_gain, d_shift


def row_col_unpack(flat, rows, cols, row_major_blocks, nt):
    nb_outer = flat.shape[0] // nt
    blocks = flat.reshape(nb_outer, nt, rows, cols)
    if row_major_blocks:
        return blocks.transpose(0, 2, 1, 3).reshape(nb_outer * rows, nt * cols)
    return blocks.transpose(1, 2, 0, 3).reshape(nt * rows, nb_outer * cols)


def row_col_pack(full, rows, cols, row_major_blocks, nt):
    if row_major_blocks:
        nb_outer = full.shape[0] // rows
        blocks = full.reshape(nb_outer, rows, nt, cols).transpose(0, 2, 1, 3)
    else:
        nb_outer = full.shape[1] // cols
        blocks = full.reshape(nt, rows, nb_outer, cols).transpose(2, 0, 1, 3)
    return blocks.reshape(nb_outer * nt, rows * cols)


def vec_unpack(flat, length, nt):
    nb_outer = flat.shape[0] // nt
    blocks = flat.reshape(nb_outer, nt, -1, length)[:, 0]
    return blocks.transpose(1, 0, 2).reshape(blocks.shape[1], nb_outer * length)


def vec_pack(full, length, nt):
    n = full.shape[0]
    nb_outer = full.shape[1] // length
    blocks = full.reshape(n, nb_outer, length).transpose(1, 0, 2).reshape(nb_outer, 1, n * length)
    return jnp.broadcast_to(blocks, (nb_outer, nt, n * length)).reshape(nb_outer * nt, n * length)


def reduce_packed(pack):
    devices, chunk_len = pack.shape
    padded = -(-chunk_len // 2048) * 2048
    pack = jnp.pad(pack, ((0, 0), (0, padded - chunk_len))).reshape(-1, 128)
    stage = lax.psum_scatter(pack, ("dp", "ctx"), scatter_dimension=0, tiled=True)
    own = lax.psum_scatter(stage, "tensor", scatter_dimension=0, tiled=True)
    return own.reshape(-1)[:chunk_len].astype(jnp.float32)


def body(
    tokens,
    cotangent,
    lengths,
    w_query,
    w_key,
    w_value,
    w_output,
    w_in,
    w_out,
    bias_query,
    bias_value,
    bias_output,
    gain_first,
    shift_first,
    gain_second,
    shift_second,
    bias_out,
    bias_in,
):
    seqs, local_rows, width = tokens.shape
    ctx_rank = lax.axis_index("ctx")
    tensor_rank = lax.axis_index("tensor")
    nt = lax.axis_size("tensor")
    chunk = ctx_rank * nt + tensor_rank
    seq_len = local_rows * lax.axis_size("ctx") * lax.axis_size("tensor")
    heads = width // HD
    scale = HD ** (-0.5)

    qr, qc = w_query.shape
    orr, oc = w_output.shape
    ir, ic = w_in.shape
    outr, outc = w_out.shape
    vlen = bias_query.shape[0]
    hlen = bias_in.shape[0]

    vectors = jnp.stack(
        [bias_query, bias_value, bias_output, gain_first, shift_first, gain_second, shift_second, bias_out]
    )
    attn_pack = jnp.concatenate(
        [w_query.reshape(-1), w_key.reshape(-1), w_value.reshape(-1), w_output.reshape(-1), vectors.reshape(-1)]
    )
    ffn_pack = jnp.concatenate([w_in.reshape(-1), w_out.reshape(-1), bias_in.reshape(-1)])
    attn_all = lax.all_gather(attn_pack, ALL, axis=0, tiled=False)
    ffn_all = lax.all_gather(ffn_pack, ALL, axis=0, tiled=False)

    sq = qr * qc
    so = orr * oc
    wq = row_col_unpack(attn_all[:, 0:sq], qr, qc, True, nt)
    wk = row_col_unpack(attn_all[:, sq : 2 * sq], qr, qc, True, nt)
    wv = row_col_unpack(attn_all[:, 2 * sq : 3 * sq], qr, qc, True, nt)
    wo = row_col_unpack(attn_all[:, 3 * sq : 3 * sq + so], orr, oc, False, nt)
    vec_full = vec_unpack(attn_all[:, 3 * sq + so :], vlen, nt).astype(jnp.float32)
    b_q, b_v, b_o, g1, s1, g2, s2, b_out = [vec_full[i] for i in range(8)]
    wkv = jnp.concatenate([wk, wv], axis=1)

    si = ir * ic
    sout = outr * outc
    w_in_f = row_col_unpack(ffn_all[:, 0:si], ir, ic, True, nt)
    w_out_f = row_col_unpack(ffn_all[:, si : si + sout], outr, outc, False, nt)
    b_in = vec_unpack(ffn_all[:, si + sout :], hlen, nt)[0].astype(jnp.float32)

    positions = jnp.arange(seq_len, dtype=jnp.int32)
    row_positions = chunk * local_rows + jnp.arange(local_rows, dtype=jnp.int32)

    fwd = []
    for s in range(seqs):
        x_own = tokens[s]
        length = lengths[s]
        x_all = lax.all_gather(x_own, SEQ_AXES, axis=0, tiled=True)
        q = (mm(x_own, wq) + b_q).astype(jnp.bfloat16)
        kv = mm(x_all, wkv)
        k = kv[:, :width].astype(jnp.bfloat16)
        v = (kv[:, width:] + b_v).astype(jnp.bfloat16)
        key_valid = positions < length
        qh = q.reshape(local_rows, heads, HD)
        kh = k.reshape(seq_len, heads, HD)
        vh = v.reshape(seq_len, heads, HD)
        raw = jnp.einsum("qhd,khd->hqk", qh, kh, preferred_element_type=jnp.float32) * scale
        scores = jnp.where(key_valid, raw, masked_value)
        top = jnp.max(scores, axis=-1, keepdims=True)
        weights = jnp.exp(scores - top)
        total = jnp.sum(weights, axis=-1, keepdims=True)
        probs = (weights / total).astype(jnp.bfloat16)
        mixed = jnp.einsum("hqk,khd->qhd", probs, vh, preferred_element_type=jnp.float32)
        attended = mixed.reshape(local_rows, width).astype(jnp.bfloat16)
        lse = top + jnp.log(total)
        first_in = x_own.astype(jnp.float32) + (mm(attended, wo) + b_o)
        first, normed1, inv1 = ln_forward(first_in, g1, s1)
        fwd.append(dict(x_all=x_all, q=q, k=k, v=v, lse=lse, attended=attended, first=first,
                        normed1=normed1, inv1=inv1, key_valid=key_valid, length=length))

    outputs = []
    for s in range(seqs):
        f = fwd[s]
        first_low = f["first"].astype(jnp.bfloat16)
        hidden_pre = mm(first_low, w_in_f) + b_in
        activated = exact_gelu(hidden_pre).astype(jnp.bfloat16)
        second_in = f["first"] + mm(activated, w_out_f) + b_out
        result, normed2, inv2 = ln_forward(second_in, g2, s2)
        outputs.append(result.astype(jnp.bfloat16))
        f.update(first_low=first_low, hidden_pre=hidden_pre, activated=activated, normed2=normed2, inv2=inv2)

    g_w_in = jnp.zeros((width, w_in_f.shape[1]), jnp.float32)
    g_w_out = jnp.zeros((w_out_f.shape[0], width), jnp.float32)
    g_b_in = jnp.zeros((w_in_f.shape[1],), jnp.float32)
    g_vec = [jnp.zeros((width,), jnp.float32) for _ in range(8)]
    for s in range(seqs):
        f = fwd[s]
        row_valid = (row_positions < f["length"]).astype(jnp.float32)
        upstream = cotangent[s].astype(jnp.float32) * row_valid[:, None]
        d_second, d_g2, d_s2 = ln_backward(upstream, f["normed2"], f["inv2"], g2)
        d_ffn = d_second.astype(jnp.bfloat16)
        g_w_out = g_w_out + mm_tn(f["activated"], d_ffn)
        d_act = mm_nt(d_ffn, w_out_f)
        _, gelu_pull = jax.vjp(exact_gelu, f["hidden_pre"])
        d_hidden = gelu_pull(d_act)[0].astype(jnp.bfloat16)
        g_w_in = g_w_in + mm_tn(f["first_low"], d_hidden)
        g_b_in = g_b_in + jnp.sum(d_hidden.astype(jnp.float32), axis=0)
        d_first = d_second + mm_nt(d_hidden, w_in_f)
        d_first_in, d_g1, d_s1 = ln_backward(d_first, f["normed1"], f["inv1"], g1)
        g_vec[5] = g_vec[5] + d_g2
        g_vec[6] = g_vec[6] + d_s2
        g_vec[7] = g_vec[7] + jnp.sum(d_second, axis=0)
        g_vec[3] = g_vec[3] + d_g1
        g_vec[4] = g_vec[4] + d_s1
        g_vec[2] = g_vec[2] + jnp.sum(d_first_in, axis=0)
        f.update(d_first_in=d_first_in)

    ffn_grad_pack = jnp.concatenate(
        [
            row_col_pack(g_w_in, ir, ic, True, nt),
            row_col_pack(g_w_out, outr, outc, False, nt),
            vec_pack(g_b_in[None, :], hlen, nt),
        ],
        axis=1,
    ).astype(jnp.bfloat16)
    ffn_grad = reduce_packed(ffn_grad_pack)

    g_wq = jnp.zeros((width, width), jnp.float32)
    g_wkv = jnp.zeros((width, 2 * width), jnp.float32)
    g_wo = jnp.zeros((width, width), jnp.float32)
    grad_tokens = []
    for s in range(seqs):
        f = fwd[s]
        d_branch = f["d_first_in"].astype(jnp.bfloat16)
        g_wo = g_wo + mm_tn(f["attended"], d_branch)
        d_att = mm_nt(d_branch, wo).astype(jnp.bfloat16)
        qh = f["q"].reshape(local_rows, heads, HD)
        kh = f["k"].reshape(seq_len, heads, HD)
        vh = f["v"].reshape(seq_len, heads, HD)
        dah = d_att.reshape(local_rows, heads, HD)
        raw = jnp.einsum("qhd,khd->hqk", qh, kh, preferred_element_type=jnp.float32) * scale
        scores = jnp.where(f["key_valid"], raw, masked_value)
        probs = jnp.exp(scores - f["lse"])
        d_probs = jnp.einsum("qhd,khd->hqk", dah, vh, preferred_element_type=jnp.float32)
        centre = jnp.sum(probs * d_probs, axis=-1, keepdims=True)
        d_scores = jnp.where(f["key_valid"], probs * (d_probs - centre), 0.0).astype(jnp.bfloat16)
        dq = (jnp.einsum("hqk,khd->qhd", d_scores, kh, preferred_element_type=jnp.float32) * scale).astype(
            jnp.bfloat16
        )
        dk_part = jnp.einsum("hqk,qhd->khd", d_scores, qh, preferred_element_type=jnp.float32) * scale
        dv_part = jnp.einsum("hqk,qhd->khd", probs.astype(jnp.bfloat16), dah, preferred_element_type=jnp.float32)
        dq = dq.reshape(local_rows, width)
        dkv = jnp.concatenate(
            [dk_part.reshape(seq_len, width), dv_part.reshape(seq_len, width)], axis=1
        ).astype(jnp.bfloat16)
        g_wq = g_wq + mm_tn(tokens[s], dq)
        g_wkv = g_wkv + mm_tn(f["x_all"], dkv)
        g_vec[0] = g_vec[0] + jnp.sum(dq.astype(jnp.float32), axis=0)
        g_vec[1] = g_vec[1] + jnp.sum(dkv[:, width:].astype(jnp.float32), axis=0)
        dx_kv = mm_nt(dkv, wkv).astype(jnp.bfloat16)
        dx_kv_own = lax.psum_scatter(dx_kv, SEQ_AXES, scatter_dimension=0, tiled=True).astype(jnp.float32)
        d_tok = f["d_first_in"] + mm_nt(dq, wq) + dx_kv_own
        grad_tokens.append(d_tok.astype(jnp.bfloat16))

    attn_grad_pack = jnp.concatenate(
        [
            row_col_pack(g_wq, qr, qc, True, nt),
            row_col_pack(g_wkv[:, :width], qr, qc, True, nt),
            row_col_pack(g_wkv[:, width:], qr, qc, True, nt),
            row_col_pack(g_wo, orr, oc, False, nt),
            vec_pack(jnp.stack(g_vec), vlen, nt),
        ],
        axis=1,
    ).astype(jnp.bfloat16)
    attn_grad = reduce_packed(attn_grad_pack)

    grad_wq = attn_grad[0:sq].reshape(qr, qc)
    grad_wk = attn_grad[sq : 2 * sq].reshape(qr, qc)
    grad_wv = attn_grad[2 * sq : 3 * sq].reshape(qr, qc)
    grad_wo = attn_grad[3 * sq : 3 * sq + so].reshape(orr, oc)
    grad_vec = attn_grad[3 * sq + so :].reshape(8, vlen)
    grad_w_in = ffn_grad[0:si].reshape(ir, ic)
    grad_w_out = ffn_grad[si : si + sout].reshape(outr, outc)
    grad_b_in = ffn_grad[si + sout :]

    return (
        jnp.stack(outputs),
        jnp.stack(grad_tokens),
        grad_wq,
        grad_wk,
        grad_wv,
        grad_wo,
        grad_w_in,
        grad_w_out,
        grad_vec[0],
        grad_vec[1],
        grad_vec[2],
        grad_vec[3],
        grad_vec[4],
        grad_vec[5],
        grad_vec[6],
        grad_vec[7],
        grad_b_in,
    )


def solution(mesh):
    row_spec = P("dp", ("ctx", "tensor"), None)
    w_rc = P(("dp", "ctx"), "tensor")
    w_cr = P("tensor", ("dp", "ctx"))
    vec = P(("dp", "ctx"))
    return jax.shard_map(
        body,
        mesh=mesh,
        in_specs=(row_spec, row_spec, P("dp"), w_rc, w_rc, w_rc, w_cr, w_rc, w_cr) + (vec,) * 9,
        out_specs=(row_spec, row_spec, w_rc, w_rc, w_rc, w_cr, w_rc, w_cr) + (vec,) * 9,
        check_vma=False,
    )
```

```python
import functools

import jax
import jax.numpy as jnp
from jax import lax
from jax.experimental import pallas as pl
from jax.experimental.pallas import tpu as pltpu
from jax.sharding import PartitionSpec as P

HD = 64
epsilon = 1e-05
masked_value = -1e30
ALL = ("dp", "ctx", "tensor")
SEQ_AXES = ("ctx", "tensor")


def exact_gelu(value):
    return jax.nn.gelu(value, approximate=False)


def mm(left, right):
    return jnp.dot(left, right, preferred_element_type=jnp.float32)


def mm_tn(left, right):
    return lax.dot_general(left, right, (((0,), (0,)), ((), ())), preferred_element_type=jnp.float32)


def mm_nt(left, right):
    return lax.dot_general(left, right, (((1,), (1,)), ((), ())), preferred_element_type=jnp.float32)


def ln_forward(hidden, gain, shift):
    mean = jnp.mean(hidden, axis=-1, keepdims=True)
    centre = hidden - mean
    var = jnp.mean(centre * centre, axis=-1, keepdims=True)
    inv = lax.rsqrt(var + epsilon)
    normed = centre * inv
    return normed * gain + shift, normed, inv


def ln_backward(grad_out, normed, inv, gain):
    d_normed = grad_out * gain
    width = normed.shape[-1]
    mean_d = jnp.sum(d_normed, axis=-1, keepdims=True) / width
    mean_dn = jnp.sum(d_normed * normed, axis=-1, keepdims=True) / width
    d_in = inv * (d_normed - mean_d - normed * mean_dn)
    d_gain = jnp.sum(grad_out * normed, axis=0)
    d_shift = jnp.sum(grad_out, axis=0)
    return d_in, d_gain, d_shift


KEY_BLOCK = 512


def _attn_fwd_kernel(len_ref, q_ref, k_ref, v_ref, o_ref, lse_ref, s_buf, *, scale, seq_len):
    length = len_ref[0]
    n_blocks = (length + KEY_BLOCK - 1) // KEY_BLOCK
    q = q_ref[0]
    rows = q.shape[0]

    def scores_of(b):
        start = pl.multiple_of(b * KEY_BLOCK, KEY_BLOCK)
        k_blk = k_ref[0, pl.ds(start, KEY_BLOCK), :]
        s = lax.dot_general(q, k_blk, (((1,), (1,)), ((), ())), preferred_element_type=jnp.float32) * scale
        pos = start + lax.broadcasted_iota(jnp.int32, s.shape, 1)
        return start, jnp.where(pos < length, s, masked_value)

    def pass_max(b, m):
        start, s = scores_of(b)
        s_buf[:, pl.ds(start, KEY_BLOCK)] = s
        return jnp.maximum(m, jnp.max(s, axis=1, keepdims=True))

    m = lax.fori_loop(0, n_blocks, pass_max, jnp.full((rows, 1), -jnp.inf, jnp.float32))

    def pass_sum(b, l):
        start = pl.multiple_of(b * KEY_BLOCK, KEY_BLOCK)
        e = jnp.exp(s_buf[:, pl.ds(start, KEY_BLOCK)] - m)
        s_buf[:, pl.ds(start, KEY_BLOCK)] = e
        return l + jnp.sum(e, axis=1, keepdims=True)

    l = lax.fori_loop(0, n_blocks, pass_sum, jnp.zeros((rows, 1), jnp.float32))

    def pass_out(b, acc):
        start = pl.multiple_of(b * KEY_BLOCK, KEY_BLOCK)
        probs = (s_buf[:, pl.ds(start, KEY_BLOCK)] / l).astype(jnp.bfloat16)
        v_blk = v_ref[0, pl.ds(start, KEY_BLOCK), :]
        return acc + jnp.dot(probs, v_blk, preferred_element_type=jnp.float32)

    acc = lax.fori_loop(0, n_blocks, pass_out, jnp.zeros((rows, q.shape[1]), jnp.float32))
    o_ref[0] = acc.astype(o_ref.dtype)
    lse_ref[0] = m + jnp.log(l)


def attention_fwd(length, qh, kh, vh, scale):
    heads, rows, hd = qh.shape
    seq_len = kh.shape[1]
    kernel = functools.partial(_attn_fwd_kernel, scale=scale, seq_len=seq_len)
    flops = 4 * heads * rows * seq_len * hd
    return pl.pallas_call(
        kernel,
        out_shape=(
            jax.ShapeDtypeStruct((heads, rows, hd), jnp.bfloat16),
            jax.ShapeDtypeStruct((heads, rows, 1), jnp.float32),
        ),
        grid_spec=pltpu.PrefetchScalarGridSpec(
            num_scalar_prefetch=1,
            grid=(heads,),
            in_specs=[
                pl.BlockSpec((1, rows, hd), lambda h, n: (h, 0, 0)),
                pl.BlockSpec((1, seq_len, hd), lambda h, n: (h, 0, 0)),
                pl.BlockSpec((1, seq_len, hd), lambda h, n: (h, 0, 0)),
            ],
            out_specs=[
                pl.BlockSpec((1, rows, hd), lambda h, n: (h, 0, 0)),
                pl.BlockSpec((1, rows, 1), lambda h, n: (h, 0, 0)),
            ],
            scratch_shapes=[pltpu.VMEM((rows, seq_len), jnp.float32)],
        ),
        cost_estimate=pl.CostEstimate(
            flops=flops, transcendentals=heads * rows * seq_len,
            bytes_accessed=2 * (qh.size + kh.size + vh.size + qh.size) + 4 * heads * rows,
        ),
    )(length.reshape(1), qh, kh, vh)


def _attn_bwd_kernel(len_ref, q_ref, k_ref, v_ref, do_ref, lse_ref, dq_ref, dk_ref, dv_ref, p_buf, dp_buf, *, scale):
    length = len_ref[0]
    n_blocks = (length + KEY_BLOCK - 1) // KEY_BLOCK
    total_blocks = k_ref.shape[1] // KEY_BLOCK
    q = q_ref[0]
    do = do_ref[0]
    lse = lse_ref[0]
    rows = q.shape[0]

    def pass_one(b, centre):
        start = pl.multiple_of(b * KEY_BLOCK, KEY_BLOCK)
        k_blk = k_ref[0, pl.ds(start, KEY_BLOCK), :]
        v_blk = v_ref[0, pl.ds(start, KEY_BLOCK), :]
        s = lax.dot_general(q, k_blk, (((1,), (1,)), ((), ())), preferred_element_type=jnp.float32) * scale
        pos = start + lax.broadcasted_iota(jnp.int32, s.shape, 1)
        s = jnp.where(pos < length, s, masked_value)
        p = jnp.exp(s - lse)
        dp = lax.dot_general(do, v_blk, (((1,), (1,)), ((), ())), preferred_element_type=jnp.float32)
        p_buf[:, pl.ds(start, KEY_BLOCK)] = p
        dp_buf[:, pl.ds(start, KEY_BLOCK)] = dp
        return centre + jnp.sum(p * dp, axis=1, keepdims=True)

    centre = lax.fori_loop(0, n_blocks, pass_one, jnp.zeros((rows, 1), jnp.float32))

    def pass_two(b, dq):
        start = pl.multiple_of(b * KEY_BLOCK, KEY_BLOCK)
        k_blk = k_ref[0, pl.ds(start, KEY_BLOCK), :]
        p = p_buf[:, pl.ds(start, KEY_BLOCK)]
        dp = dp_buf[:, pl.ds(start, KEY_BLOCK)]
        pos = start + lax.broadcasted_iota(jnp.int32, p.shape, 1)
        ds = jnp.where(pos < length, p * (dp - centre), 0.0).astype(jnp.bfloat16)
        dk_ref[0, pl.ds(start, KEY_BLOCK), :] = (
            lax.dot_general(ds, q, (((0,), (0,)), ((), ())), preferred_element_type=jnp.float32) * scale
        )
        dv_ref[0, pl.ds(start, KEY_BLOCK), :] = lax.dot_general(
            p.astype(jnp.bfloat16), do, (((0,), (0,)), ((), ())), preferred_element_type=jnp.float32
        )
        return dq + jnp.dot(ds, k_blk, preferred_element_type=jnp.float32)

    dq = lax.fori_loop(0, n_blocks, pass_two, jnp.zeros((rows, q.shape[1]), jnp.float32))
    dq_ref[0] = (dq * scale).astype(dq_ref.dtype)

    def pass_zero(b, carry):
        start = pl.multiple_of(b * KEY_BLOCK, KEY_BLOCK)
        dk_ref[0, pl.ds(start, KEY_BLOCK), :] = jnp.zeros((KEY_BLOCK, q.shape[1]), jnp.float32)
        dv_ref[0, pl.ds(start, KEY_BLOCK), :] = jnp.zeros((KEY_BLOCK, q.shape[1]), jnp.float32)
        return carry

    lax.fori_loop(n_blocks, total_blocks, pass_zero, 0)


def attention_bwd(length, qh, kh, vh, doh, lse, scale):
    heads, rows, hd = qh.shape
    seq_len = kh.shape[1]
    kernel = functools.partial(_attn_bwd_kernel, scale=scale)
    flops = 8 * heads * rows * seq_len * hd
    return pl.pallas_call(
        kernel,
        out_shape=(
            jax.ShapeDtypeStruct((heads, rows, hd), jnp.bfloat16),
            jax.ShapeDtypeStruct((heads, seq_len, hd), jnp.float32),
            jax.ShapeDtypeStruct((heads, seq_len, hd), jnp.float32),
        ),
        grid_spec=pltpu.PrefetchScalarGridSpec(
            num_scalar_prefetch=1,
            grid=(heads,),
            in_specs=[
                pl.BlockSpec((1, rows, hd), lambda h, n: (h, 0, 0)),
                pl.BlockSpec((1, seq_len, hd), lambda h, n: (h, 0, 0)),
                pl.BlockSpec((1, seq_len, hd), lambda h, n: (h, 0, 0)),
                pl.BlockSpec((1, rows, hd), lambda h, n: (h, 0, 0)),
                pl.BlockSpec((1, rows, 1), lambda h, n: (h, 0, 0)),
            ],
            out_specs=[
                pl.BlockSpec((1, rows, hd), lambda h, n: (h, 0, 0)),
                pl.BlockSpec((1, seq_len, hd), lambda h, n: (h, 0, 0)),
                pl.BlockSpec((1, seq_len, hd), lambda h, n: (h, 0, 0)),
            ],
            scratch_shapes=[pltpu.VMEM((rows, seq_len), jnp.float32), pltpu.VMEM((rows, seq_len), jnp.float32)],
        ),
        cost_estimate=pl.CostEstimate(
            flops=flops, transcendentals=heads * rows * seq_len,
            bytes_accessed=2 * (3 * qh.size + 2 * kh.size) + 8 * kh.size,
        ),
    )(length.reshape(1), qh, kh, vh, doh, lse)


def row_col_unpack(flat, rows, cols, row_major_blocks, nt):
    nb_outer = flat.shape[0] // nt
    blocks = flat.reshape(nb_outer, nt, rows, cols)
    if row_major_blocks:
        return blocks.transpose(0, 2, 1, 3).reshape(nb_outer * rows, nt * cols)
    return blocks.transpose(1, 2, 0, 3).reshape(nt * rows, nb_outer * cols)


def row_col_pack(full, rows, cols, row_major_blocks, nt):
    if row_major_blocks:
        nb_outer = full.shape[0] // rows
        blocks = full.reshape(nb_outer, rows, nt, cols).transpose(0, 2, 1, 3)
    else:
        nb_outer = full.shape[1] // cols
        blocks = full.reshape(nt, rows, nb_outer, cols).transpose(2, 0, 1, 3)
    return blocks.reshape(nb_outer * nt, rows * cols)


def vec_unpack(flat, length, nt):
    nb_outer = flat.shape[0] // nt
    blocks = flat.reshape(nb_outer, nt, -1, length)[:, 0]
    return blocks.transpose(1, 0, 2).reshape(blocks.shape[1], nb_outer * length)


def vec_pack(full, length, nt):
    n = full.shape[0]
    nb_outer = full.shape[1] // length
    blocks = full.reshape(n, nb_outer, length).transpose(1, 0, 2).reshape(nb_outer, 1, n * length)
    return jnp.broadcast_to(blocks, (nb_outer, nt, n * length)).reshape(nb_outer * nt, n * length)


def reduce_packed(pack):
    devices, chunk_len = pack.shape
    padded = -(-chunk_len // 2048) * 2048
    pack = jnp.pad(pack, ((0, 0), (0, padded - chunk_len))).reshape(-1, 128)
    stage = lax.psum_scatter(pack, ("dp", "ctx"), scatter_dimension=0, tiled=True)
    own = lax.psum_scatter(stage, "tensor", scatter_dimension=0, tiled=True)
    return own.reshape(-1)[:chunk_len].astype(jnp.float32)


def body(
    tokens,
    cotangent,
    lengths,
    w_query,
    w_key,
    w_value,
    w_output,
    w_in,
    w_out,
    bias_query,
    bias_value,
    bias_output,
    gain_first,
    shift_first,
    gain_second,
    shift_second,
    bias_out,
    bias_in,
):
    seqs, local_rows, width = tokens.shape
    ctx_rank = lax.axis_index("ctx")
    tensor_rank = lax.axis_index("tensor")
    nt = lax.axis_size("tensor")
    chunk = ctx_rank * nt + tensor_rank
    seq_len = local_rows * lax.axis_size("ctx") * lax.axis_size("tensor")
    heads = width // HD
    scale = HD ** (-0.5)

    qr, qc = w_query.shape
    orr, oc = w_output.shape
    ir, ic = w_in.shape
    outr, outc = w_out.shape
    vlen = bias_query.shape[0]
    hlen = bias_in.shape[0]

    vectors = jnp.stack(
        [bias_query, bias_value, bias_output, gain_first, shift_first, gain_second, shift_second, bias_out]
    )
    attn_pack = jnp.concatenate(
        [w_query.reshape(-1), w_key.reshape(-1), w_value.reshape(-1), w_output.reshape(-1), vectors.reshape(-1)]
    )
    ffn_pack = jnp.concatenate([w_in.reshape(-1), w_out.reshape(-1), bias_in.reshape(-1)])
    attn_all = lax.all_gather(attn_pack, ALL, axis=0, tiled=False)
    ffn_all = lax.all_gather(ffn_pack, ALL, axis=0, tiled=False)

    sq = qr * qc
    so = orr * oc
    wq = row_col_unpack(attn_all[:, 0:sq], qr, qc, True, nt)
    wk = row_col_unpack(attn_all[:, sq : 2 * sq], qr, qc, True, nt)
    wv = row_col_unpack(attn_all[:, 2 * sq : 3 * sq], qr, qc, True, nt)
    wo = row_col_unpack(attn_all[:, 3 * sq : 3 * sq + so], orr, oc, False, nt)
    vec_full = vec_unpack(attn_all[:, 3 * sq + so :], vlen, nt).astype(jnp.float32)
    b_q, b_v, b_o, g1, s1, g2, s2, b_out = [vec_full[i] for i in range(8)]
    wkv = jnp.concatenate([wk, wv], axis=1)

    si = ir * ic
    sout = outr * outc
    w_in_f = row_col_unpack(ffn_all[:, 0:si], ir, ic, True, nt)
    w_out_f = row_col_unpack(ffn_all[:, si : si + sout], outr, outc, False, nt)
    b_in = vec_unpack(ffn_all[:, si + sout :], hlen, nt)[0].astype(jnp.float32)

    positions = jnp.arange(seq_len, dtype=jnp.int32)
    row_positions = chunk * local_rows + jnp.arange(local_rows, dtype=jnp.int32)

    fwd = []
    for s in range(seqs):
        x_own = tokens[s]
        length = lengths[s]
        x_all = lax.all_gather(x_own, SEQ_AXES, axis=0, tiled=True)
        q = (mm(x_own, wq) + b_q).astype(jnp.bfloat16)
        kv = mm(x_all, wkv)
        k = kv[:, :width].astype(jnp.bfloat16)
        v = (kv[:, width:] + b_v).astype(jnp.bfloat16)
        qh = q.reshape(local_rows, heads, HD).transpose(1, 0, 2)
        kh = k.reshape(seq_len, heads, HD).transpose(1, 0, 2)
        vh = v.reshape(seq_len, heads, HD).transpose(1, 0, 2)
        oh, lse = attention_fwd(length, qh, kh, vh, scale)
        attended = oh.transpose(1, 0, 2).reshape(local_rows, width)
        first_in = x_own.astype(jnp.float32) + (mm(attended, wo) + b_o)
        first, normed1, inv1 = ln_forward(first_in, g1, s1)
        fwd.append(dict(x_all=x_all, qh=qh, kh=kh, vh=vh, lse=lse, attended=attended, first=first,
                        normed1=normed1, inv1=inv1, length=length))

    outputs = []
    for s in range(seqs):
        f = fwd[s]
        first_low = f["first"].astype(jnp.bfloat16)
        hidden_pre = mm(first_low, w_in_f) + b_in
        activated = exact_gelu(hidden_pre).astype(jnp.bfloat16)
        second_in = f["first"] + mm(activated, w_out_f) + b_out
        result, normed2, inv2 = ln_forward(second_in, g2, s2)
        outputs.append(result.astype(jnp.bfloat16))
        f.update(first_low=first_low, hidden_pre=hidden_pre, activated=activated, normed2=normed2, inv2=inv2)

    g_w_in = jnp.zeros((width, w_in_f.shape[1]), jnp.float32)
    g_w_out = jnp.zeros((w_out_f.shape[0], width), jnp.float32)
    g_b_in = jnp.zeros((w_in_f.shape[1],), jnp.float32)
    g_vec = [jnp.zeros((width,), jnp.float32) for _ in range(8)]
    for s in range(seqs):
        f = fwd[s]
        row_valid = (row_positions < f["length"]).astype(jnp.float32)
        upstream = cotangent[s].astype(jnp.float32) * row_valid[:, None]
        d_second, d_g2, d_s2 = ln_backward(upstream, f["normed2"], f["inv2"], g2)
        d_ffn = d_second.astype(jnp.bfloat16)
        g_w_out = g_w_out + mm_tn(f["activated"], d_ffn)
        d_act = mm_nt(d_ffn, w_out_f)
        _, gelu_pull = jax.vjp(exact_gelu, f["hidden_pre"])
        d_hidden = gelu_pull(d_act)[0].astype(jnp.bfloat16)
        g_w_in = g_w_in + mm_tn(f["first_low"], d_hidden)
        g_b_in = g_b_in + jnp.sum(d_hidden.astype(jnp.float32), axis=0)
        d_first = d_second + mm_nt(d_hidden, w_in_f)
        d_first_in, d_g1, d_s1 = ln_backward(d_first, f["normed1"], f["inv1"], g1)
        g_vec[5] = g_vec[5] + d_g2
        g_vec[6] = g_vec[6] + d_s2
        g_vec[7] = g_vec[7] + jnp.sum(d_second, axis=0)
        g_vec[3] = g_vec[3] + d_g1
        g_vec[4] = g_vec[4] + d_s1
        g_vec[2] = g_vec[2] + jnp.sum(d_first_in, axis=0)
        f.update(d_first_in=d_first_in)

    ffn_grad_pack = jnp.concatenate(
        [
            row_col_pack(g_w_in, ir, ic, True, nt),
            row_col_pack(g_w_out, outr, outc, False, nt),
            vec_pack(g_b_in[None, :], hlen, nt),
        ],
        axis=1,
    ).astype(jnp.bfloat16)
    ffn_grad = reduce_packed(ffn_grad_pack)

    g_wq = jnp.zeros((width, width), jnp.float32)
    g_wkv = jnp.zeros((width, 2 * width), jnp.float32)
    g_wo = jnp.zeros((width, width), jnp.float32)
    grad_tokens = []
    for s in range(seqs):
        f = fwd[s]
        d_branch = f["d_first_in"].astype(jnp.bfloat16)
        g_wo = g_wo + mm_tn(f["attended"], d_branch)
        d_att = mm_nt(d_branch, wo).astype(jnp.bfloat16)
        dah = d_att.reshape(local_rows, heads, HD).transpose(1, 0, 2)
        dqh, dkh, dvh = attention_bwd(f["length"], f["qh"], f["kh"], f["vh"], dah, f["lse"], scale)
        dq = dqh.transpose(1, 0, 2).reshape(local_rows, width)
        dkv = jnp.concatenate(
            [dkh.transpose(1, 0, 2).reshape(seq_len, width), dvh.transpose(1, 0, 2).reshape(seq_len, width)], axis=1
        ).astype(jnp.bfloat16)
        g_wq = g_wq + mm_tn(tokens[s], dq)
        g_wkv = g_wkv + mm_tn(f["x_all"], dkv)
        g_vec[0] = g_vec[0] + jnp.sum(dq.astype(jnp.float32), axis=0)
        g_vec[1] = g_vec[1] + jnp.sum(dkv[:, width:].astype(jnp.float32), axis=0)
        dx_kv = mm_nt(dkv, wkv).astype(jnp.bfloat16)
        dx_kv_own = lax.psum_scatter(dx_kv, SEQ_AXES, scatter_dimension=0, tiled=True).astype(jnp.float32)
        d_tok = f["d_first_in"] + mm_nt(dq, wq) + dx_kv_own
        grad_tokens.append(d_tok.astype(jnp.bfloat16))

    attn_grad_pack = jnp.concatenate(
        [
            row_col_pack(g_wq, qr, qc, True, nt),
            row_col_pack(g_wkv[:, :width], qr, qc, True, nt),
            row_col_pack(g_wkv[:, width:], qr, qc, True, nt),
            row_col_pack(g_wo, orr, oc, False, nt),
            vec_pack(jnp.stack(g_vec), vlen, nt),
        ],
        axis=1,
    ).astype(jnp.bfloat16)
    attn_grad = reduce_packed(attn_grad_pack)

    grad_wq = attn_grad[0:sq].reshape(qr, qc)
    grad_wk = attn_grad[sq : 2 * sq].reshape(qr, qc)
    grad_wv = attn_grad[2 * sq : 3 * sq].reshape(qr, qc)
    grad_wo = attn_grad[3 * sq : 3 * sq + so].reshape(orr, oc)
    grad_vec = attn_grad[3 * sq + so :].reshape(8, vlen)
    grad_w_in = ffn_grad[0:si].reshape(ir, ic)
    grad_w_out = ffn_grad[si : si + sout].reshape(outr, outc)
    grad_b_in = ffn_grad[si + sout :]

    return (
        jnp.stack(outputs),
        jnp.stack(grad_tokens),
        grad_wq,
        grad_wk,
        grad_wv,
        grad_wo,
        grad_w_in,
        grad_w_out,
        grad_vec[0],
        grad_vec[1],
        grad_vec[2],
        grad_vec[3],
        grad_vec[4],
        grad_vec[5],
        grad_vec[6],
        grad_vec[7],
        grad_b_in,
    )


def solution(mesh):
    row_spec = P("dp", ("ctx", "tensor"), None)
    w_rc = P(("dp", "ctx"), "tensor")
    w_cr = P("tensor", ("dp", "ctx"))
    vec = P(("dp", "ctx"))
    return jax.shard_map(
        body,
        mesh=mesh,
        in_specs=(row_spec, row_spec, P("dp"), w_rc, w_rc, w_rc, w_cr, w_rc, w_cr) + (vec,) * 9,
        out_specs=(row_spec, row_spec, w_rc, w_rc, w_rc, w_cr, w_rc, w_cr) + (vec,) * 9,
        check_vma=False,
    )
```

```python
import functools

import jax
import jax.numpy as jnp
from jax import lax
from jax.experimental import pallas as pl
from jax.experimental.pallas import tpu as pltpu
from jax.sharding import PartitionSpec as P

HD = 64
epsilon = 1e-05
masked_value = -1e30
ALL = ("dp", "ctx", "tensor")
SEQ_AXES = ("ctx", "tensor")


def exact_gelu(value):
    return jax.nn.gelu(value, approximate=False)


def mm(left, right):
    return jnp.dot(left, right, preferred_element_type=jnp.float32)


def mm_tn(left, right):
    return lax.dot_general(left, right, (((0,), (0,)), ((), ())), preferred_element_type=jnp.float32)


def mm_nt(left, right):
    return lax.dot_general(left, right, (((1,), (1,)), ((), ())), preferred_element_type=jnp.float32)


def ln_forward(hidden, gain, shift):
    mean = jnp.mean(hidden, axis=-1, keepdims=True)
    centre = hidden - mean
    var = jnp.mean(centre * centre, axis=-1, keepdims=True)
    inv = lax.rsqrt(var + epsilon)
    normed = centre * inv
    return normed * gain + shift, normed, inv


def ln_backward(grad_out, normed, inv, gain):
    d_normed = grad_out * gain
    width = normed.shape[-1]
    mean_d = jnp.sum(d_normed, axis=-1, keepdims=True) / width
    mean_dn = jnp.sum(d_normed * normed, axis=-1, keepdims=True) / width
    d_in = inv * (d_normed - mean_d - normed * mean_dn)
    d_gain = jnp.sum(grad_out * normed, axis=0)
    d_shift = jnp.sum(grad_out, axis=0)
    return d_in, d_gain, d_shift


KEY_BLOCK = 512


def _attn_fwd_kernel(len_ref, q_ref, k_ref, v_ref, o_ref, lse_ref, s_buf, *, scale, seq_len):
    length = len_ref[0]
    n_blocks = (length + KEY_BLOCK - 1) // KEY_BLOCK
    q = q_ref[0]
    rows = q.shape[0]

    def scores_of(b):
        start = pl.multiple_of(b * KEY_BLOCK, KEY_BLOCK)
        k_blk = k_ref[0, pl.ds(start, KEY_BLOCK), :]
        s = lax.dot_general(q, k_blk, (((1,), (1,)), ((), ())), preferred_element_type=jnp.float32) * scale
        pos = start + lax.broadcasted_iota(jnp.int32, s.shape, 1)
        return start, jnp.where(pos < length, s, masked_value)

    def pass_max(b, m):
        start, s = scores_of(b)
        s_buf[:, pl.ds(start, KEY_BLOCK)] = s
        return jnp.maximum(m, jnp.max(s, axis=1, keepdims=True))

    m = lax.fori_loop(0, n_blocks, pass_max, jnp.full((rows, 1), -jnp.inf, jnp.float32))

    def pass_sum(b, l):
        start = pl.multiple_of(b * KEY_BLOCK, KEY_BLOCK)
        e = jnp.exp(s_buf[:, pl.ds(start, KEY_BLOCK)] - m)
        s_buf[:, pl.ds(start, KEY_BLOCK)] = e
        return l + jnp.sum(e, axis=1, keepdims=True)

    l = lax.fori_loop(0, n_blocks, pass_sum, jnp.zeros((rows, 1), jnp.float32))

    def pass_out(b, acc):
        start = pl.multiple_of(b * KEY_BLOCK, KEY_BLOCK)
        probs = (s_buf[:, pl.ds(start, KEY_BLOCK)] / l).astype(jnp.bfloat16)
        v_blk = v_ref[0, pl.ds(start, KEY_BLOCK), :]
        return acc + jnp.dot(probs, v_blk, preferred_element_type=jnp.float32)

    acc = lax.fori_loop(0, n_blocks, pass_out, jnp.zeros((rows, q.shape[1]), jnp.float32))
    o_ref[0] = acc.astype(o_ref.dtype)
    lse_ref[0] = m + jnp.log(l)


def attention_fwd(length, qh, kh, vh, scale):
    heads, rows, hd = qh.shape
    seq_len = kh.shape[1]
    kernel = functools.partial(_attn_fwd_kernel, scale=scale, seq_len=seq_len)
    flops = 4 * heads * rows * seq_len * hd
    return pl.pallas_call(
        kernel,
        out_shape=(
            jax.ShapeDtypeStruct((heads, rows, hd), jnp.bfloat16),
            jax.ShapeDtypeStruct((heads, rows, 1), jnp.float32),
        ),
        grid_spec=pltpu.PrefetchScalarGridSpec(
            num_scalar_prefetch=1,
            grid=(heads,),
            in_specs=[
                pl.BlockSpec((1, rows, hd), lambda h, n: (h, 0, 0)),
                pl.BlockSpec((1, seq_len, hd), lambda h, n: (h, 0, 0)),
                pl.BlockSpec((1, seq_len, hd), lambda h, n: (h, 0, 0)),
            ],
            out_specs=[
                pl.BlockSpec((1, rows, hd), lambda h, n: (h, 0, 0)),
                pl.BlockSpec((1, rows, 1), lambda h, n: (h, 0, 0)),
            ],
            scratch_shapes=[pltpu.VMEM((rows, seq_len), jnp.float32)],
        ),
        cost_estimate=pl.CostEstimate(
            flops=flops, transcendentals=heads * rows * seq_len,
            bytes_accessed=2 * (qh.size + kh.size + vh.size + qh.size) + 4 * heads * rows,
        ),
    )(length.reshape(1), qh, kh, vh)


def _attn_bwd_kernel(len_ref, q_ref, k_ref, v_ref, do_ref, lse_ref, dq_ref, dk_ref, dv_ref, p_buf, dp_buf, *, scale):
    length = len_ref[0]
    n_blocks = (length + KEY_BLOCK - 1) // KEY_BLOCK
    total_blocks = k_ref.shape[1] // KEY_BLOCK
    q = q_ref[0]
    do = do_ref[0]
    lse = lse_ref[0]
    rows = q.shape[0]

    def pass_one(b, centre):
        start = pl.multiple_of(b * KEY_BLOCK, KEY_BLOCK)
        k_blk = k_ref[0, pl.ds(start, KEY_BLOCK), :]
        v_blk = v_ref[0, pl.ds(start, KEY_BLOCK), :]
        s = lax.dot_general(q, k_blk, (((1,), (1,)), ((), ())), preferred_element_type=jnp.float32) * scale
        pos = start + lax.broadcasted_iota(jnp.int32, s.shape, 1)
        s = jnp.where(pos < length, s, masked_value)
        p = jnp.exp(s - lse)
        dp = lax.dot_general(do, v_blk, (((1,), (1,)), ((), ())), preferred_element_type=jnp.float32)
        p_buf[:, pl.ds(start, KEY_BLOCK)] = p
        dp_buf[:, pl.ds(start, KEY_BLOCK)] = dp
        return centre + jnp.sum(p * dp, axis=1, keepdims=True)

    centre = lax.fori_loop(0, n_blocks, pass_one, jnp.zeros((rows, 1), jnp.float32))

    def pass_two(b, dq):
        start = pl.multiple_of(b * KEY_BLOCK, KEY_BLOCK)
        k_blk = k_ref[0, pl.ds(start, KEY_BLOCK), :]
        p = p_buf[:, pl.ds(start, KEY_BLOCK)]
        dp = dp_buf[:, pl.ds(start, KEY_BLOCK)]
        pos = start + lax.broadcasted_iota(jnp.int32, p.shape, 1)
        ds = jnp.where(pos < length, p * (dp - centre), 0.0).astype(jnp.bfloat16)
        dk_ref[0, pl.ds(start, KEY_BLOCK), :] = (
            lax.dot_general(ds, q, (((0,), (0,)), ((), ())), preferred_element_type=jnp.float32) * scale
        )
        dv_ref[0, pl.ds(start, KEY_BLOCK), :] = lax.dot_general(
            p.astype(jnp.bfloat16), do, (((0,), (0,)), ((), ())), preferred_element_type=jnp.float32
        )
        return dq + jnp.dot(ds, k_blk, preferred_element_type=jnp.float32)

    dq = lax.fori_loop(0, n_blocks, pass_two, jnp.zeros((rows, q.shape[1]), jnp.float32))
    dq_ref[0] = (dq * scale).astype(dq_ref.dtype)

    def pass_zero(b, carry):
        start = pl.multiple_of(b * KEY_BLOCK, KEY_BLOCK)
        dk_ref[0, pl.ds(start, KEY_BLOCK), :] = jnp.zeros((KEY_BLOCK, q.shape[1]), jnp.float32)
        dv_ref[0, pl.ds(start, KEY_BLOCK), :] = jnp.zeros((KEY_BLOCK, q.shape[1]), jnp.float32)
        return carry

    lax.fori_loop(n_blocks, total_blocks, pass_zero, 0)


def attention_bwd(length, qh, kh, vh, doh, lse, scale):
    heads, rows, hd = qh.shape
    seq_len = kh.shape[1]
    kernel = functools.partial(_attn_bwd_kernel, scale=scale)
    flops = 8 * heads * rows * seq_len * hd
    return pl.pallas_call(
        kernel,
        out_shape=(
            jax.ShapeDtypeStruct((heads, rows, hd), jnp.bfloat16),
            jax.ShapeDtypeStruct((heads, seq_len, hd), jnp.float32),
            jax.ShapeDtypeStruct((heads, seq_len, hd), jnp.float32),
        ),
        grid_spec=pltpu.PrefetchScalarGridSpec(
            num_scalar_prefetch=1,
            grid=(heads,),
            in_specs=[
                pl.BlockSpec((1, rows, hd), lambda h, n: (h, 0, 0)),
                pl.BlockSpec((1, seq_len, hd), lambda h, n: (h, 0, 0)),
                pl.BlockSpec((1, seq_len, hd), lambda h, n: (h, 0, 0)),
                pl.BlockSpec((1, rows, hd), lambda h, n: (h, 0, 0)),
                pl.BlockSpec((1, rows, 1), lambda h, n: (h, 0, 0)),
            ],
            out_specs=[
                pl.BlockSpec((1, rows, hd), lambda h, n: (h, 0, 0)),
                pl.BlockSpec((1, seq_len, hd), lambda h, n: (h, 0, 0)),
                pl.BlockSpec((1, seq_len, hd), lambda h, n: (h, 0, 0)),
            ],
            scratch_shapes=[pltpu.VMEM((rows, seq_len), jnp.float32), pltpu.VMEM((rows, seq_len), jnp.float32)],
        ),
        cost_estimate=pl.CostEstimate(
            flops=flops, transcendentals=heads * rows * seq_len,
            bytes_accessed=2 * (3 * qh.size + 2 * kh.size) + 8 * kh.size,
        ),
    )(length.reshape(1), qh, kh, vh, doh, lse)


def row_col_unpack(flat, rows, cols, row_major_blocks, nt):
    nb_outer = flat.shape[0] // nt
    blocks = flat.reshape(nb_outer, nt, rows, cols)
    if row_major_blocks:
        return blocks.transpose(0, 2, 1, 3).reshape(nb_outer * rows, nt * cols)
    return blocks.transpose(1, 2, 0, 3).reshape(nt * rows, nb_outer * cols)


def row_col_pack(full, rows, cols, row_major_blocks, nt):
    if row_major_blocks:
        nb_outer = full.shape[0] // rows
        blocks = full.reshape(nb_outer, rows, nt, cols).transpose(0, 2, 1, 3)
    else:
        nb_outer = full.shape[1] // cols
        blocks = full.reshape(nt, rows, nb_outer, cols).transpose(2, 0, 1, 3)
    return blocks.reshape(nb_outer * nt, rows * cols)


def vec_unpack(flat, length, nt):
    nb_outer = flat.shape[0] // nt
    blocks = flat.reshape(nb_outer, nt, -1, length)[:, 0]
    return blocks.transpose(1, 0, 2).reshape(blocks.shape[1], nb_outer * length)


def vec_pack(full, length, nt):
    n = full.shape[0]
    nb_outer = full.shape[1] // length
    blocks = full.reshape(n, nb_outer, length).transpose(1, 0, 2).reshape(nb_outer, 1, n * length)
    return jnp.broadcast_to(blocks, (nb_outer, nt, n * length)).reshape(nb_outer * nt, n * length)


def ctx_swap(x):
    return lax.ppermute(x, "ctx", [(0, 1), (1, 0)])


def ctx_join(own, other, ctx_rank, axis):
    first = jnp.concatenate([own, other], axis=axis)
    second = jnp.concatenate([other, own], axis=axis)
    return jnp.where(ctx_rank == 0, first, second)


def gather_packed(pack, ctx_rank):
    nd, nt = lax.axis_size("dp"), lax.axis_size("tensor")
    own = lax.all_gather(pack, ("dp", "tensor"), axis=0, tiled=False).reshape(nd, 1, nt, -1)
    other = ctx_swap(own)
    return ctx_join(own, other, ctx_rank, 1).reshape(nd * 2 * nt, -1)


def reduce_packed(pack, ctx_rank):
    nd, nt = lax.axis_size("dp"), lax.axis_size("tensor")
    devices, chunk_len = pack.shape
    padded = -(-chunk_len // 2048) * 2048
    pack = jnp.pad(pack, ((0, 0), (0, padded - chunk_len))).reshape(nd, 2, nt, padded)
    mine = lax.dynamic_index_in_dim(pack, ctx_rank, axis=1, keepdims=False)
    theirs = lax.dynamic_index_in_dim(pack, 1 - ctx_rank, axis=1, keepdims=False)
    summed = (mine.astype(jnp.float32) + ctx_swap(theirs).astype(jnp.float32)).astype(jnp.bfloat16)
    own = lax.psum_scatter(summed.reshape(-1, 128), ("dp", "tensor"), scatter_dimension=0, tiled=True)
    return own.reshape(-1)[:chunk_len].astype(jnp.float32)


def body(
    tokens,
    cotangent,
    lengths,
    w_query,
    w_key,
    w_value,
    w_output,
    w_in,
    w_out,
    bias_query,
    bias_value,
    bias_output,
    gain_first,
    shift_first,
    gain_second,
    shift_second,
    bias_out,
    bias_in,
):
    seqs, local_rows, width = tokens.shape
    ctx_rank = lax.axis_index("ctx")
    tensor_rank = lax.axis_index("tensor")
    nt = lax.axis_size("tensor")
    chunk = ctx_rank * nt + tensor_rank
    seq_len = local_rows * lax.axis_size("ctx") * lax.axis_size("tensor")
    heads = width // HD
    scale = HD ** (-0.5)

    qr, qc = w_query.shape
    orr, oc = w_output.shape
    ir, ic = w_in.shape
    outr, outc = w_out.shape
    vlen = bias_query.shape[0]
    hlen = bias_in.shape[0]

    vectors = jnp.stack(
        [bias_query, bias_value, bias_output, gain_first, shift_first, gain_second, shift_second, bias_out]
    )
    attn_pack = jnp.concatenate(
        [w_query.reshape(-1), w_key.reshape(-1), w_value.reshape(-1), w_output.reshape(-1), vectors.reshape(-1)]
    )
    ffn_pack = jnp.concatenate([w_in.reshape(-1), w_out.reshape(-1), bias_in.reshape(-1)])
    attn_all = gather_packed(attn_pack, ctx_rank)
    ffn_all = gather_packed(ffn_pack, ctx_rank)

    sq = qr * qc
    so = orr * oc
    wq = row_col_unpack(attn_all[:, 0:sq], qr, qc, True, nt)
    wk = row_col_unpack(attn_all[:, sq : 2 * sq], qr, qc, True, nt)
    wv = row_col_unpack(attn_all[:, 2 * sq : 3 * sq], qr, qc, True, nt)
    wo = row_col_unpack(attn_all[:, 3 * sq : 3 * sq + so], orr, oc, False, nt)
    vec_full = vec_unpack(attn_all[:, 3 * sq + so :], vlen, nt).astype(jnp.float32)
    b_q, b_v, b_o, g1, s1, g2, s2, b_out = [vec_full[i] for i in range(8)]
    wkv = jnp.concatenate([wk, wv], axis=1)

    si = ir * ic
    sout = outr * outc
    w_in_f = row_col_unpack(ffn_all[:, 0:si], ir, ic, True, nt)
    w_out_f = row_col_unpack(ffn_all[:, si : si + sout], outr, outc, False, nt)
    b_in = vec_unpack(ffn_all[:, si + sout :], hlen, nt)[0].astype(jnp.float32)

    positions = jnp.arange(seq_len, dtype=jnp.int32)
    row_positions = chunk * local_rows + jnp.arange(local_rows, dtype=jnp.int32)

    fwd = []
    for s in range(seqs):
        x_own = tokens[s]
        length = lengths[s]
        x_half = lax.all_gather(x_own, "tensor", axis=0, tiled=True)
        x_all = ctx_join(x_half, ctx_swap(x_half), ctx_rank, 0)
        q = (mm(x_own, wq) + b_q).astype(jnp.bfloat16)
        kv = mm(x_all, wkv)
        k = kv[:, :width].astype(jnp.bfloat16)
        v = (kv[:, width:] + b_v).astype(jnp.bfloat16)
        qh = q.reshape(local_rows, heads, HD).transpose(1, 0, 2)
        kh = k.reshape(seq_len, heads, HD).transpose(1, 0, 2)
        vh = v.reshape(seq_len, heads, HD).transpose(1, 0, 2)
        oh, lse = attention_fwd(length, qh, kh, vh, scale)
        attended = oh.transpose(1, 0, 2).reshape(local_rows, width)
        first_in = x_own.astype(jnp.float32) + (mm(attended, wo) + b_o)
        first, normed1, inv1 = ln_forward(first_in, g1, s1)
        fwd.append(dict(x_all=x_all, qh=qh, kh=kh, vh=vh, lse=lse, attended=attended, first=first,
                        normed1=normed1, inv1=inv1, length=length))

    outputs = []
    for s in range(seqs):
        f = fwd[s]
        first_low = f["first"].astype(jnp.bfloat16)
        hidden_pre = mm(first_low, w_in_f) + b_in
        activated = exact_gelu(hidden_pre).astype(jnp.bfloat16)
        second_in = f["first"] + mm(activated, w_out_f) + b_out
        result, normed2, inv2 = ln_forward(second_in, g2, s2)
        outputs.append(result.astype(jnp.bfloat16))
        f.update(first_low=first_low, hidden_pre=hidden_pre, activated=activated, normed2=normed2, inv2=inv2)

    g_w_in = jnp.zeros((width, w_in_f.shape[1]), jnp.float32)
    g_w_out = jnp.zeros((w_out_f.shape[0], width), jnp.float32)
    g_b_in = jnp.zeros((w_in_f.shape[1],), jnp.float32)
    g_vec = [jnp.zeros((width,), jnp.float32) for _ in range(8)]
    for s in range(seqs):
        f = fwd[s]
        row_valid = (row_positions < f["length"]).astype(jnp.float32)
        upstream = cotangent[s].astype(jnp.float32) * row_valid[:, None]
        d_second, d_g2, d_s2 = ln_backward(upstream, f["normed2"], f["inv2"], g2)
        d_ffn = d_second.astype(jnp.bfloat16)
        g_w_out = g_w_out + mm_tn(f["activated"], d_ffn)
        d_act = mm_nt(d_ffn, w_out_f)
        _, gelu_pull = jax.vjp(exact_gelu, f["hidden_pre"])
        d_hidden = gelu_pull(d_act)[0].astype(jnp.bfloat16)
        g_w_in = g_w_in + mm_tn(f["first_low"], d_hidden)
        g_b_in = g_b_in + jnp.sum(d_hidden.astype(jnp.float32), axis=0)
        d_first = d_second + mm_nt(d_hidden, w_in_f)
        d_first_in, d_g1, d_s1 = ln_backward(d_first, f["normed1"], f["inv1"], g1)
        g_vec[5] = g_vec[5] + d_g2
        g_vec[6] = g_vec[6] + d_s2
        g_vec[7] = g_vec[7] + jnp.sum(d_second, axis=0)
        g_vec[3] = g_vec[3] + d_g1
        g_vec[4] = g_vec[4] + d_s1
        g_vec[2] = g_vec[2] + jnp.sum(d_first_in, axis=0)
        f.update(d_first_in=d_first_in)

    ffn_grad_pack = jnp.concatenate(
        [
            row_col_pack(g_w_in, ir, ic, True, nt),
            row_col_pack(g_w_out, outr, outc, False, nt),
            vec_pack(g_b_in[None, :], hlen, nt),
        ],
        axis=1,
    ).astype(jnp.bfloat16)
    ffn_grad = reduce_packed(ffn_grad_pack, ctx_rank)

    g_wq = jnp.zeros((width, width), jnp.float32)
    g_wkv = jnp.zeros((width, 2 * width), jnp.float32)
    g_wo = jnp.zeros((width, width), jnp.float32)
    grad_tokens = []
    for s in range(seqs):
        f = fwd[s]
        d_branch = f["d_first_in"].astype(jnp.bfloat16)
        g_wo = g_wo + mm_tn(f["attended"], d_branch)
        d_att = mm_nt(d_branch, wo).astype(jnp.bfloat16)
        dah = d_att.reshape(local_rows, heads, HD).transpose(1, 0, 2)
        dqh, dkh, dvh = attention_bwd(f["length"], f["qh"], f["kh"], f["vh"], dah, f["lse"], scale)
        dq = dqh.transpose(1, 0, 2).reshape(local_rows, width)
        dkv = jnp.concatenate(
            [dkh.transpose(1, 0, 2).reshape(seq_len, width), dvh.transpose(1, 0, 2).reshape(seq_len, width)], axis=1
        ).astype(jnp.bfloat16)
        g_wq = g_wq + mm_tn(tokens[s], dq)
        g_wkv = g_wkv + mm_tn(f["x_all"], dkv)
        g_vec[0] = g_vec[0] + jnp.sum(dq.astype(jnp.float32), axis=0)
        g_vec[1] = g_vec[1] + jnp.sum(dkv[:, width:].astype(jnp.float32), axis=0)
        dx_kv = mm_nt(dkv, wkv).reshape(2, seq_len // 2, width)
        dx_mine = lax.dynamic_index_in_dim(dx_kv, ctx_rank, axis=0, keepdims=False)
        dx_theirs = lax.dynamic_index_in_dim(dx_kv, 1 - ctx_rank, axis=0, keepdims=False).astype(jnp.bfloat16)
        dx_half = (dx_mine + ctx_swap(dx_theirs).astype(jnp.float32)).astype(jnp.bfloat16)
        dx_kv_own = lax.psum_scatter(dx_half, "tensor", scatter_dimension=0, tiled=True).astype(jnp.float32)
        d_tok = f["d_first_in"] + mm_nt(dq, wq) + dx_kv_own
        grad_tokens.append(d_tok.astype(jnp.bfloat16))

    attn_grad_pack = jnp.concatenate(
        [
            row_col_pack(g_wq, qr, qc, True, nt),
            row_col_pack(g_wkv[:, :width], qr, qc, True, nt),
            row_col_pack(g_wkv[:, width:], qr, qc, True, nt),
            row_col_pack(g_wo, orr, oc, False, nt),
            vec_pack(jnp.stack(g_vec), vlen, nt),
        ],
        axis=1,
    ).astype(jnp.bfloat16)
    attn_grad = reduce_packed(attn_grad_pack, ctx_rank)

    grad_wq = attn_grad[0:sq].reshape(qr, qc)
    grad_wk = attn_grad[sq : 2 * sq].reshape(qr, qc)
    grad_wv = attn_grad[2 * sq : 3 * sq].reshape(qr, qc)
    grad_wo = attn_grad[3 * sq : 3 * sq + so].reshape(orr, oc)
    grad_vec = attn_grad[3 * sq + so :].reshape(8, vlen)
    grad_w_in = ffn_grad[0:si].reshape(ir, ic)
    grad_w_out = ffn_grad[si : si + sout].reshape(outr, outc)
    grad_b_in = ffn_grad[si + sout :]

    return (
        jnp.stack(outputs),
        jnp.stack(grad_tokens),
        grad_wq,
        grad_wk,
        grad_wv,
        grad_wo,
        grad_w_in,
        grad_w_out,
        grad_vec[0],
        grad_vec[1],
        grad_vec[2],
        grad_vec[3],
        grad_vec[4],
        grad_vec[5],
        grad_vec[6],
        grad_vec[7],
        grad_b_in,
    )


def solution(mesh):
    row_spec = P("dp", ("ctx", "tensor"), None)
    w_rc = P(("dp", "ctx"), "tensor")
    w_cr = P("tensor", ("dp", "ctx"))
    vec = P(("dp", "ctx"))
    return jax.shard_map(
        body,
        mesh=mesh,
        in_specs=(row_spec, row_spec, P("dp"), w_rc, w_rc, w_rc, w_cr, w_rc, w_cr) + (vec,) * 9,
        out_specs=(row_spec, row_spec, w_rc, w_rc, w_rc, w_cr, w_rc, w_cr) + (vec,) * 9,
        check_vma=False,
    )
```

```python
import functools

import jax
import jax.numpy as jnp
from jax import lax
from jax.experimental import pallas as pl
from jax.experimental.pallas import tpu as pltpu
from jax.sharding import PartitionSpec as P

HD = 64
epsilon = 1e-05
masked_value = -1e30
ALL = ("dp", "ctx", "tensor")
SEQ_AXES = ("ctx", "tensor")


def exact_gelu(value):
    return jax.nn.gelu(value, approximate=False)


def mm(left, right):
    return jnp.dot(left, right, preferred_element_type=jnp.float32)


def mm_tn(left, right):
    return lax.dot_general(left, right, (((0,), (0,)), ((), ())), preferred_element_type=jnp.float32)


def mm_nt(left, right):
    return lax.dot_general(left, right, (((1,), (1,)), ((), ())), preferred_element_type=jnp.float32)


def ln_forward(hidden, gain, shift):
    mean = jnp.mean(hidden, axis=-1, keepdims=True)
    centre = hidden - mean
    var = jnp.mean(centre * centre, axis=-1, keepdims=True)
    inv = lax.rsqrt(var + epsilon)
    normed = centre * inv
    return normed * gain + shift, normed, inv


def ln_backward(grad_out, normed, inv, gain):
    d_normed = grad_out * gain
    width = normed.shape[-1]
    mean_d = jnp.sum(d_normed, axis=-1, keepdims=True) / width
    mean_dn = jnp.sum(d_normed * normed, axis=-1, keepdims=True) / width
    d_in = inv * (d_normed - mean_d - normed * mean_dn)
    d_gain = jnp.sum(grad_out * normed, axis=0)
    d_shift = jnp.sum(grad_out, axis=0)
    return d_in, d_gain, d_shift


KEY_BLOCK = 512


def _attn_fwd_kernel(len_ref, q_ref, k_ref, v_ref, o_ref, lse_ref, s_buf, *, scale, seq_len):
    length = len_ref[0]
    n_blocks = (length + KEY_BLOCK - 1) // KEY_BLOCK
    q = q_ref[0]
    rows = q.shape[0]

    def scores_of(b):
        start = pl.multiple_of(b * KEY_BLOCK, KEY_BLOCK)
        k_blk = k_ref[0, pl.ds(start, KEY_BLOCK), :]
        s = lax.dot_general(q, k_blk, (((1,), (1,)), ((), ())), preferred_element_type=jnp.float32) * scale
        pos = start + lax.broadcasted_iota(jnp.int32, s.shape, 1)
        return start, jnp.where(pos < length, s, masked_value)

    def pass_max(b, m):
        start, s = scores_of(b)
        s_buf[:, pl.ds(start, KEY_BLOCK)] = s
        return jnp.maximum(m, jnp.max(s, axis=1, keepdims=True))

    m = lax.fori_loop(0, n_blocks, pass_max, jnp.full((rows, 1), -jnp.inf, jnp.float32))

    def pass_sum(b, l):
        start = pl.multiple_of(b * KEY_BLOCK, KEY_BLOCK)
        e = jnp.exp(s_buf[:, pl.ds(start, KEY_BLOCK)] - m)
        s_buf[:, pl.ds(start, KEY_BLOCK)] = e
        return l + jnp.sum(e, axis=1, keepdims=True)

    l = lax.fori_loop(0, n_blocks, pass_sum, jnp.zeros((rows, 1), jnp.float32))

    def pass_out(b, acc):
        start = pl.multiple_of(b * KEY_BLOCK, KEY_BLOCK)
        probs = (s_buf[:, pl.ds(start, KEY_BLOCK)] / l).astype(jnp.bfloat16)
        v_blk = v_ref[0, pl.ds(start, KEY_BLOCK), :]
        return acc + jnp.dot(probs, v_blk, preferred_element_type=jnp.float32)

    acc = lax.fori_loop(0, n_blocks, pass_out, jnp.zeros((rows, q.shape[1]), jnp.float32))
    o_ref[0] = acc.astype(o_ref.dtype)
    lse_ref[0] = m + jnp.log(l)


def attention_fwd(length, qh, kh, vh, scale):
    heads, rows, hd = qh.shape
    seq_len = kh.shape[1]
    kernel = functools.partial(_attn_fwd_kernel, scale=scale, seq_len=seq_len)
    flops = 4 * heads * rows * seq_len * hd
    return pl.pallas_call(
        kernel,
        out_shape=(
            jax.ShapeDtypeStruct((heads, rows, hd), jnp.bfloat16),
            jax.ShapeDtypeStruct((heads, rows, 1), jnp.float32),
        ),
        grid_spec=pltpu.PrefetchScalarGridSpec(
            num_scalar_prefetch=1,
            grid=(heads,),
            in_specs=[
                pl.BlockSpec((1, rows, hd), lambda h, n: (h, 0, 0)),
                pl.BlockSpec((1, seq_len, hd), lambda h, n: (h, 0, 0)),
                pl.BlockSpec((1, seq_len, hd), lambda h, n: (h, 0, 0)),
            ],
            out_specs=[
                pl.BlockSpec((1, rows, hd), lambda h, n: (h, 0, 0)),
                pl.BlockSpec((1, rows, 1), lambda h, n: (h, 0, 0)),
            ],
            scratch_shapes=[pltpu.VMEM((rows, seq_len), jnp.float32)],
        ),
        cost_estimate=pl.CostEstimate(
            flops=flops, transcendentals=heads * rows * seq_len,
            bytes_accessed=2 * (qh.size + kh.size + vh.size + qh.size) + 4 * heads * rows,
        ),
    )(length.reshape(1), qh, kh, vh)


def _attn_bwd_kernel(len_ref, q_ref, k_ref, v_ref, do_ref, lse_ref, dq_ref, dk_ref, dv_ref, p_buf, dp_buf, *, scale):
    length = len_ref[0]
    n_blocks = (length + KEY_BLOCK - 1) // KEY_BLOCK
    total_blocks = k_ref.shape[1] // KEY_BLOCK
    q = q_ref[0]
    do = do_ref[0]
    lse = lse_ref[0]
    rows = q.shape[0]

    def pass_one(b, centre):
        start = pl.multiple_of(b * KEY_BLOCK, KEY_BLOCK)
        k_blk = k_ref[0, pl.ds(start, KEY_BLOCK), :]
        v_blk = v_ref[0, pl.ds(start, KEY_BLOCK), :]
        s = lax.dot_general(q, k_blk, (((1,), (1,)), ((), ())), preferred_element_type=jnp.float32) * scale
        pos = start + lax.broadcasted_iota(jnp.int32, s.shape, 1)
        s = jnp.where(pos < length, s, masked_value)
        p = jnp.exp(s - lse)
        dp = lax.dot_general(do, v_blk, (((1,), (1,)), ((), ())), preferred_element_type=jnp.float32)
        p_buf[:, pl.ds(start, KEY_BLOCK)] = p
        dp_buf[:, pl.ds(start, KEY_BLOCK)] = dp
        return centre + jnp.sum(p * dp, axis=1, keepdims=True)

    centre = lax.fori_loop(0, n_blocks, pass_one, jnp.zeros((rows, 1), jnp.float32))

    def pass_two(b, dq):
        start = pl.multiple_of(b * KEY_BLOCK, KEY_BLOCK)
        k_blk = k_ref[0, pl.ds(start, KEY_BLOCK), :]
        p = p_buf[:, pl.ds(start, KEY_BLOCK)]
        dp = dp_buf[:, pl.ds(start, KEY_BLOCK)]
        pos = start + lax.broadcasted_iota(jnp.int32, p.shape, 1)
        ds = jnp.where(pos < length, p * (dp - centre), 0.0).astype(jnp.bfloat16)
        dk_ref[0, pl.ds(start, KEY_BLOCK), :] = (
            lax.dot_general(ds, q, (((0,), (0,)), ((), ())), preferred_element_type=jnp.float32) * scale
        )
        dv_ref[0, pl.ds(start, KEY_BLOCK), :] = lax.dot_general(
            p.astype(jnp.bfloat16), do, (((0,), (0,)), ((), ())), preferred_element_type=jnp.float32
        )
        return dq + jnp.dot(ds, k_blk, preferred_element_type=jnp.float32)

    dq = lax.fori_loop(0, n_blocks, pass_two, jnp.zeros((rows, q.shape[1]), jnp.float32))
    dq_ref[0] = (dq * scale).astype(dq_ref.dtype)

    def pass_zero(b, carry):
        start = pl.multiple_of(b * KEY_BLOCK, KEY_BLOCK)
        dk_ref[0, pl.ds(start, KEY_BLOCK), :] = jnp.zeros((KEY_BLOCK, q.shape[1]), jnp.float32)
        dv_ref[0, pl.ds(start, KEY_BLOCK), :] = jnp.zeros((KEY_BLOCK, q.shape[1]), jnp.float32)
        return carry

    lax.fori_loop(n_blocks, total_blocks, pass_zero, 0)


def attention_bwd(length, qh, kh, vh, doh, lse, scale):
    heads, rows, hd = qh.shape
    seq_len = kh.shape[1]
    kernel = functools.partial(_attn_bwd_kernel, scale=scale)
    flops = 8 * heads * rows * seq_len * hd
    return pl.pallas_call(
        kernel,
        out_shape=(
            jax.ShapeDtypeStruct((heads, rows, hd), jnp.bfloat16),
            jax.ShapeDtypeStruct((heads, seq_len, hd), jnp.float32),
            jax.ShapeDtypeStruct((heads, seq_len, hd), jnp.float32),
        ),
        grid_spec=pltpu.PrefetchScalarGridSpec(
            num_scalar_prefetch=1,
            grid=(heads,),
            in_specs=[
                pl.BlockSpec((1, rows, hd), lambda h, n: (h, 0, 0)),
                pl.BlockSpec((1, seq_len, hd), lambda h, n: (h, 0, 0)),
                pl.BlockSpec((1, seq_len, hd), lambda h, n: (h, 0, 0)),
                pl.BlockSpec((1, rows, hd), lambda h, n: (h, 0, 0)),
                pl.BlockSpec((1, rows, 1), lambda h, n: (h, 0, 0)),
            ],
            out_specs=[
                pl.BlockSpec((1, rows, hd), lambda h, n: (h, 0, 0)),
                pl.BlockSpec((1, seq_len, hd), lambda h, n: (h, 0, 0)),
                pl.BlockSpec((1, seq_len, hd), lambda h, n: (h, 0, 0)),
            ],
            scratch_shapes=[pltpu.VMEM((rows, seq_len), jnp.float32), pltpu.VMEM((rows, seq_len), jnp.float32)],
        ),
        cost_estimate=pl.CostEstimate(
            flops=flops, transcendentals=heads * rows * seq_len,
            bytes_accessed=2 * (3 * qh.size + 2 * kh.size) + 8 * kh.size,
        ),
    )(length.reshape(1), qh, kh, vh, doh, lse)


def row_col_unpack(flat, rows, cols, row_major_blocks, nt):
    nb_outer = flat.shape[0] // nt
    blocks = flat.reshape(nb_outer, nt, rows, cols)
    if row_major_blocks:
        return blocks.transpose(0, 2, 1, 3).reshape(nb_outer * rows, nt * cols)
    return blocks.transpose(1, 2, 0, 3).reshape(nt * rows, nb_outer * cols)


def row_col_pack(full, rows, cols, row_major_blocks, nt):
    if row_major_blocks:
        nb_outer = full.shape[0] // rows
        blocks = full.reshape(nb_outer, rows, nt, cols).transpose(0, 2, 1, 3)
    else:
        nb_outer = full.shape[1] // cols
        blocks = full.reshape(nt, rows, nb_outer, cols).transpose(2, 0, 1, 3)
    return blocks.reshape(nb_outer * nt, rows * cols)


def vec_unpack(flat, length, nt):
    nb_outer = flat.shape[0] // nt
    blocks = flat.reshape(nb_outer, nt, -1, length)[:, 0]
    return blocks.transpose(1, 0, 2).reshape(blocks.shape[1], nb_outer * length)


def vec_pack(full, length, nt):
    n = full.shape[0]
    nb_outer = full.shape[1] // length
    blocks = full.reshape(n, nb_outer, length).transpose(1, 0, 2).reshape(nb_outer, 1, n * length)
    return jnp.broadcast_to(blocks, (nb_outer, nt, n * length)).reshape(nb_outer * nt, n * length)


def ctx_swap(x):
    return lax.ppermute(x, "ctx", [(0, 1), (1, 0)])


def reduce_packed(pack, ctx_rank):
    nd, nt = lax.axis_size("dp"), lax.axis_size("tensor")
    devices, chunk_len = pack.shape
    padded = -(-chunk_len // 2048) * 2048
    pack = jnp.pad(pack, ((0, 0), (0, padded - chunk_len))).reshape(nd, 2, nt, padded)
    mine = lax.dynamic_index_in_dim(pack, ctx_rank, axis=1, keepdims=False)
    theirs = lax.dynamic_index_in_dim(pack, 1 - ctx_rank, axis=1, keepdims=False)
    summed = (mine.astype(jnp.float32) + ctx_swap(theirs).astype(jnp.float32)).astype(jnp.bfloat16)
    own = lax.psum_scatter(summed.reshape(-1, 128), ("dp", "tensor"), scatter_dimension=0, tiled=True)
    return own.reshape(-1)[:chunk_len].astype(jnp.float32)


def body(
    tokens,
    cotangent,
    lengths,
    w_query,
    w_key,
    w_value,
    w_output,
    w_in,
    w_out,
    bias_query,
    bias_value,
    bias_output,
    gain_first,
    shift_first,
    gain_second,
    shift_second,
    bias_out,
    bias_in,
):
    seqs, local_rows, width = tokens.shape
    ctx_rank = lax.axis_index("ctx")
    tensor_rank = lax.axis_index("tensor")
    nt = lax.axis_size("tensor")
    chunk = ctx_rank * nt + tensor_rank
    seq_len = local_rows * lax.axis_size("ctx") * lax.axis_size("tensor")
    heads = width // HD
    scale = HD ** (-0.5)

    qr, qc = w_query.shape
    orr, oc = w_output.shape
    ir, ic = w_in.shape
    outr, outc = w_out.shape
    vlen = bias_query.shape[0]
    hlen = bias_in.shape[0]

    vectors = jnp.stack(
        [bias_query, bias_value, bias_output, gain_first, shift_first, gain_second, shift_second, bias_out]
    )
    attn_pack = jnp.concatenate(
        [w_query.reshape(-1), w_key.reshape(-1), w_value.reshape(-1), w_output.reshape(-1), vectors.reshape(-1)]
    )
    ffn_pack = jnp.concatenate([w_in.reshape(-1), w_out.reshape(-1), bias_in.reshape(-1)])
    attn_all = lax.all_gather(attn_pack, ALL, axis=0, tiled=False)
    ffn_all = lax.all_gather(ffn_pack, ALL, axis=0, tiled=False)

    sq = qr * qc
    so = orr * oc
    wq = row_col_unpack(attn_all[:, 0:sq], qr, qc, True, nt)
    wk = row_col_unpack(attn_all[:, sq : 2 * sq], qr, qc, True, nt)
    wv = row_col_unpack(attn_all[:, 2 * sq : 3 * sq], qr, qc, True, nt)
    wo = row_col_unpack(attn_all[:, 3 * sq : 3 * sq + so], orr, oc, False, nt)
    vec_full = vec_unpack(attn_all[:, 3 * sq + so :], vlen, nt).astype(jnp.float32)
    b_q, b_v, b_o, g1, s1, g2, s2, b_out = [vec_full[i] for i in range(8)]
    wkv = jnp.concatenate([wk, wv], axis=1)

    si = ir * ic
    sout = outr * outc
    w_in_f = row_col_unpack(ffn_all[:, 0:si], ir, ic, True, nt)
    w_out_f = row_col_unpack(ffn_all[:, si : si + sout], outr, outc, False, nt)
    b_in = vec_unpack(ffn_all[:, si + sout :], hlen, nt)[0].astype(jnp.float32)

    positions = jnp.arange(seq_len, dtype=jnp.int32)
    row_positions = chunk * local_rows + jnp.arange(local_rows, dtype=jnp.int32)

    fwd = []
    for s in range(seqs):
        x_own = tokens[s]
        length = lengths[s]
        x_all = lax.all_gather(x_own, SEQ_AXES, axis=0, tiled=True)
        q = (mm(x_own, wq) + b_q).astype(jnp.bfloat16)
        kv = mm(x_all, wkv)
        k = kv[:, :width].astype(jnp.bfloat16)
        v = (kv[:, width:] + b_v).astype(jnp.bfloat16)
        qh = q.reshape(local_rows, heads, HD).transpose(1, 0, 2)
        kh = k.reshape(seq_len, heads, HD).transpose(1, 0, 2)
        vh = v.reshape(seq_len, heads, HD).transpose(1, 0, 2)
        oh, lse = attention_fwd(length, qh, kh, vh, scale)
        attended = oh.transpose(1, 0, 2).reshape(local_rows, width)
        first_in = x_own.astype(jnp.float32) + (mm(attended, wo) + b_o)
        first, normed1, inv1 = ln_forward(first_in, g1, s1)
        fwd.append(dict(x_all=x_all, qh=qh, kh=kh, vh=vh, lse=lse, attended=attended, first=first,
                        normed1=normed1, inv1=inv1, length=length))

    outputs = []
    for s in range(seqs):
        f = fwd[s]
        first_low = f["first"].astype(jnp.bfloat16)
        hidden_pre = mm(first_low, w_in_f) + b_in
        activated = exact_gelu(hidden_pre).astype(jnp.bfloat16)
        second_in = f["first"] + mm(activated, w_out_f) + b_out
        result, normed2, inv2 = ln_forward(second_in, g2, s2)
        outputs.append(result.astype(jnp.bfloat16))
        f.update(first_low=first_low, hidden_pre=hidden_pre, activated=activated, normed2=normed2, inv2=inv2)

    g_w_in = jnp.zeros((width, w_in_f.shape[1]), jnp.float32)
    g_w_out = jnp.zeros((w_out_f.shape[0], width), jnp.float32)
    g_b_in = jnp.zeros((w_in_f.shape[1],), jnp.float32)
    g_vec = [jnp.zeros((width,), jnp.float32) for _ in range(8)]
    for s in range(seqs):
        f = fwd[s]
        row_valid = (row_positions < f["length"]).astype(jnp.float32)
        upstream = cotangent[s].astype(jnp.float32) * row_valid[:, None]
        d_second, d_g2, d_s2 = ln_backward(upstream, f["normed2"], f["inv2"], g2)
        d_ffn = d_second.astype(jnp.bfloat16)
        g_w_out = g_w_out + mm_tn(f["activated"], d_ffn)
        d_act = mm_nt(d_ffn, w_out_f)
        _, gelu_pull = jax.vjp(exact_gelu, f["hidden_pre"])
        d_hidden = gelu_pull(d_act)[0].astype(jnp.bfloat16)
        g_w_in = g_w_in + mm_tn(f["first_low"], d_hidden)
        g_b_in = g_b_in + jnp.sum(d_hidden.astype(jnp.float32), axis=0)
        d_first = d_second + mm_nt(d_hidden, w_in_f)
        d_first_in, d_g1, d_s1 = ln_backward(d_first, f["normed1"], f["inv1"], g1)
        g_vec[5] = g_vec[5] + d_g2
        g_vec[6] = g_vec[6] + d_s2
        g_vec[7] = g_vec[7] + jnp.sum(d_second, axis=0)
        g_vec[3] = g_vec[3] + d_g1
        g_vec[4] = g_vec[4] + d_s1
        g_vec[2] = g_vec[2] + jnp.sum(d_first_in, axis=0)
        f.update(d_first_in=d_first_in)

    ffn_grad_pack = jnp.concatenate(
        [
            row_col_pack(g_w_in, ir, ic, True, nt),
            row_col_pack(g_w_out, outr, outc, False, nt),
            vec_pack(g_b_in[None, :], hlen, nt),
        ],
        axis=1,
    ).astype(jnp.bfloat16)
    ffn_grad = reduce_packed(ffn_grad_pack, ctx_rank)

    g_wq = jnp.zeros((width, width), jnp.float32)
    g_wkv = jnp.zeros((width, 2 * width), jnp.float32)
    g_wo = jnp.zeros((width, width), jnp.float32)
    grad_tokens = []
    for s in range(seqs):
        f = fwd[s]
        d_branch = f["d_first_in"].astype(jnp.bfloat16)
        g_wo = g_wo + mm_tn(f["attended"], d_branch)
        d_att = mm_nt(d_branch, wo).astype(jnp.bfloat16)
        dah = d_att.reshape(local_rows, heads, HD).transpose(1, 0, 2)
        dqh, dkh, dvh = attention_bwd(f["length"], f["qh"], f["kh"], f["vh"], dah, f["lse"], scale)
        dq = dqh.transpose(1, 0, 2).reshape(local_rows, width)
        dkv = jnp.concatenate(
            [dkh.transpose(1, 0, 2).reshape(seq_len, width), dvh.transpose(1, 0, 2).reshape(seq_len, width)], axis=1
        ).astype(jnp.bfloat16)
        g_wq = g_wq + mm_tn(tokens[s], dq)
        g_wkv = g_wkv + mm_tn(f["x_all"], dkv)
        g_vec[0] = g_vec[0] + jnp.sum(dq.astype(jnp.float32), axis=0)
        g_vec[1] = g_vec[1] + jnp.sum(dkv[:, width:].astype(jnp.float32), axis=0)
        dx_kv = mm_nt(dkv, wkv).reshape(2, seq_len // 2, width)
        dx_mine = lax.dynamic_index_in_dim(dx_kv, ctx_rank, axis=0, keepdims=False)
        dx_theirs = lax.dynamic_index_in_dim(dx_kv, 1 - ctx_rank, axis=0, keepdims=False).astype(jnp.bfloat16)
        dx_half = (dx_mine + ctx_swap(dx_theirs).astype(jnp.float32)).astype(jnp.bfloat16)
        dx_kv_own = lax.psum_scatter(dx_half, "tensor", scatter_dimension=0, tiled=True).astype(jnp.float32)
        d_tok = f["d_first_in"] + mm_nt(dq, wq) + dx_kv_own
        grad_tokens.append(d_tok.astype(jnp.bfloat16))

    attn_grad_pack = jnp.concatenate(
        [
            row_col_pack(g_wq, qr, qc, True, nt),
            row_col_pack(g_wkv[:, :width], qr, qc, True, nt),
            row_col_pack(g_wkv[:, width:], qr, qc, True, nt),
            row_col_pack(g_wo, orr, oc, False, nt),
            vec_pack(jnp.stack(g_vec), vlen, nt),
        ],
        axis=1,
    ).astype(jnp.bfloat16)
    attn_grad = reduce_packed(attn_grad_pack, ctx_rank)

    grad_wq = attn_grad[0:sq].reshape(qr, qc)
    grad_wk = attn_grad[sq : 2 * sq].reshape(qr, qc)
    grad_wv = attn_grad[2 * sq : 3 * sq].reshape(qr, qc)
    grad_wo = attn_grad[3 * sq : 3 * sq + so].reshape(orr, oc)
    grad_vec = attn_grad[3 * sq + so :].reshape(8, vlen)
    grad_w_in = ffn_grad[0:si].reshape(ir, ic)
    grad_w_out = ffn_grad[si : si + sout].reshape(outr, outc)
    grad_b_in = ffn_grad[si + sout :]

    return (
        jnp.stack(outputs),
        jnp.stack(grad_tokens),
        grad_wq,
        grad_wk,
        grad_wv,
        grad_wo,
        grad_w_in,
        grad_w_out,
        grad_vec[0],
        grad_vec[1],
        grad_vec[2],
        grad_vec[3],
        grad_vec[4],
        grad_vec[5],
        grad_vec[6],
        grad_vec[7],
        grad_b_in,
    )


def solution(mesh):
    row_spec = P("dp", ("ctx", "tensor"), None)
    w_rc = P(("dp", "ctx"), "tensor")
    w_cr = P("tensor", ("dp", "ctx"))
    vec = P(("dp", "ctx"))
    return jax.shard_map(
        body,
        mesh=mesh,
        in_specs=(row_spec, row_spec, P("dp"), w_rc, w_rc, w_rc, w_cr, w_rc, w_cr) + (vec,) * 9,
        out_specs=(row_spec, row_spec, w_rc, w_rc, w_rc, w_cr, w_rc, w_cr) + (vec,) * 9,
        check_vma=False,
    )
```

```python
import functools

import jax
import jax.numpy as jnp
from jax import lax
from jax.experimental import pallas as pl
from jax.experimental.pallas import tpu as pltpu
from jax.sharding import PartitionSpec as P

HD = 64
epsilon = 1e-05
masked_value = -1e30
ALL = ("dp", "ctx", "tensor")
SEQ_AXES = ("ctx", "tensor")


def exact_gelu(value):
    return jax.nn.gelu(value, approximate=False)


def mm(left, right):
    return jnp.dot(left, right, preferred_element_type=jnp.float32)


def mm_tn(left, right):
    return lax.dot_general(left, right, (((0,), (0,)), ((), ())), preferred_element_type=jnp.float32)


def mm_nt(left, right):
    return lax.dot_general(left, right, (((1,), (1,)), ((), ())), preferred_element_type=jnp.float32)


def ln_forward(hidden, gain, shift):
    mean = jnp.mean(hidden, axis=-1, keepdims=True)
    centre = hidden - mean
    var = jnp.mean(centre * centre, axis=-1, keepdims=True)
    inv = lax.rsqrt(var + epsilon)
    normed = centre * inv
    return normed * gain + shift, normed, inv


def ln_backward(grad_out, normed, inv, gain):
    d_normed = grad_out * gain
    width = normed.shape[-1]
    mean_d = jnp.sum(d_normed, axis=-1, keepdims=True) / width
    mean_dn = jnp.sum(d_normed * normed, axis=-1, keepdims=True) / width
    d_in = inv * (d_normed - mean_d - normed * mean_dn)
    d_gain = jnp.sum(grad_out * normed, axis=0)
    d_shift = jnp.sum(grad_out, axis=0)
    return d_in, d_gain, d_shift


KEY_BLOCK = 512


def _lane_masks(shape):
    lane = lax.broadcasted_iota(jnp.int32, shape, 1)
    return lane < HD, lane >= HD


def _nt(a, b):
    return lax.dot_general(a, b, (((1,), (1,)), ((), ())), preferred_element_type=jnp.float32)


def _tn(a, b):
    return lax.dot_general(a, b, (((0,), (0,)), ((), ())), preferred_element_type=jnp.float32)


def _attn_fwd_kernel(len_ref, q_ref, k_ref, v_ref, o_ref, lse_ref, s_buf, *, scale):
    length = len_ref[0]
    n_blocks = (length + KEY_BLOCK - 1) // KEY_BLOCK
    q = q_ref[...]
    rows = q.shape[0]
    in_a, in_b = _lane_masks(q.shape)
    zero = jnp.zeros_like(q)
    q_heads = (jnp.where(in_a, q, zero), jnp.where(in_b, q, zero))

    def pass_max(b, ms):
        start = pl.multiple_of(b * KEY_BLOCK, KEY_BLOCK)
        k_blk = k_ref[pl.ds(start, KEY_BLOCK), :]
        out = []
        for j in range(2):
            s = _nt(q_heads[j], k_blk) * scale
            pos = start + lax.broadcasted_iota(jnp.int32, s.shape, 1)
            s = jnp.where(pos < length, s, masked_value)
            s_buf[j, :, pl.ds(start, KEY_BLOCK)] = s
            out.append(jnp.maximum(ms[j], jnp.max(s, axis=1, keepdims=True)))
        return tuple(out)

    init = jnp.full((rows, 1), -jnp.inf, jnp.float32)
    ms = lax.fori_loop(0, n_blocks, pass_max, (init, init))

    def pass_sum(b, ls):
        start = pl.multiple_of(b * KEY_BLOCK, KEY_BLOCK)
        out = []
        for j in range(2):
            e = jnp.exp(s_buf[j, :, pl.ds(start, KEY_BLOCK)] - ms[j])
            s_buf[j, :, pl.ds(start, KEY_BLOCK)] = e
            out.append(ls[j] + jnp.sum(e, axis=1, keepdims=True))
        return tuple(out)

    zeros1 = jnp.zeros((rows, 1), jnp.float32)
    ls = lax.fori_loop(0, n_blocks, pass_sum, (zeros1, zeros1))

    def pass_out(b, acc):
        start = pl.multiple_of(b * KEY_BLOCK, KEY_BLOCK)
        v_blk = v_ref[pl.ds(start, KEY_BLOCK), :]
        vz = jnp.zeros_like(v_blk)
        in_a_v, in_b_v = _lane_masks(v_blk.shape)
        v_heads = (jnp.where(in_a_v, v_blk, vz), jnp.where(in_b_v, v_blk, vz))
        for j in range(2):
            probs = (s_buf[j, :, pl.ds(start, KEY_BLOCK)] / ls[j]).astype(jnp.bfloat16)
            acc = acc + jnp.dot(probs, v_heads[j], preferred_element_type=jnp.float32)
        return acc

    acc = lax.fori_loop(0, n_blocks, pass_out, jnp.zeros(q.shape, jnp.float32))
    o_ref[...] = acc.astype(o_ref.dtype)
    for j in range(2):
        lse_ref[0, j] = ms[j] + jnp.log(ls[j])


def attention_fwd(length, q, k, v, scale):
    rows, width = q.shape
    seq_len = k.shape[0]
    pairs = width // (2 * HD)
    kernel = functools.partial(_attn_fwd_kernel, scale=scale)
    return pl.pallas_call(
        kernel,
        out_shape=(
            jax.ShapeDtypeStruct((rows, width), jnp.bfloat16),
            jax.ShapeDtypeStruct((pairs, 2, rows, 1), jnp.float32),
        ),
        grid_spec=pltpu.PrefetchScalarGridSpec(
            num_scalar_prefetch=1,
            grid=(pairs,),
            in_specs=[
                pl.BlockSpec((rows, 2 * HD), lambda h, n: (0, h)),
                pl.BlockSpec((seq_len, 2 * HD), lambda h, n: (0, h)),
                pl.BlockSpec((seq_len, 2 * HD), lambda h, n: (0, h)),
            ],
            out_specs=[
                pl.BlockSpec((rows, 2 * HD), lambda h, n: (0, h)),
                pl.BlockSpec((1, 2, rows, 1), lambda h, n: (h, 0, 0, 0)),
            ],
            scratch_shapes=[pltpu.VMEM((2, rows, seq_len), jnp.float32)],
        ),
        cost_estimate=pl.CostEstimate(
            flops=8 * pairs * rows * seq_len * 2 * HD,
            transcendentals=2 * pairs * rows * seq_len,
            bytes_accessed=2 * (2 * q.size + k.size + v.size),
        ),
    )(length.reshape(1), q, k, v)


def _attn_bwd_kernel(len_ref, q_ref, k_ref, v_ref, do_ref, lse_ref, dq_ref, dk_ref, dv_ref, p_buf, dp_buf, *, scale):
    length = len_ref[0]
    n_blocks = (length + KEY_BLOCK - 1) // KEY_BLOCK
    total_blocks = k_ref.shape[0] // KEY_BLOCK
    q = q_ref[...]
    do = do_ref[...]
    rows = q.shape[0]
    in_a, in_b = _lane_masks(q.shape)
    zero = jnp.zeros_like(q)
    q_heads = (jnp.where(in_a, q, zero), jnp.where(in_b, q, zero))
    do_heads = (jnp.where(in_a, do, zero), jnp.where(in_b, do, zero))
    lses = (lse_ref[0, 0], lse_ref[0, 1])

    def pass_one(b, centres):
        start = pl.multiple_of(b * KEY_BLOCK, KEY_BLOCK)
        k_blk = k_ref[pl.ds(start, KEY_BLOCK), :]
        v_blk = v_ref[pl.ds(start, KEY_BLOCK), :]
        out = []
        for j in range(2):
            s = _nt(q_heads[j], k_blk) * scale
            pos = start + lax.broadcasted_iota(jnp.int32, s.shape, 1)
            s = jnp.where(pos < length, s, masked_value)
            p = jnp.exp(s - lses[j])
            dp = _nt(do_heads[j], v_blk)
            p_buf[j, :, pl.ds(start, KEY_BLOCK)] = p
            dp_buf[j, :, pl.ds(start, KEY_BLOCK)] = dp
            out.append(centres[j] + jnp.sum(p * dp, axis=1, keepdims=True))
        return tuple(out)

    zeros1 = jnp.zeros((rows, 1), jnp.float32)
    centres = lax.fori_loop(0, n_blocks, pass_one, (zeros1, zeros1))

    def pass_two(b, dq):
        start = pl.multiple_of(b * KEY_BLOCK, KEY_BLOCK)
        k_blk = k_ref[pl.ds(start, KEY_BLOCK), :]
        kz = jnp.zeros_like(k_blk)
        in_a_k, in_b_k = _lane_masks(k_blk.shape)
        k_heads = (jnp.where(in_a_k, k_blk, kz), jnp.where(in_b_k, k_blk, kz))
        dk = jnp.zeros(k_blk.shape, jnp.float32)
        dv = jnp.zeros(k_blk.shape, jnp.float32)
        for j in range(2):
            p = p_buf[j, :, pl.ds(start, KEY_BLOCK)]
            dp = dp_buf[j, :, pl.ds(start, KEY_BLOCK)]
            pos = start + lax.broadcasted_iota(jnp.int32, p.shape, 1)
            ds = jnp.where(pos < length, p * (dp - centres[j]), 0.0).astype(jnp.bfloat16)
            dk = dk + _tn(ds, q_heads[j])
            dv = dv + _tn(p.astype(jnp.bfloat16), do_heads[j])
            dq = dq + jnp.dot(ds, k_heads[j], preferred_element_type=jnp.float32)
        dk_ref[pl.ds(start, KEY_BLOCK), :] = (dk * scale).astype(dk_ref.dtype)
        dv_ref[pl.ds(start, KEY_BLOCK), :] = dv.astype(dv_ref.dtype)
        return dq

    dq = lax.fori_loop(0, n_blocks, pass_two, jnp.zeros(q.shape, jnp.float32))
    dq_ref[...] = (dq * scale).astype(dq_ref.dtype)

    def pass_zero(b, carry):
        start = pl.multiple_of(b * KEY_BLOCK, KEY_BLOCK)
        dk_ref[pl.ds(start, KEY_BLOCK), :] = jnp.zeros((KEY_BLOCK, q.shape[1]), dk_ref.dtype)
        dv_ref[pl.ds(start, KEY_BLOCK), :] = jnp.zeros((KEY_BLOCK, q.shape[1]), dv_ref.dtype)
        return carry

    lax.fori_loop(n_blocks, total_blocks, pass_zero, 0)


def attention_bwd(length, q, k, v, do, lse, scale):
    rows, width = q.shape
    seq_len = k.shape[0]
    pairs = width // (2 * HD)
    kernel = functools.partial(_attn_bwd_kernel, scale=scale)
    return pl.pallas_call(
        kernel,
        out_shape=(
            jax.ShapeDtypeStruct((rows, width), jnp.bfloat16),
            jax.ShapeDtypeStruct((seq_len, width), jnp.bfloat16),
            jax.ShapeDtypeStruct((seq_len, width), jnp.bfloat16),
        ),
        grid_spec=pltpu.PrefetchScalarGridSpec(
            num_scalar_prefetch=1,
            grid=(pairs,),
            in_specs=[
                pl.BlockSpec((rows, 2 * HD), lambda h, n: (0, h)),
                pl.BlockSpec((seq_len, 2 * HD), lambda h, n: (0, h)),
                pl.BlockSpec((seq_len, 2 * HD), lambda h, n: (0, h)),
                pl.BlockSpec((rows, 2 * HD), lambda h, n: (0, h)),
                pl.BlockSpec((1, 2, rows, 1), lambda h, n: (h, 0, 0, 0)),
            ],
            out_specs=[
                pl.BlockSpec((rows, 2 * HD), lambda h, n: (0, h)),
                pl.BlockSpec((seq_len, 2 * HD), lambda h, n: (0, h)),
                pl.BlockSpec((seq_len, 2 * HD), lambda h, n: (0, h)),
            ],
            scratch_shapes=[pltpu.VMEM((2, rows, seq_len), jnp.float32), pltpu.VMEM((2, rows, seq_len), jnp.float32)],
        ),
        cost_estimate=pl.CostEstimate(
            flops=20 * pairs * rows * seq_len * 2 * HD,
            transcendentals=2 * pairs * rows * seq_len,
            bytes_accessed=2 * (3 * q.size + 4 * k.size),
        ),
    )(length.reshape(1), q, k, v, do, lse)


def pad_cols(x, multiple):
    cols = x.shape[1]
    padded = -(-cols // multiple) * multiple
    return jnp.pad(x, ((0, 0), (0, padded - cols)))


def gather_rows(pieces, replicated, nt):
    local = jnp.concatenate(pieces + [replicated], axis=1)
    width = local.shape[1]
    staged = lax.all_gather(local, "tensor", axis=1, tiled=True).reshape(local.shape[0], nt, width)
    parts, at = [], 0
    for p in pieces:
        parts.append(staged[:, :, at : at + p.shape[1]].reshape(local.shape[0], nt * p.shape[1]))
        at += p.shape[1]
    parts.append(staged[:, 0, at:])
    joined = jnp.concatenate(parts, axis=1)
    full = lax.all_gather(joined, ("dp", "ctx"), axis=0, tiled=True)
    out, at = [], 0
    for p in pieces:
        out.append(full[:, at : at + nt * p.shape[1]])
        at += nt * p.shape[1]
    out.append(full[:, at:])
    return out


def reduce_rows(pieces, replicated, nt):
    local = jnp.concatenate(pieces + [replicated], axis=1).astype(jnp.bfloat16)
    width = local.shape[1]
    staged = lax.psum_scatter(pad_cols(local, 128), ("dp", "ctx"), scatter_dimension=0, tiled=True)
    rb = staged.shape[0]
    parts, at = [], 0
    for p in pieces:
        c = p.shape[1] // nt
        parts.append(staged[:, at : at + p.shape[1]].reshape(rb, nt, c))
        at += p.shape[1]
    rep = staged[:, at:width]
    parts.append(jnp.broadcast_to(rep[:, None, :], (rb, nt, rep.shape[1])))
    slots = jnp.concatenate(parts, axis=2)
    slot_width = slots.shape[2]
    padded = -(-slot_width // 128) * 128
    slots = jnp.pad(slots, ((0, 0), (0, 0), (0, padded - slot_width))).transpose(1, 0, 2)
    own = lax.psum_scatter(slots, "tensor", scatter_dimension=0, tiled=True)[0].astype(jnp.float32)
    out, at = [], 0
    for p in pieces:
        c = p.shape[1] // nt
        out.append(own[:, at : at + c])
        at += c
    out.append(own[:, at : at + rep.shape[1]])
    return out


def body(
    tokens,
    cotangent,
    lengths,
    w_query,
    w_key,
    w_value,
    w_output,
    w_in,
    w_out,
    bias_query,
    bias_value,
    bias_output,
    gain_first,
    shift_first,
    gain_second,
    shift_second,
    bias_out,
    bias_in,
):
    seqs, local_rows, width = tokens.shape
    ctx_rank = lax.axis_index("ctx")
    tensor_rank = lax.axis_index("tensor")
    nt = lax.axis_size("tensor")
    chunk = ctx_rank * nt + tensor_rank
    seq_len = local_rows * lax.axis_size("ctx") * nt
    scale = HD ** (-0.5)
    rb = w_query.shape[0]
    hidden = w_in.shape[1] * nt

    attn_vec = jnp.stack([bias_query, bias_value, bias_output, gain_first, shift_first], axis=1)
    wq, wk, wv, wo_t, attn_vec = gather_rows([w_query, w_key, w_value, w_output.T], attn_vec, nt)
    ffn_vec = jnp.concatenate(
        [jnp.stack([gain_second, shift_second, bias_out], axis=1), bias_in.reshape(rb, -1)], axis=1
    )
    w_in_f, w_out_t, ffn_vec = gather_rows([w_in, w_out.T], ffn_vec, nt)
    attn_vec = attn_vec.astype(jnp.float32)
    ffn_vec = ffn_vec.astype(jnp.float32)
    b_q, b_v, b_o, g1, s1 = [attn_vec[:, i] for i in range(5)]
    g2, s2, b_out = [ffn_vec[:, i] for i in range(3)]
    b_in = ffn_vec[:, 3:].reshape(hidden)

    row_positions = chunk * local_rows + jnp.arange(local_rows, dtype=jnp.int32)

    fwd = []
    for s in range(seqs):
        x_own = tokens[s]
        length = lengths[s]
        x_all = lax.all_gather(x_own, SEQ_AXES, axis=0, tiled=True)
        q = (mm(x_own, wq) + b_q).astype(jnp.bfloat16)
        k = mm(x_all, wk).astype(jnp.bfloat16)
        v = (mm(x_all, wv) + b_v).astype(jnp.bfloat16)
        attended, lse = attention_fwd(length, q, k, v, scale)
        first_in = x_own.astype(jnp.float32) + (mm_nt(attended, wo_t) + b_o)
        first, normed1, inv1 = ln_forward(first_in, g1, s1)
        fwd.append(dict(x_all=x_all, q=q, k=k, v=v, lse=lse, attended=attended, first=first,
                        normed1=normed1, inv1=inv1, length=length))

    outputs = []
    for s in range(seqs):
        f = fwd[s]
        first_low = f["first"].astype(jnp.bfloat16)
        hidden_pre = mm(first_low, w_in_f) + b_in
        activated = exact_gelu(hidden_pre).astype(jnp.bfloat16)
        second_in = f["first"] + mm_nt(activated, w_out_t) + b_out
        result, normed2, inv2 = ln_forward(second_in, g2, s2)
        outputs.append(result.astype(jnp.bfloat16))
        f.update(first_low=first_low, hidden_pre=hidden_pre, activated=activated, normed2=normed2, inv2=inv2)

    g_w_in = jnp.zeros((width, hidden), jnp.float32)
    g_w_out_t = jnp.zeros((width, hidden), jnp.float32)
    g_b_in = jnp.zeros((hidden,), jnp.float32)
    g_vec = [jnp.zeros((width,), jnp.float32) for _ in range(8)]
    for s in range(seqs):
        f = fwd[s]
        row_valid = (row_positions < f["length"]).astype(jnp.float32)
        upstream = cotangent[s].astype(jnp.float32) * row_valid[:, None]
        d_second, d_g2, d_s2 = ln_backward(upstream, f["normed2"], f["inv2"], g2)
        d_ffn = d_second.astype(jnp.bfloat16)
        g_w_out_t = g_w_out_t + mm_tn(d_ffn, f["activated"])
        d_act = mm(d_ffn, w_out_t)
        _, gelu_pull = jax.vjp(exact_gelu, f["hidden_pre"])
        d_hidden = gelu_pull(d_act)[0].astype(jnp.bfloat16)
        g_w_in = g_w_in + mm_tn(f["first_low"], d_hidden)
        g_b_in = g_b_in + jnp.sum(d_hidden.astype(jnp.float32), axis=0)
        d_first = d_second + mm_nt(d_hidden, w_in_f)
        d_first_in, d_g1, d_s1 = ln_backward(d_first, f["normed1"], f["inv1"], g1)
        g_vec[5] = g_vec[5] + d_g2
        g_vec[6] = g_vec[6] + d_s2
        g_vec[7] = g_vec[7] + jnp.sum(d_second, axis=0)
        g_vec[3] = g_vec[3] + d_g1
        g_vec[4] = g_vec[4] + d_s1
        g_vec[2] = g_vec[2] + jnp.sum(d_first_in, axis=0)
        f.update(d_first_in=d_first_in)

    ffn_rep = jnp.concatenate([jnp.stack([g_vec[5], g_vec[6], g_vec[7]], axis=1), g_b_in.reshape(width, -1)], axis=1)
    grad_w_in, grad_w_out_t, ffn_rep_out = reduce_rows([g_w_in, g_w_out_t], ffn_rep, nt)

    g_wq = jnp.zeros((width, width), jnp.float32)
    g_wk = jnp.zeros((width, width), jnp.float32)
    g_wv = jnp.zeros((width, width), jnp.float32)
    g_wo_t = jnp.zeros((width, width), jnp.float32)
    grad_tokens = []
    for s in range(seqs):
        f = fwd[s]
        d_branch = f["d_first_in"].astype(jnp.bfloat16)
        g_wo_t = g_wo_t + mm_tn(d_branch, f["attended"])
        d_att = mm(d_branch, wo_t).astype(jnp.bfloat16)
        dq, dk, dv = attention_bwd(f["length"], f["q"], f["k"], f["v"], d_att, f["lse"], scale)
        g_wq = g_wq + mm_tn(tokens[s], dq)
        g_wk = g_wk + mm_tn(f["x_all"], dk)
        g_wv = g_wv + mm_tn(f["x_all"], dv)
        g_vec[0] = g_vec[0] + jnp.sum(dq.astype(jnp.float32), axis=0)
        g_vec[1] = g_vec[1] + jnp.sum(dv.astype(jnp.float32), axis=0)
        dx_kv = (mm_nt(dk, wk) + mm_nt(dv, wv)).astype(jnp.bfloat16)
        dx_kv_own = lax.psum_scatter(dx_kv, SEQ_AXES, scatter_dimension=0, tiled=True).astype(jnp.float32)
        d_tok = f["d_first_in"] + mm_nt(dq, wq) + dx_kv_own
        grad_tokens.append(d_tok.astype(jnp.bfloat16))

    attn_rep = jnp.stack(g_vec[0:5], axis=1)
    grad_wq, grad_wk, grad_wv, grad_wo_t, attn_rep_out = reduce_rows([g_wq, g_wk, g_wv, g_wo_t], attn_rep, nt)

    return (
        jnp.stack(outputs),
        jnp.stack(grad_tokens),
        grad_wq,
        grad_wk,
        grad_wv,
        grad_wo_t.T,
        grad_w_in,
        grad_w_out_t.T,
        attn_rep_out[:, 0],
        attn_rep_out[:, 1],
        attn_rep_out[:, 2],
        attn_rep_out[:, 3],
        attn_rep_out[:, 4],
        ffn_rep_out[:, 0],
        ffn_rep_out[:, 1],
        ffn_rep_out[:, 2],
        ffn_rep_out[:, 3:].reshape(-1),
    )


def solution(mesh):
    row_spec = P("dp", ("ctx", "tensor"), None)
    w_rc = P(("dp", "ctx"), "tensor")
    w_cr = P("tensor", ("dp", "ctx"))
    vec = P(("dp", "ctx"))
    return jax.shard_map(
        body,
        mesh=mesh,
        in_specs=(row_spec, row_spec, P("dp"), w_rc, w_rc, w_rc, w_cr, w_rc, w_cr) + (vec,) * 9,
        out_specs=(row_spec, row_spec, w_rc, w_rc, w_rc, w_cr, w_rc, w_cr) + (vec,) * 9,
        check_vma=False,
    )
```

```python
import functools

import jax
import jax.numpy as jnp
from jax import lax
from jax.experimental import pallas as pl
from jax.experimental.pallas import tpu as pltpu
from jax.sharding import PartitionSpec as P

HD = 64
epsilon = 1e-05
masked_value = -1e30
ALL = ("dp", "ctx", "tensor")
SEQ_AXES = ("ctx", "tensor")


def exact_gelu(value):
    return jax.nn.gelu(value, approximate=False)


def mm(left, right):
    return jnp.dot(left, right, preferred_element_type=jnp.float32)


def mm_tn(left, right):
    return lax.dot_general(left, right, (((0,), (0,)), ((), ())), preferred_element_type=jnp.float32)


def mm_nt(left, right):
    return lax.dot_general(left, right, (((1,), (1,)), ((), ())), preferred_element_type=jnp.float32)


def ln_forward(hidden, gain, shift):
    mean = jnp.mean(hidden, axis=-1, keepdims=True)
    centre = hidden - mean
    var = jnp.mean(centre * centre, axis=-1, keepdims=True)
    inv = lax.rsqrt(var + epsilon)
    normed = centre * inv
    return normed * gain + shift, normed, inv


def ln_backward(grad_out, normed, inv, gain):
    d_normed = grad_out * gain
    width = normed.shape[-1]
    mean_d = jnp.sum(d_normed, axis=-1, keepdims=True) / width
    mean_dn = jnp.sum(d_normed * normed, axis=-1, keepdims=True) / width
    d_in = inv * (d_normed - mean_d - normed * mean_dn)
    d_gain = jnp.sum(grad_out * normed, axis=0)
    d_shift = jnp.sum(grad_out, axis=0)
    return d_in, d_gain, d_shift


KEY_BLOCK = 512


def _lane_masks(shape):
    lane = lax.broadcasted_iota(jnp.int32, shape, 1)
    return lane < HD, lane >= HD


def _nt(a, b):
    return lax.dot_general(a, b, (((1,), (1,)), ((), ())), preferred_element_type=jnp.float32)


def _tn(a, b):
    return lax.dot_general(a, b, (((0,), (0,)), ((), ())), preferred_element_type=jnp.float32)


def _attn_fwd_kernel(len_ref, q_ref, k_ref, v_ref, o_ref, lse_ref, s_buf, *, scale):
    length = len_ref[0]
    n_blocks = (length + KEY_BLOCK - 1) // KEY_BLOCK
    q = q_ref[...]
    rows = q.shape[0]
    in_a, in_b = _lane_masks(q.shape)
    zero = jnp.zeros_like(q)
    q_heads = (jnp.where(in_a, q, zero), jnp.where(in_b, q, zero))

    def pass_max(b, ms):
        start = pl.multiple_of(b * KEY_BLOCK, KEY_BLOCK)
        k_blk = k_ref[pl.ds(start, KEY_BLOCK), :]
        out = []
        for j in range(2):
            s = _nt(q_heads[j], k_blk) * scale
            pos = start + lax.broadcasted_iota(jnp.int32, s.shape, 1)
            s = jnp.where(pos < length, s, masked_value)
            s_buf[j, :, pl.ds(start, KEY_BLOCK)] = s
            out.append(jnp.maximum(ms[j], jnp.max(s, axis=1, keepdims=True)))
        return tuple(out)

    init = jnp.full((rows, 1), -jnp.inf, jnp.float32)
    ms = lax.fori_loop(0, n_blocks, pass_max, (init, init))

    def pass_sum(b, ls):
        start = pl.multiple_of(b * KEY_BLOCK, KEY_BLOCK)
        out = []
        for j in range(2):
            e = jnp.exp(s_buf[j, :, pl.ds(start, KEY_BLOCK)] - ms[j])
            s_buf[j, :, pl.ds(start, KEY_BLOCK)] = e
            out.append(ls[j] + jnp.sum(e, axis=1, keepdims=True))
        return tuple(out)

    zeros1 = jnp.zeros((rows, 1), jnp.float32)
    ls = lax.fori_loop(0, n_blocks, pass_sum, (zeros1, zeros1))

    def pass_out(b, acc):
        start = pl.multiple_of(b * KEY_BLOCK, KEY_BLOCK)
        v_blk = v_ref[pl.ds(start, KEY_BLOCK), :]
        vz = jnp.zeros_like(v_blk)
        in_a_v, in_b_v = _lane_masks(v_blk.shape)
        v_heads = (jnp.where(in_a_v, v_blk, vz), jnp.where(in_b_v, v_blk, vz))
        for j in range(2):
            probs = (s_buf[j, :, pl.ds(start, KEY_BLOCK)] / ls[j]).astype(jnp.bfloat16)
            acc = acc + jnp.dot(probs, v_heads[j], preferred_element_type=jnp.float32)
        return acc

    acc = lax.fori_loop(0, n_blocks, pass_out, jnp.zeros(q.shape, jnp.float32))
    o_ref[...] = acc.astype(o_ref.dtype)
    for j in range(2):
        lse_ref[0, j] = ms[j] + jnp.log(ls[j])


def attention_fwd(length, q, k, v, scale):
    rows, width = q.shape
    seq_len = k.shape[0]
    pairs = width // (2 * HD)
    kernel = functools.partial(_attn_fwd_kernel, scale=scale)
    return pl.pallas_call(
        kernel,
        out_shape=(
            jax.ShapeDtypeStruct((rows, width), jnp.bfloat16),
            jax.ShapeDtypeStruct((pairs, 2, rows, 1), jnp.float32),
        ),
        grid_spec=pltpu.PrefetchScalarGridSpec(
            num_scalar_prefetch=1,
            grid=(pairs,),
            in_specs=[
                pl.BlockSpec((rows, 2 * HD), lambda h, n: (0, h)),
                pl.BlockSpec((seq_len, 2 * HD), lambda h, n: (0, h)),
                pl.BlockSpec((seq_len, 2 * HD), lambda h, n: (0, h)),
            ],
            out_specs=[
                pl.BlockSpec((rows, 2 * HD), lambda h, n: (0, h)),
                pl.BlockSpec((1, 2, rows, 1), lambda h, n: (h, 0, 0, 0)),
            ],
            scratch_shapes=[pltpu.VMEM((2, rows, seq_len), jnp.float32)],
        ),
        cost_estimate=pl.CostEstimate(
            flops=8 * pairs * rows * seq_len * 2 * HD,
            transcendentals=2 * pairs * rows * seq_len,
            bytes_accessed=2 * (2 * q.size + k.size + v.size),
        ),
    )(length.reshape(1), q, k, v)


def _attn_bwd_kernel(len_ref, q_ref, k_ref, v_ref, do_ref, lse_ref, dq_ref, dk_ref, dv_ref, p_buf, dp_buf, *, scale):
    length = len_ref[0]
    n_blocks = (length + KEY_BLOCK - 1) // KEY_BLOCK
    total_blocks = k_ref.shape[0] // KEY_BLOCK
    q = q_ref[...]
    do = do_ref[...]
    rows = q.shape[0]
    in_a, in_b = _lane_masks(q.shape)
    zero = jnp.zeros_like(q)
    q_heads = (jnp.where(in_a, q, zero), jnp.where(in_b, q, zero))
    do_heads = (jnp.where(in_a, do, zero), jnp.where(in_b, do, zero))
    lses = (lse_ref[0, 0], lse_ref[0, 1])

    def pass_one(b, centres):
        start = pl.multiple_of(b * KEY_BLOCK, KEY_BLOCK)
        k_blk = k_ref[pl.ds(start, KEY_BLOCK), :]
        v_blk = v_ref[pl.ds(start, KEY_BLOCK), :]
        out = []
        for j in range(2):
            s = _nt(q_heads[j], k_blk) * scale
            pos = start + lax.broadcasted_iota(jnp.int32, s.shape, 1)
            s = jnp.where(pos < length, s, masked_value)
            p = jnp.exp(s - lses[j])
            dp = _nt(do_heads[j], v_blk)
            p_buf[j, :, pl.ds(start, KEY_BLOCK)] = p
            dp_buf[j, :, pl.ds(start, KEY_BLOCK)] = dp
            out.append(centres[j] + jnp.sum(p * dp, axis=1, keepdims=True))
        return tuple(out)

    zeros1 = jnp.zeros((rows, 1), jnp.float32)
    centres = lax.fori_loop(0, n_blocks, pass_one, (zeros1, zeros1))

    def pass_two(b, dq):
        start = pl.multiple_of(b * KEY_BLOCK, KEY_BLOCK)
        k_blk = k_ref[pl.ds(start, KEY_BLOCK), :]
        kz = jnp.zeros_like(k_blk)
        in_a_k, in_b_k = _lane_masks(k_blk.shape)
        k_heads = (jnp.where(in_a_k, k_blk, kz), jnp.where(in_b_k, k_blk, kz))
        dk = jnp.zeros(k_blk.shape, jnp.float32)
        dv = jnp.zeros(k_blk.shape, jnp.float32)
        for j in range(2):
            p = p_buf[j, :, pl.ds(start, KEY_BLOCK)]
            dp = dp_buf[j, :, pl.ds(start, KEY_BLOCK)]
            pos = start + lax.broadcasted_iota(jnp.int32, p.shape, 1)
            ds = jnp.where(pos < length, p * (dp - centres[j]), 0.0).astype(jnp.bfloat16)
            dk = dk + _tn(ds, q_heads[j])
            dv = dv + _tn(p.astype(jnp.bfloat16), do_heads[j])
            dq = dq + jnp.dot(ds, k_heads[j], preferred_element_type=jnp.float32)
        dk_ref[pl.ds(start, KEY_BLOCK), :] = (dk * scale).astype(dk_ref.dtype)
        dv_ref[pl.ds(start, KEY_BLOCK), :] = dv.astype(dv_ref.dtype)
        return dq

    dq = lax.fori_loop(0, n_blocks, pass_two, jnp.zeros(q.shape, jnp.float32))
    dq_ref[...] = (dq * scale).astype(dq_ref.dtype)

    def pass_zero(b, carry):
        start = pl.multiple_of(b * KEY_BLOCK, KEY_BLOCK)
        dk_ref[pl.ds(start, KEY_BLOCK), :] = jnp.zeros((KEY_BLOCK, q.shape[1]), dk_ref.dtype)
        dv_ref[pl.ds(start, KEY_BLOCK), :] = jnp.zeros((KEY_BLOCK, q.shape[1]), dv_ref.dtype)
        return carry

    lax.fori_loop(n_blocks, total_blocks, pass_zero, 0)


def attention_bwd(length, q, k, v, do, lse, scale):
    rows, width = q.shape
    seq_len = k.shape[0]
    pairs = width // (2 * HD)
    kernel = functools.partial(_attn_bwd_kernel, scale=scale)
    return pl.pallas_call(
        kernel,
        out_shape=(
            jax.ShapeDtypeStruct((rows, width), jnp.bfloat16),
            jax.ShapeDtypeStruct((seq_len, width), jnp.bfloat16),
            jax.ShapeDtypeStruct((seq_len, width), jnp.bfloat16),
        ),
        grid_spec=pltpu.PrefetchScalarGridSpec(
            num_scalar_prefetch=1,
            grid=(pairs,),
            in_specs=[
                pl.BlockSpec((rows, 2 * HD), lambda h, n: (0, h)),
                pl.BlockSpec((seq_len, 2 * HD), lambda h, n: (0, h)),
                pl.BlockSpec((seq_len, 2 * HD), lambda h, n: (0, h)),
                pl.BlockSpec((rows, 2 * HD), lambda h, n: (0, h)),
                pl.BlockSpec((1, 2, rows, 1), lambda h, n: (h, 0, 0, 0)),
            ],
            out_specs=[
                pl.BlockSpec((rows, 2 * HD), lambda h, n: (0, h)),
                pl.BlockSpec((seq_len, 2 * HD), lambda h, n: (0, h)),
                pl.BlockSpec((seq_len, 2 * HD), lambda h, n: (0, h)),
            ],
            scratch_shapes=[pltpu.VMEM((2, rows, seq_len), jnp.float32), pltpu.VMEM((2, rows, seq_len), jnp.float32)],
        ),
        cost_estimate=pl.CostEstimate(
            flops=20 * pairs * rows * seq_len * 2 * HD,
            transcendentals=2 * pairs * rows * seq_len,
            bytes_accessed=2 * (3 * q.size + 4 * k.size),
        ),
    )(length.reshape(1), q, k, v, do, lse)


def pad_cols(x, multiple):
    cols = x.shape[1]
    padded = -(-cols // multiple) * multiple
    return jnp.pad(x, ((0, 0), (0, padded - cols)))


def gather_rows(pieces, replicated, nt):
    local = jnp.concatenate(pieces + [replicated], axis=1)
    width = local.shape[1]
    staged = lax.all_gather(local, "tensor", axis=1, tiled=True).reshape(local.shape[0], nt, width)
    parts, at = [], 0
    for p in pieces:
        parts.append(staged[:, :, at : at + p.shape[1]].reshape(local.shape[0], nt * p.shape[1]))
        at += p.shape[1]
    parts.append(staged[:, 0, at:])
    joined = jnp.concatenate(parts, axis=1)
    full = lax.all_gather(joined, ("dp", "ctx"), axis=0, tiled=True)
    out, at = [], 0
    for p in pieces:
        out.append(full[:, at : at + nt * p.shape[1]])
        at += nt * p.shape[1]
    out.append(full[:, at:])
    return out


def reduce_rows(pieces, replicated, nt, gate=None):
    local = jnp.concatenate(pieces + [replicated], axis=1).astype(jnp.bfloat16)
    width = local.shape[1]
    local = pad_cols(local, 128)
    if gate is not None:
        local = local + (gate[0, 0] * 0).astype(local.dtype)
    staged = lax.psum_scatter(local, ("dp", "ctx"), scatter_dimension=0, tiled=True)
    rb = staged.shape[0]
    parts, at = [], 0
    for p in pieces:
        c = p.shape[1] // nt
        parts.append(staged[:, at : at + p.shape[1]].reshape(rb, nt, c))
        at += p.shape[1]
    rep = staged[:, at:width]
    parts.append(jnp.broadcast_to(rep[:, None, :], (rb, nt, rep.shape[1])))
    slots = jnp.concatenate(parts, axis=2)
    slot_width = slots.shape[2]
    padded = -(-slot_width // 128) * 128
    slots = jnp.pad(slots, ((0, 0), (0, 0), (0, padded - slot_width))).transpose(1, 0, 2)
    own = lax.psum_scatter(slots, "tensor", scatter_dimension=0, tiled=True)[0].astype(jnp.float32)
    out, at = [], 0
    for p in pieces:
        c = p.shape[1] // nt
        out.append(own[:, at : at + c])
        at += c
    out.append(own[:, at : at + rep.shape[1]])
    return out


def body(
    tokens,
    cotangent,
    lengths,
    w_query,
    w_key,
    w_value,
    w_output,
    w_in,
    w_out,
    bias_query,
    bias_value,
    bias_output,
    gain_first,
    shift_first,
    gain_second,
    shift_second,
    bias_out,
    bias_in,
):
    seqs, local_rows, width = tokens.shape
    ctx_rank = lax.axis_index("ctx")
    tensor_rank = lax.axis_index("tensor")
    nt = lax.axis_size("tensor")
    chunk = ctx_rank * nt + tensor_rank
    seq_len = local_rows * lax.axis_size("ctx") * nt
    scale = HD ** (-0.5)
    rb = w_query.shape[0]
    hidden = w_in.shape[1] * nt

    attn_vec = jnp.stack([bias_query, bias_value, bias_output, gain_first, shift_first], axis=1)
    wq, wk, wv, wo_t, attn_vec = gather_rows([w_query, w_key, w_value, w_output.T], attn_vec, nt)
    ffn_vec = jnp.concatenate(
        [jnp.stack([gain_second, shift_second, bias_out], axis=1), bias_in.reshape(rb, -1)], axis=1
    )
    w_in_f, w_out_t, ffn_vec = gather_rows([w_in, w_out.T], ffn_vec, nt)
    attn_vec = attn_vec.astype(jnp.float32)
    ffn_vec = ffn_vec.astype(jnp.float32)
    b_q, b_v, b_o, g1, s1 = [attn_vec[:, i] for i in range(5)]
    g2, s2, b_out = [ffn_vec[:, i] for i in range(3)]
    b_in = ffn_vec[:, 3:].reshape(hidden)

    row_positions = chunk * local_rows + jnp.arange(local_rows, dtype=jnp.int32)

    fwd = []
    for s in range(seqs):
        x_own = tokens[s]
        length = lengths[s]
        x_all = lax.all_gather(x_own, SEQ_AXES, axis=0, tiled=True)
        q = (mm(x_own, wq) + b_q).astype(jnp.bfloat16)
        k = mm(x_all, wk).astype(jnp.bfloat16)
        v = (mm(x_all, wv) + b_v).astype(jnp.bfloat16)
        attended, lse = attention_fwd(length, q, k, v, scale)
        first_in = x_own.astype(jnp.float32) + (mm_nt(attended, wo_t) + b_o)
        first, normed1, inv1 = ln_forward(first_in, g1, s1)
        fwd.append(dict(x_all=x_all, q=q, k=k, v=v, lse=lse, attended=attended, first=first,
                        normed1=normed1, inv1=inv1, length=length))

    outputs = []
    for s in range(seqs):
        f = fwd[s]
        first_low = f["first"].astype(jnp.bfloat16)
        hidden_pre = mm(first_low, w_in_f) + b_in
        activated = exact_gelu(hidden_pre).astype(jnp.bfloat16)
        second_in = f["first"] + mm_nt(activated, w_out_t) + b_out
        result, normed2, inv2 = ln_forward(second_in, g2, s2)
        outputs.append(result.astype(jnp.bfloat16))
        f.update(first_low=first_low, hidden_pre=hidden_pre, activated=activated, normed2=normed2, inv2=inv2)

    g_w_in = jnp.zeros((width, hidden), jnp.float32)
    g_w_out_t = jnp.zeros((width, hidden), jnp.float32)
    g_b_in = jnp.zeros((hidden,), jnp.float32)
    g_vec = [jnp.zeros((width,), jnp.float32) for _ in range(8)]
    for s in range(seqs):
        f = fwd[s]
        row_valid = (row_positions < f["length"]).astype(jnp.float32)
        upstream = cotangent[s].astype(jnp.float32) * row_valid[:, None]
        d_second, d_g2, d_s2 = ln_backward(upstream, f["normed2"], f["inv2"], g2)
        d_ffn = d_second.astype(jnp.bfloat16)
        g_w_out_t = g_w_out_t + mm_tn(d_ffn, f["activated"])
        d_act = mm(d_ffn, w_out_t)
        _, gelu_pull = jax.vjp(exact_gelu, f["hidden_pre"])
        d_hidden = gelu_pull(d_act)[0].astype(jnp.bfloat16)
        g_w_in = g_w_in + mm_tn(f["first_low"], d_hidden)
        g_b_in = g_b_in + jnp.sum(d_hidden.astype(jnp.float32), axis=0)
        d_first = d_second + mm_nt(d_hidden, w_in_f)
        d_first_in, d_g1, d_s1 = ln_backward(d_first, f["normed1"], f["inv1"], g1)
        g_vec[5] = g_vec[5] + d_g2
        g_vec[6] = g_vec[6] + d_s2
        g_vec[7] = g_vec[7] + jnp.sum(d_second, axis=0)
        g_vec[3] = g_vec[3] + d_g1
        g_vec[4] = g_vec[4] + d_s1
        g_vec[2] = g_vec[2] + jnp.sum(d_first_in, axis=0)
        f.update(d_first_in=d_first_in)

    ffn_rep = jnp.concatenate([jnp.stack([g_vec[5], g_vec[6], g_vec[7]], axis=1), g_b_in.reshape(width, -1)], axis=1)

    g_wq = jnp.zeros((width, width), jnp.float32)
    g_wk = jnp.zeros((width, width), jnp.float32)
    g_wv = jnp.zeros((width, width), jnp.float32)
    g_wo_t = jnp.zeros((width, width), jnp.float32)
    grad_tokens = []
    dx_gate = []
    for s in range(seqs):
        f = fwd[s]
        d_branch = f["d_first_in"].astype(jnp.bfloat16)
        g_wo_t = g_wo_t + mm_tn(d_branch, f["attended"])
        d_att = mm(d_branch, wo_t).astype(jnp.bfloat16)
        dq, dk, dv = attention_bwd(f["length"], f["q"], f["k"], f["v"], d_att, f["lse"], scale)
        g_wq = g_wq + mm_tn(tokens[s], dq)
        g_wk = g_wk + mm_tn(f["x_all"], dk)
        g_wv = g_wv + mm_tn(f["x_all"], dv)
        g_vec[0] = g_vec[0] + jnp.sum(dq.astype(jnp.float32), axis=0)
        g_vec[1] = g_vec[1] + jnp.sum(dv.astype(jnp.float32), axis=0)
        dx_kv = (mm_nt(dk, wk) + mm_nt(dv, wv)).astype(jnp.bfloat16)
        dx_kv_own = lax.psum_scatter(dx_kv, SEQ_AXES, scatter_dimension=0, tiled=True).astype(jnp.float32)
        dx_gate.append(dx_kv_own[0:1, 0:1])
        d_tok = f["d_first_in"] + mm_nt(dq, wq) + dx_kv_own
        grad_tokens.append(d_tok.astype(jnp.bfloat16))

    grad_w_in, grad_w_out_t, ffn_rep_out = reduce_rows([g_w_in, g_w_out_t], ffn_rep, nt, gate=sum(dx_gate))
    attn_rep = jnp.stack(g_vec[0:5], axis=1)
    grad_wq, grad_wk, grad_wv, grad_wo_t, attn_rep_out = reduce_rows(
        [g_wq, g_wk, g_wv, g_wo_t], attn_rep, nt, gate=ffn_rep_out
    )

    return (
        jnp.stack(outputs),
        jnp.stack(grad_tokens),
        grad_wq,
        grad_wk,
        grad_wv,
        grad_wo_t.T,
        grad_w_in,
        grad_w_out_t.T,
        attn_rep_out[:, 0],
        attn_rep_out[:, 1],
        attn_rep_out[:, 2],
        attn_rep_out[:, 3],
        attn_rep_out[:, 4],
        ffn_rep_out[:, 0],
        ffn_rep_out[:, 1],
        ffn_rep_out[:, 2],
        ffn_rep_out[:, 3:].reshape(-1),
    )


def solution(mesh):
    row_spec = P("dp", ("ctx", "tensor"), None)
    w_rc = P(("dp", "ctx"), "tensor")
    w_cr = P("tensor", ("dp", "ctx"))
    vec = P(("dp", "ctx"))
    return jax.shard_map(
        body,
        mesh=mesh,
        in_specs=(row_spec, row_spec, P("dp"), w_rc, w_rc, w_rc, w_cr, w_rc, w_cr) + (vec,) * 9,
        out_specs=(row_spec, row_spec, w_rc, w_rc, w_rc, w_cr, w_rc, w_cr) + (vec,) * 9,
        check_vma=False,
    )
```

```python
import functools

import jax
import jax.numpy as jnp
from jax import lax
from jax.experimental import pallas as pl
from jax.experimental.pallas import tpu as pltpu
from jax.sharding import PartitionSpec as P

HD = 64
epsilon = 1e-05
masked_value = -1e30
ALL = ("dp", "ctx", "tensor")
SEQ_AXES = ("ctx", "tensor")


def exact_gelu(value):
    return jax.nn.gelu(value, approximate=False)


def mm(left, right):
    return jnp.dot(left, right, preferred_element_type=jnp.float32)


def mm_tn(left, right):
    return lax.dot_general(left, right, (((0,), (0,)), ((), ())), preferred_element_type=jnp.float32)


def mm_nt(left, right):
    return lax.dot_general(left, right, (((1,), (1,)), ((), ())), preferred_element_type=jnp.float32)


def ln_forward(hidden, gain, shift):
    mean = jnp.mean(hidden, axis=-1, keepdims=True)
    centre = hidden - mean
    var = jnp.mean(centre * centre, axis=-1, keepdims=True)
    inv = lax.rsqrt(var + epsilon)
    normed = centre * inv
    return normed * gain + shift, normed, inv


def ln_backward(grad_out, normed, inv, gain):
    d_normed = grad_out * gain
    width = normed.shape[-1]
    mean_d = jnp.sum(d_normed, axis=-1, keepdims=True) / width
    mean_dn = jnp.sum(d_normed * normed, axis=-1, keepdims=True) / width
    d_in = inv * (d_normed - mean_d - normed * mean_dn)
    d_gain = jnp.sum(grad_out * normed, axis=0)
    d_shift = jnp.sum(grad_out, axis=0)
    return d_in, d_gain, d_shift


KEY_BLOCK = 512


def _lane_masks(shape):
    lane = lax.broadcasted_iota(jnp.int32, shape, 1)
    return lane < HD, lane >= HD


def _nt(a, b):
    return lax.dot_general(a, b, (((1,), (1,)), ((), ())), preferred_element_type=jnp.float32)


def _tn(a, b):
    return lax.dot_general(a, b, (((0,), (0,)), ((), ())), preferred_element_type=jnp.float32)


def _attn_fwd_kernel(len_ref, q_ref, k_ref, v_ref, o_ref, lse_ref, s_buf, *, scale):
    length = len_ref[0]
    n_blocks = (length + KEY_BLOCK - 1) // KEY_BLOCK
    q = q_ref[...]
    rows = q.shape[0]
    in_a, in_b = _lane_masks(q.shape)
    zero = jnp.zeros_like(q)
    q_heads = (jnp.where(in_a, q, zero), jnp.where(in_b, q, zero))

    def pass_max(b, ms):
        start = pl.multiple_of(b * KEY_BLOCK, KEY_BLOCK)
        k_blk = k_ref[pl.ds(start, KEY_BLOCK), :]
        out = []
        for j in range(2):
            s = _nt(q_heads[j], k_blk) * scale
            pos = start + lax.broadcasted_iota(jnp.int32, s.shape, 1)
            s = jnp.where(pos < length, s, masked_value)
            s_buf[j, :, pl.ds(start, KEY_BLOCK)] = s
            out.append(jnp.maximum(ms[j], jnp.max(s, axis=1, keepdims=True)))
        return tuple(out)

    init = jnp.full((rows, 1), -jnp.inf, jnp.float32)
    ms = lax.fori_loop(0, n_blocks, pass_max, (init, init))

    def pass_sum(b, ls):
        start = pl.multiple_of(b * KEY_BLOCK, KEY_BLOCK)
        out = []
        for j in range(2):
            e = jnp.exp(s_buf[j, :, pl.ds(start, KEY_BLOCK)] - ms[j])
            s_buf[j, :, pl.ds(start, KEY_BLOCK)] = e
            out.append(ls[j] + jnp.sum(e, axis=1, keepdims=True))
        return tuple(out)

    zeros1 = jnp.zeros((rows, 1), jnp.float32)
    ls = lax.fori_loop(0, n_blocks, pass_sum, (zeros1, zeros1))

    def pass_out(b, acc):
        start = pl.multiple_of(b * KEY_BLOCK, KEY_BLOCK)
        v_blk = v_ref[pl.ds(start, KEY_BLOCK), :]
        vz = jnp.zeros_like(v_blk)
        in_a_v, in_b_v = _lane_masks(v_blk.shape)
        v_heads = (jnp.where(in_a_v, v_blk, vz), jnp.where(in_b_v, v_blk, vz))
        for j in range(2):
            probs = (s_buf[j, :, pl.ds(start, KEY_BLOCK)] / ls[j]).astype(jnp.bfloat16)
            acc = acc + jnp.dot(probs, v_heads[j], preferred_element_type=jnp.float32)
        return acc

    acc = lax.fori_loop(0, n_blocks, pass_out, jnp.zeros(q.shape, jnp.float32))
    o_ref[...] = acc.astype(o_ref.dtype)
    for j in range(2):
        lse_ref[0, j] = ms[j] + jnp.log(ls[j])


def attention_fwd(length, q, k, v, scale):
    rows, width = q.shape
    seq_len = k.shape[0]
    pairs = width // (2 * HD)
    kernel = functools.partial(_attn_fwd_kernel, scale=scale)
    return pl.pallas_call(
        kernel,
        out_shape=(
            jax.ShapeDtypeStruct((rows, width), jnp.bfloat16),
            jax.ShapeDtypeStruct((pairs, 2, rows, 1), jnp.float32),
        ),
        grid_spec=pltpu.PrefetchScalarGridSpec(
            num_scalar_prefetch=1,
            grid=(pairs,),
            in_specs=[
                pl.BlockSpec((rows, 2 * HD), lambda h, n: (0, h)),
                pl.BlockSpec((seq_len, 2 * HD), lambda h, n: (0, h)),
                pl.BlockSpec((seq_len, 2 * HD), lambda h, n: (0, h)),
            ],
            out_specs=[
                pl.BlockSpec((rows, 2 * HD), lambda h, n: (0, h)),
                pl.BlockSpec((1, 2, rows, 1), lambda h, n: (h, 0, 0, 0)),
            ],
            scratch_shapes=[pltpu.VMEM((2, rows, seq_len), jnp.float32)],
        ),
        cost_estimate=pl.CostEstimate(
            flops=8 * pairs * rows * seq_len * 2 * HD,
            transcendentals=2 * pairs * rows * seq_len,
            bytes_accessed=2 * (2 * q.size + k.size + v.size),
        ),
    )(length.reshape(1), q, k, v)


def _attn_bwd_kernel(len_ref, q_ref, k_ref, v_ref, do_ref, lse_ref, dq_ref, dk_ref, dv_ref, p_buf, dp_buf, *, scale):
    length = len_ref[0]
    n_blocks = (length + KEY_BLOCK - 1) // KEY_BLOCK
    total_blocks = k_ref.shape[0] // KEY_BLOCK
    q = q_ref[...]
    do = do_ref[...]
    rows = q.shape[0]
    in_a, in_b = _lane_masks(q.shape)
    zero = jnp.zeros_like(q)
    q_heads = (jnp.where(in_a, q, zero), jnp.where(in_b, q, zero))
    do_heads = (jnp.where(in_a, do, zero), jnp.where(in_b, do, zero))
    lses = (lse_ref[0, 0], lse_ref[0, 1])

    def pass_one(b, centres):
        start = pl.multiple_of(b * KEY_BLOCK, KEY_BLOCK)
        k_blk = k_ref[pl.ds(start, KEY_BLOCK), :]
        v_blk = v_ref[pl.ds(start, KEY_BLOCK), :]
        out = []
        for j in range(2):
            s = _nt(q_heads[j], k_blk) * scale
            pos = start + lax.broadcasted_iota(jnp.int32, s.shape, 1)
            s = jnp.where(pos < length, s, masked_value)
            p = jnp.exp(s - lses[j])
            dp = _nt(do_heads[j], v_blk)
            p_buf[j, :, pl.ds(start, KEY_BLOCK)] = p
            dp_buf[j, :, pl.ds(start, KEY_BLOCK)] = dp
            out.append(centres[j] + jnp.sum(p * dp, axis=1, keepdims=True))
        return tuple(out)

    zeros1 = jnp.zeros((rows, 1), jnp.float32)
    centres = lax.fori_loop(0, n_blocks, pass_one, (zeros1, zeros1))

    def pass_two(b, dq):
        start = pl.multiple_of(b * KEY_BLOCK, KEY_BLOCK)
        k_blk = k_ref[pl.ds(start, KEY_BLOCK), :]
        kz = jnp.zeros_like(k_blk)
        in_a_k, in_b_k = _lane_masks(k_blk.shape)
        k_heads = (jnp.where(in_a_k, k_blk, kz), jnp.where(in_b_k, k_blk, kz))
        dk = jnp.zeros(k_blk.shape, jnp.float32)
        dv = jnp.zeros(k_blk.shape, jnp.float32)
        for j in range(2):
            p = p_buf[j, :, pl.ds(start, KEY_BLOCK)]
            dp = dp_buf[j, :, pl.ds(start, KEY_BLOCK)]
            pos = start + lax.broadcasted_iota(jnp.int32, p.shape, 1)
            ds = jnp.where(pos < length, p * (dp - centres[j]), 0.0).astype(jnp.bfloat16)
            dk = dk + _tn(ds, q_heads[j])
            dv = dv + _tn(p.astype(jnp.bfloat16), do_heads[j])
            dq = dq + jnp.dot(ds, k_heads[j], preferred_element_type=jnp.float32)
        dk_ref[pl.ds(start, KEY_BLOCK), :] = (dk * scale).astype(dk_ref.dtype)
        dv_ref[pl.ds(start, KEY_BLOCK), :] = dv.astype(dv_ref.dtype)
        return dq

    dq = lax.fori_loop(0, n_blocks, pass_two, jnp.zeros(q.shape, jnp.float32))
    dq_ref[...] = (dq * scale).astype(dq_ref.dtype)

    def pass_zero(b, carry):
        start = pl.multiple_of(b * KEY_BLOCK, KEY_BLOCK)
        dk_ref[pl.ds(start, KEY_BLOCK), :] = jnp.zeros((KEY_BLOCK, q.shape[1]), dk_ref.dtype)
        dv_ref[pl.ds(start, KEY_BLOCK), :] = jnp.zeros((KEY_BLOCK, q.shape[1]), dv_ref.dtype)
        return carry

    lax.fori_loop(n_blocks, total_blocks, pass_zero, 0)


def attention_bwd(length, q, k, v, do, lse, scale):
    rows, width = q.shape
    seq_len = k.shape[0]
    pairs = width // (2 * HD)
    kernel = functools.partial(_attn_bwd_kernel, scale=scale)
    return pl.pallas_call(
        kernel,
        out_shape=(
            jax.ShapeDtypeStruct((rows, width), jnp.bfloat16),
            jax.ShapeDtypeStruct((seq_len, width), jnp.bfloat16),
            jax.ShapeDtypeStruct((seq_len, width), jnp.bfloat16),
        ),
        grid_spec=pltpu.PrefetchScalarGridSpec(
            num_scalar_prefetch=1,
            grid=(pairs,),
            in_specs=[
                pl.BlockSpec((rows, 2 * HD), lambda h, n: (0, h)),
                pl.BlockSpec((seq_len, 2 * HD), lambda h, n: (0, h)),
                pl.BlockSpec((seq_len, 2 * HD), lambda h, n: (0, h)),
                pl.BlockSpec((rows, 2 * HD), lambda h, n: (0, h)),
                pl.BlockSpec((1, 2, rows, 1), lambda h, n: (h, 0, 0, 0)),
            ],
            out_specs=[
                pl.BlockSpec((rows, 2 * HD), lambda h, n: (0, h)),
                pl.BlockSpec((seq_len, 2 * HD), lambda h, n: (0, h)),
                pl.BlockSpec((seq_len, 2 * HD), lambda h, n: (0, h)),
            ],
            scratch_shapes=[pltpu.VMEM((2, rows, seq_len), jnp.float32), pltpu.VMEM((2, rows, seq_len), jnp.float32)],
        ),
        cost_estimate=pl.CostEstimate(
            flops=20 * pairs * rows * seq_len * 2 * HD,
            transcendentals=2 * pairs * rows * seq_len,
            bytes_accessed=2 * (3 * q.size + 4 * k.size),
        ),
    )(length.reshape(1), q, k, v, do, lse)


def ctx_swap(x):
    return lax.ppermute(x, "ctx", [(0, 1), (1, 0)])


def pad_cols(x, multiple):
    cols = x.shape[1]
    padded = -(-cols // multiple) * multiple
    return jnp.pad(x, ((0, 0), (0, padded - cols)))


def gather_rows(pieces, replicated, nt):
    local = jnp.concatenate(pieces + [replicated], axis=1)
    width = local.shape[1]
    staged = lax.all_gather(local, "tensor", axis=1, tiled=True).reshape(local.shape[0], nt, width)
    parts, at = [], 0
    for p in pieces:
        parts.append(staged[:, :, at : at + p.shape[1]].reshape(local.shape[0], nt * p.shape[1]))
        at += p.shape[1]
    parts.append(staged[:, 0, at:])
    joined = jnp.concatenate(parts, axis=1)
    full = lax.all_gather(joined, ("dp", "ctx"), axis=0, tiled=True)
    out, at = [], 0
    for p in pieces:
        out.append(full[:, at : at + nt * p.shape[1]])
        at += nt * p.shape[1]
    out.append(full[:, at:])
    return out


def reduce_rows(pieces, replicated, nt, gate=None):
    local = jnp.concatenate(pieces + [replicated], axis=1).astype(jnp.bfloat16)
    width = local.shape[1]
    local = pad_cols(local, 128)
    if gate is not None:
        local = local + (gate[0, 0] * 0).astype(local.dtype)
    staged = lax.psum_scatter(local, ("dp", "ctx"), scatter_dimension=0, tiled=True)
    rb = staged.shape[0]
    parts, at = [], 0
    for p in pieces:
        c = p.shape[1] // nt
        parts.append(staged[:, at : at + p.shape[1]].reshape(rb, nt, c))
        at += p.shape[1]
    rep = staged[:, at:width]
    parts.append(jnp.broadcast_to(rep[:, None, :], (rb, nt, rep.shape[1])))
    slots = jnp.concatenate(parts, axis=2)
    slot_width = slots.shape[2]
    padded = -(-slot_width // 128) * 128
    slots = jnp.pad(slots, ((0, 0), (0, 0), (0, padded - slot_width))).transpose(1, 0, 2)
    own = lax.psum_scatter(slots, "tensor", scatter_dimension=0, tiled=True)[0].astype(jnp.float32)
    out, at = [], 0
    for p in pieces:
        c = p.shape[1] // nt
        out.append(own[:, at : at + c])
        at += c
    out.append(own[:, at : at + rep.shape[1]])
    return out


def body(
    tokens,
    cotangent,
    lengths,
    w_query,
    w_key,
    w_value,
    w_output,
    w_in,
    w_out,
    bias_query,
    bias_value,
    bias_output,
    gain_first,
    shift_first,
    gain_second,
    shift_second,
    bias_out,
    bias_in,
):
    seqs, local_rows, width = tokens.shape
    ctx_rank = lax.axis_index("ctx")
    tensor_rank = lax.axis_index("tensor")
    nt = lax.axis_size("tensor")
    chunk = ctx_rank * nt + tensor_rank
    seq_len = local_rows * lax.axis_size("ctx") * nt
    scale = HD ** (-0.5)
    rb = w_query.shape[0]
    hidden = w_in.shape[1] * nt

    attn_vec = jnp.stack([bias_query, bias_value, bias_output, gain_first, shift_first], axis=1)
    wq, wk, wv, wo_t, attn_vec = gather_rows([w_query, w_key, w_value, w_output.T], attn_vec, nt)
    ffn_vec = jnp.concatenate(
        [jnp.stack([gain_second, shift_second, bias_out], axis=1), bias_in.reshape(rb, -1)], axis=1
    )
    w_in_f, w_out_t, ffn_vec = gather_rows([w_in, w_out.T], ffn_vec, nt)
    attn_vec = attn_vec.astype(jnp.float32)
    ffn_vec = ffn_vec.astype(jnp.float32)
    b_q, b_v, b_o, g1, s1 = [attn_vec[:, i] for i in range(5)]
    g2, s2, b_out = [ffn_vec[:, i] for i in range(3)]
    b_in = ffn_vec[:, 3:].reshape(hidden)

    row_positions = chunk * local_rows + jnp.arange(local_rows, dtype=jnp.int32)

    fwd = []
    for s in range(seqs):
        x_own = tokens[s]
        length = lengths[s]
        x_all = lax.all_gather(x_own, SEQ_AXES, axis=0, tiled=True)
        q = (mm(x_own, wq) + b_q).astype(jnp.bfloat16)
        k = mm(x_all, wk).astype(jnp.bfloat16)
        v = (mm(x_all, wv) + b_v).astype(jnp.bfloat16)
        attended, lse = attention_fwd(length, q, k, v, scale)
        first_in = x_own.astype(jnp.float32) + (mm_nt(attended, wo_t) + b_o)
        first, normed1, inv1 = ln_forward(first_in, g1, s1)
        fwd.append(dict(x_all=x_all, q=q, k=k, v=v, lse=lse, attended=attended, first=first,
                        normed1=normed1, inv1=inv1, length=length))

    outputs = []
    for s in range(seqs):
        f = fwd[s]
        first_low = f["first"].astype(jnp.bfloat16)
        hidden_pre = mm(first_low, w_in_f) + b_in
        activated = exact_gelu(hidden_pre).astype(jnp.bfloat16)
        second_in = f["first"] + mm_nt(activated, w_out_t) + b_out
        result, normed2, inv2 = ln_forward(second_in, g2, s2)
        outputs.append(result.astype(jnp.bfloat16))
        f.update(first_low=first_low, hidden_pre=hidden_pre, activated=activated, normed2=normed2, inv2=inv2)

    g_w_in = jnp.zeros((width, hidden), jnp.float32)
    g_w_out_t = jnp.zeros((width, hidden), jnp.float32)
    g_b_in = jnp.zeros((hidden,), jnp.float32)
    g_vec = [jnp.zeros((width,), jnp.float32) for _ in range(8)]
    for s in range(seqs):
        f = fwd[s]
        row_valid = (row_positions < f["length"]).astype(jnp.float32)
        upstream = cotangent[s].astype(jnp.float32) * row_valid[:, None]
        d_second, d_g2, d_s2 = ln_backward(upstream, f["normed2"], f["inv2"], g2)
        d_ffn = d_second.astype(jnp.bfloat16)
        g_w_out_t = g_w_out_t + mm_tn(d_ffn, f["activated"])
        d_act = mm(d_ffn, w_out_t)
        _, gelu_pull = jax.vjp(exact_gelu, f["hidden_pre"])
        d_hidden = gelu_pull(d_act)[0].astype(jnp.bfloat16)
        g_w_in = g_w_in + mm_tn(f["first_low"], d_hidden)
        g_b_in = g_b_in + jnp.sum(d_hidden.astype(jnp.float32), axis=0)
        d_first = d_second + mm_nt(d_hidden, w_in_f)
        d_first_in, d_g1, d_s1 = ln_backward(d_first, f["normed1"], f["inv1"], g1)
        g_vec[5] = g_vec[5] + d_g2
        g_vec[6] = g_vec[6] + d_s2
        g_vec[7] = g_vec[7] + jnp.sum(d_second, axis=0)
        g_vec[3] = g_vec[3] + d_g1
        g_vec[4] = g_vec[4] + d_s1
        g_vec[2] = g_vec[2] + jnp.sum(d_first_in, axis=0)
        f.update(d_first_in=d_first_in)

    ffn_rep = jnp.concatenate([jnp.stack([g_vec[5], g_vec[6], g_vec[7]], axis=1), g_b_in.reshape(width, -1)], axis=1)

    g_wq = jnp.zeros((width, width), jnp.float32)
    g_wk = jnp.zeros((width, width), jnp.float32)
    g_wv = jnp.zeros((width, width), jnp.float32)
    g_wo_t = jnp.zeros((width, width), jnp.float32)
    grad_tokens = []
    dx_gate = []
    for s in range(seqs):
        f = fwd[s]
        d_branch = f["d_first_in"].astype(jnp.bfloat16)
        g_wo_t = g_wo_t + mm_tn(d_branch, f["attended"])
        d_att = mm(d_branch, wo_t).astype(jnp.bfloat16)
        if dx_gate:
            d_att = d_att + (prev_half[0, 0] * 0).astype(d_att.dtype)
        dq, dk, dv = attention_bwd(f["length"], f["q"], f["k"], f["v"], d_att, f["lse"], scale)
        g_wq = g_wq + mm_tn(tokens[s], dq)
        g_wk = g_wk + mm_tn(f["x_all"], dk)
        g_wv = g_wv + mm_tn(f["x_all"], dv)
        g_vec[0] = g_vec[0] + jnp.sum(dq.astype(jnp.float32), axis=0)
        g_vec[1] = g_vec[1] + jnp.sum(dv.astype(jnp.float32), axis=0)
        dx_kv = (mm_nt(dk, wk) + mm_nt(dv, wv)).reshape(2, seq_len // 2, width)
        dx_mine = lax.dynamic_index_in_dim(dx_kv, ctx_rank, axis=0, keepdims=False)
        dx_theirs = lax.dynamic_index_in_dim(dx_kv, 1 - ctx_rank, axis=0, keepdims=False).astype(jnp.bfloat16)
        dx_half = (dx_mine + ctx_swap(dx_theirs).astype(jnp.float32)).astype(jnp.bfloat16)
        dx_kv_own = lax.psum_scatter(dx_half, "tensor", scatter_dimension=0, tiled=True).astype(jnp.float32)
        dx_gate.append(dx_kv_own[0:1, 0:1])
        prev_half = dx_half
        d_tok = f["d_first_in"] + mm_nt(dq, wq) + dx_kv_own
        grad_tokens.append(d_tok.astype(jnp.bfloat16))

    attn_rep = jnp.stack(g_vec[0:5], axis=1)
    grad_w_in, grad_w_out_t, grad_wq, grad_wk, grad_wv, grad_wo_t, rep_out = reduce_rows(
        [g_w_in, g_w_out_t, g_wq, g_wk, g_wv, g_wo_t],
        jnp.concatenate([ffn_rep, attn_rep], axis=1),
        nt,
        gate=sum(dx_gate),
    )
    ffn_rep_out = rep_out[:, : ffn_rep.shape[1]]
    attn_rep_out = rep_out[:, ffn_rep.shape[1] :]

    return (
        jnp.stack(outputs),
        jnp.stack(grad_tokens),
        grad_wq,
        grad_wk,
        grad_wv,
        grad_wo_t.T,
        grad_w_in,
        grad_w_out_t.T,
        attn_rep_out[:, 0],
        attn_rep_out[:, 1],
        attn_rep_out[:, 2],
        attn_rep_out[:, 3],
        attn_rep_out[:, 4],
        ffn_rep_out[:, 0],
        ffn_rep_out[:, 1],
        ffn_rep_out[:, 2],
        ffn_rep_out[:, 3:].reshape(-1),
    )


def solution(mesh):
    row_spec = P("dp", ("ctx", "tensor"), None)
    w_rc = P(("dp", "ctx"), "tensor")
    w_cr = P("tensor", ("dp", "ctx"))
    vec = P(("dp", "ctx"))
    return jax.shard_map(
        body,
        mesh=mesh,
        in_specs=(row_spec, row_spec, P("dp"), w_rc, w_rc, w_rc, w_cr, w_rc, w_cr) + (vec,) * 9,
        out_specs=(row_spec, row_spec, w_rc, w_rc, w_rc, w_cr, w_rc, w_cr) + (vec,) * 9,
        check_vma=False,
    )
```

```python
import functools

import jax
import jax.numpy as jnp
from jax import lax
from jax.experimental import pallas as pl
from jax.experimental.pallas import tpu as pltpu
from jax.sharding import PartitionSpec as P

HD = 64
epsilon = 1e-05
masked_value = -1e30
ALL = ("dp", "ctx", "tensor")
SEQ_AXES = ("ctx", "tensor")


def exact_gelu(value):
    return jax.nn.gelu(value, approximate=False)


def mm(left, right):
    return jnp.dot(left, right, preferred_element_type=jnp.float32)


def mm_tn(left, right):
    return lax.dot_general(left, right, (((0,), (0,)), ((), ())), preferred_element_type=jnp.float32)


def mm_nt(left, right):
    return lax.dot_general(left, right, (((1,), (1,)), ((), ())), preferred_element_type=jnp.float32)


def ln_forward(hidden, gain, shift):
    mean = jnp.mean(hidden, axis=-1, keepdims=True)
    centre = hidden - mean
    var = jnp.mean(centre * centre, axis=-1, keepdims=True)
    inv = lax.rsqrt(var + epsilon)
    normed = centre * inv
    return normed * gain + shift, normed, inv


def ln_backward(grad_out, normed, inv, gain):
    d_normed = grad_out * gain
    width = normed.shape[-1]
    mean_d = jnp.sum(d_normed, axis=-1, keepdims=True) / width
    mean_dn = jnp.sum(d_normed * normed, axis=-1, keepdims=True) / width
    d_in = inv * (d_normed - mean_d - normed * mean_dn)
    d_gain = jnp.sum(grad_out * normed, axis=0)
    d_shift = jnp.sum(grad_out, axis=0)
    return d_in, d_gain, d_shift


KEY_BLOCK = 512


def _lane_masks(shape):
    lane = lax.broadcasted_iota(jnp.int32, shape, 1)
    return lane < HD, lane >= HD


def _nt(a, b):
    return lax.dot_general(a, b, (((1,), (1,)), ((), ())), preferred_element_type=jnp.float32)


def _tn(a, b):
    return lax.dot_general(a, b, (((0,), (0,)), ((), ())), preferred_element_type=jnp.float32)


def _attn_fwd_kernel(len_ref, q_ref, k_ref, v_ref, o_ref, lse_ref, s_buf, *, scale):
    length = len_ref[0]
    n_blocks = (length + KEY_BLOCK - 1) // KEY_BLOCK
    q = q_ref[...]
    rows = q.shape[0]
    in_a, in_b = _lane_masks(q.shape)
    zero = jnp.zeros_like(q)
    q_heads = (jnp.where(in_a, q, zero), jnp.where(in_b, q, zero))

    def pass_max(b, ms):
        start = pl.multiple_of(b * KEY_BLOCK, KEY_BLOCK)
        k_blk = k_ref[pl.ds(start, KEY_BLOCK), :]
        out = []
        for j in range(2):
            s = _nt(q_heads[j], k_blk) * scale
            pos = start + lax.broadcasted_iota(jnp.int32, s.shape, 1)
            s = jnp.where(pos < length, s, masked_value)
            s_buf[j, :, pl.ds(start, KEY_BLOCK)] = s
            out.append(jnp.maximum(ms[j], jnp.max(s, axis=1, keepdims=True)))
        return tuple(out)

    init = jnp.full((rows, 1), -jnp.inf, jnp.float32)
    ms = lax.fori_loop(0, n_blocks, pass_max, (init, init))

    def pass_sum(b, ls):
        start = pl.multiple_of(b * KEY_BLOCK, KEY_BLOCK)
        out = []
        for j in range(2):
            e = jnp.exp(s_buf[j, :, pl.ds(start, KEY_BLOCK)] - ms[j])
            s_buf[j, :, pl.ds(start, KEY_BLOCK)] = e
            out.append(ls[j] + jnp.sum(e, axis=1, keepdims=True))
        return tuple(out)

    zeros1 = jnp.zeros((rows, 1), jnp.float32)
    ls = lax.fori_loop(0, n_blocks, pass_sum, (zeros1, zeros1))

    def pass_out(b, acc):
        start = pl.multiple_of(b * KEY_BLOCK, KEY_BLOCK)
        v_blk = v_ref[pl.ds(start, KEY_BLOCK), :]
        vz = jnp.zeros_like(v_blk)
        in_a_v, in_b_v = _lane_masks(v_blk.shape)
        v_heads = (jnp.where(in_a_v, v_blk, vz), jnp.where(in_b_v, v_blk, vz))
        for j in range(2):
            probs = (s_buf[j, :, pl.ds(start, KEY_BLOCK)] / ls[j]).astype(jnp.bfloat16)
            acc = acc + jnp.dot(probs, v_heads[j], preferred_element_type=jnp.float32)
        return acc

    acc = lax.fori_loop(0, n_blocks, pass_out, jnp.zeros(q.shape, jnp.float32))
    o_ref[...] = acc.astype(o_ref.dtype)
    for j in range(2):
        lse_ref[0, j] = ms[j] + jnp.log(ls[j])


def attention_fwd(length, q, k, v, scale):
    rows, width = q.shape
    seq_len = k.shape[0]
    pairs = width // (2 * HD)
    kernel = functools.partial(_attn_fwd_kernel, scale=scale)
    return pl.pallas_call(
        kernel,
        out_shape=(
            jax.ShapeDtypeStruct((rows, width), jnp.bfloat16),
            jax.ShapeDtypeStruct((pairs, 2, rows, 1), jnp.float32),
        ),
        grid_spec=pltpu.PrefetchScalarGridSpec(
            num_scalar_prefetch=1,
            grid=(pairs,),
            in_specs=[
                pl.BlockSpec((rows, 2 * HD), lambda h, n: (0, h)),
                pl.BlockSpec((seq_len, 2 * HD), lambda h, n: (0, h)),
                pl.BlockSpec((seq_len, 2 * HD), lambda h, n: (0, h)),
            ],
            out_specs=[
                pl.BlockSpec((rows, 2 * HD), lambda h, n: (0, h)),
                pl.BlockSpec((1, 2, rows, 1), lambda h, n: (h, 0, 0, 0)),
            ],
            scratch_shapes=[pltpu.VMEM((2, rows, seq_len), jnp.float32)],
        ),
        cost_estimate=pl.CostEstimate(
            flops=8 * pairs * rows * seq_len * 2 * HD,
            transcendentals=2 * pairs * rows * seq_len,
            bytes_accessed=2 * (2 * q.size + k.size + v.size),
        ),
    )(length.reshape(1), q, k, v)


def _attn_bwd_kernel(len_ref, q_ref, k_ref, v_ref, do_ref, lse_ref, dq_ref, dk_ref, dv_ref, p_buf, dp_buf, *, scale):
    length = len_ref[0]
    n_blocks = (length + KEY_BLOCK - 1) // KEY_BLOCK
    total_blocks = k_ref.shape[0] // KEY_BLOCK
    q = q_ref[...]
    do = do_ref[...]
    rows = q.shape[0]
    in_a, in_b = _lane_masks(q.shape)
    zero = jnp.zeros_like(q)
    q_heads = (jnp.where(in_a, q, zero), jnp.where(in_b, q, zero))
    do_heads = (jnp.where(in_a, do, zero), jnp.where(in_b, do, zero))
    lses = (lse_ref[0, 0], lse_ref[0, 1])

    def pass_one(b, centres):
        start = pl.multiple_of(b * KEY_BLOCK, KEY_BLOCK)
        k_blk = k_ref[pl.ds(start, KEY_BLOCK), :]
        v_blk = v_ref[pl.ds(start, KEY_BLOCK), :]
        out = []
        for j in range(2):
            s = _nt(q_heads[j], k_blk) * scale
            pos = start + lax.broadcasted_iota(jnp.int32, s.shape, 1)
            s = jnp.where(pos < length, s, masked_value)
            p = jnp.exp(s - lses[j])
            dp = _nt(do_heads[j], v_blk)
            p_buf[j, :, pl.ds(start, KEY_BLOCK)] = p
            dp_buf[j, :, pl.ds(start, KEY_BLOCK)] = dp
            out.append(centres[j] + jnp.sum(p * dp, axis=1, keepdims=True))
        return tuple(out)

    zeros1 = jnp.zeros((rows, 1), jnp.float32)
    centres = lax.fori_loop(0, n_blocks, pass_one, (zeros1, zeros1))

    def pass_two(b, dq):
        start = pl.multiple_of(b * KEY_BLOCK, KEY_BLOCK)
        k_blk = k_ref[pl.ds(start, KEY_BLOCK), :]
        kz = jnp.zeros_like(k_blk)
        in_a_k, in_b_k = _lane_masks(k_blk.shape)
        k_heads = (jnp.where(in_a_k, k_blk, kz), jnp.where(in_b_k, k_blk, kz))
        dk = jnp.zeros(k_blk.shape, jnp.float32)
        dv = jnp.zeros(k_blk.shape, jnp.float32)
        for j in range(2):
            p = p_buf[j, :, pl.ds(start, KEY_BLOCK)]
            dp = dp_buf[j, :, pl.ds(start, KEY_BLOCK)]
            pos = start + lax.broadcasted_iota(jnp.int32, p.shape, 1)
            ds = jnp.where(pos < length, p * (dp - centres[j]), 0.0).astype(jnp.bfloat16)
            dk = dk + _tn(ds, q_heads[j])
            dv = dv + _tn(p.astype(jnp.bfloat16), do_heads[j])
            dq = dq + jnp.dot(ds, k_heads[j], preferred_element_type=jnp.float32)
        dk_ref[pl.ds(start, KEY_BLOCK), :] = (dk * scale).astype(dk_ref.dtype)
        dv_ref[pl.ds(start, KEY_BLOCK), :] = dv.astype(dv_ref.dtype)
        return dq

    dq = lax.fori_loop(0, n_blocks, pass_two, jnp.zeros(q.shape, jnp.float32))
    dq_ref[...] = (dq * scale).astype(dq_ref.dtype)

    def pass_zero(b, carry):
        start = pl.multiple_of(b * KEY_BLOCK, KEY_BLOCK)
        dk_ref[pl.ds(start, KEY_BLOCK), :] = jnp.zeros((KEY_BLOCK, q.shape[1]), dk_ref.dtype)
        dv_ref[pl.ds(start, KEY_BLOCK), :] = jnp.zeros((KEY_BLOCK, q.shape[1]), dv_ref.dtype)
        return carry

    lax.fori_loop(n_blocks, total_blocks, pass_zero, 0)


def attention_bwd(length, q, k, v, do, lse, scale):
    rows, width = q.shape
    seq_len = k.shape[0]
    pairs = width // (2 * HD)
    kernel = functools.partial(_attn_bwd_kernel, scale=scale)
    return pl.pallas_call(
        kernel,
        out_shape=(
            jax.ShapeDtypeStruct((rows, width), jnp.bfloat16),
            jax.ShapeDtypeStruct((seq_len, width), jnp.bfloat16),
            jax.ShapeDtypeStruct((seq_len, width), jnp.bfloat16),
        ),
        grid_spec=pltpu.PrefetchScalarGridSpec(
            num_scalar_prefetch=1,
            grid=(pairs,),
            in_specs=[
                pl.BlockSpec((rows, 2 * HD), lambda h, n: (0, h)),
                pl.BlockSpec((seq_len, 2 * HD), lambda h, n: (0, h)),
                pl.BlockSpec((seq_len, 2 * HD), lambda h, n: (0, h)),
                pl.BlockSpec((rows, 2 * HD), lambda h, n: (0, h)),
                pl.BlockSpec((1, 2, rows, 1), lambda h, n: (h, 0, 0, 0)),
            ],
            out_specs=[
                pl.BlockSpec((rows, 2 * HD), lambda h, n: (0, h)),
                pl.BlockSpec((seq_len, 2 * HD), lambda h, n: (0, h)),
                pl.BlockSpec((seq_len, 2 * HD), lambda h, n: (0, h)),
            ],
            scratch_shapes=[pltpu.VMEM((2, rows, seq_len), jnp.float32), pltpu.VMEM((2, rows, seq_len), jnp.float32)],
        ),
        cost_estimate=pl.CostEstimate(
            flops=20 * pairs * rows * seq_len * 2 * HD,
            transcendentals=2 * pairs * rows * seq_len,
            bytes_accessed=2 * (3 * q.size + 4 * k.size),
        ),
    )(length.reshape(1), q, k, v, do, lse)


def ctx_swap(x):
    return lax.ppermute(x, "ctx", [(0, 1), (1, 0)])


def pad_cols(x, multiple):
    cols = x.shape[1]
    padded = -(-cols // multiple) * multiple
    return jnp.pad(x, ((0, 0), (0, padded - cols)))


def gather_rows(pieces, replicated, nt):
    ctx_rank = lax.axis_index("ctx")
    local = jnp.concatenate(pieces + [replicated], axis=1)
    width = local.shape[1]
    rb = local.shape[0]
    staged = lax.all_gather(local, "tensor", axis=1, tiled=True).reshape(rb, nt, width)
    parts, at = [], 0
    for p in pieces:
        parts.append(staged[:, :, at : at + p.shape[1]].reshape(rb, nt * p.shape[1]))
        at += p.shape[1]
    parts.append(staged[:, 0, at:])
    joined = jnp.concatenate(parts, axis=1)
    own = lax.all_gather(joined, "dp", axis=0, tiled=False)
    other = ctx_swap(own)
    full = jnp.where(ctx_rank == 0, jnp.stack([own, other], axis=1), jnp.stack([other, own], axis=1))
    full = full.reshape(-1, joined.shape[1])
    out, at = [], 0
    for p in pieces:
        out.append(full[:, at : at + nt * p.shape[1]])
        at += nt * p.shape[1]
    out.append(full[:, at:])
    return out


def reduce_rows(pieces, replicated, nt, gate=None):
    local = jnp.concatenate(pieces + [replicated], axis=1).astype(jnp.bfloat16)
    width = local.shape[1]
    local = pad_cols(local, 128)
    if gate is not None:
        local = local + (gate[0, 0] * 0).astype(local.dtype)
    ctx_rank = lax.axis_index("ctx")
    halves = local.reshape(lax.axis_size("dp"), 2, -1, local.shape[1])
    mine = lax.dynamic_index_in_dim(halves, ctx_rank, axis=1, keepdims=False)
    theirs = lax.dynamic_index_in_dim(halves, 1 - ctx_rank, axis=1, keepdims=False)
    summed = (mine.astype(jnp.float32) + ctx_swap(theirs).astype(jnp.float32)).astype(jnp.bfloat16)
    staged = lax.psum_scatter(summed, "dp", scatter_dimension=0, tiled=True)[0]
    rb = staged.shape[0]
    parts, at = [], 0
    for p in pieces:
        c = p.shape[1] // nt
        parts.append(staged[:, at : at + p.shape[1]].reshape(rb, nt, c))
        at += p.shape[1]
    rep = staged[:, at:width]
    parts.append(jnp.broadcast_to(rep[:, None, :], (rb, nt, rep.shape[1])))
    slots = jnp.concatenate(parts, axis=2)
    slot_width = slots.shape[2]
    padded = -(-slot_width // 128) * 128
    slots = jnp.pad(slots, ((0, 0), (0, 0), (0, padded - slot_width))).transpose(1, 0, 2)
    own = lax.psum_scatter(slots, "tensor", scatter_dimension=0, tiled=True)[0].astype(jnp.float32)
    out, at = [], 0
    for p in pieces:
        c = p.shape[1] // nt
        out.append(own[:, at : at + c])
        at += c
    out.append(own[:, at : at + rep.shape[1]])
    return out


def body(
    tokens,
    cotangent,
    lengths,
    w_query,
    w_key,
    w_value,
    w_output,
    w_in,
    w_out,
    bias_query,
    bias_value,
    bias_output,
    gain_first,
    shift_first,
    gain_second,
    shift_second,
    bias_out,
    bias_in,
):
    seqs, local_rows, width = tokens.shape
    ctx_rank = lax.axis_index("ctx")
    tensor_rank = lax.axis_index("tensor")
    nt = lax.axis_size("tensor")
    chunk = ctx_rank * nt + tensor_rank
    seq_len = local_rows * lax.axis_size("ctx") * nt
    scale = HD ** (-0.5)
    rb = w_query.shape[0]
    hidden = w_in.shape[1] * nt

    attn_vec = jnp.stack([bias_query, bias_value, bias_output, gain_first, shift_first], axis=1)
    wq, wk, wv, wo_t, attn_vec = gather_rows([w_query, w_key, w_value, w_output.T], attn_vec, nt)
    ffn_vec = jnp.concatenate(
        [jnp.stack([gain_second, shift_second, bias_out], axis=1), bias_in.reshape(rb, -1)], axis=1
    )
    w_in_f, w_out_t, ffn_vec = gather_rows([w_in, w_out.T], ffn_vec, nt)
    attn_vec = attn_vec.astype(jnp.float32)
    ffn_vec = ffn_vec.astype(jnp.float32)
    b_q, b_v, b_o, g1, s1 = [attn_vec[:, i] for i in range(5)]
    g2, s2, b_out = [ffn_vec[:, i] for i in range(3)]
    b_in = ffn_vec[:, 3:].reshape(hidden)

    row_positions = chunk * local_rows + jnp.arange(local_rows, dtype=jnp.int32)

    fwd = []
    for s in range(seqs):
        x_own = tokens[s]
        length = lengths[s]
        x_all = lax.all_gather(x_own, SEQ_AXES, axis=0, tiled=True)
        q = (mm(x_own, wq) + b_q).astype(jnp.bfloat16)
        k = mm(x_all, wk).astype(jnp.bfloat16)
        v = (mm(x_all, wv) + b_v).astype(jnp.bfloat16)
        attended, lse = attention_fwd(length, q, k, v, scale)
        first_in = x_own.astype(jnp.float32) + (mm_nt(attended, wo_t) + b_o)
        first, normed1, inv1 = ln_forward(first_in, g1, s1)
        fwd.append(dict(x_all=x_all, q=q, k=k, v=v, lse=lse, attended=attended, first=first,
                        normed1=normed1, inv1=inv1, length=length))

    outputs = []
    for s in range(seqs):
        f = fwd[s]
        first_low = f["first"].astype(jnp.bfloat16)
        hidden_pre = mm(first_low, w_in_f) + b_in
        activated = exact_gelu(hidden_pre).astype(jnp.bfloat16)
        second_in = f["first"] + mm_nt(activated, w_out_t) + b_out
        result, normed2, inv2 = ln_forward(second_in, g2, s2)
        outputs.append(result.astype(jnp.bfloat16))
        f.update(first_low=first_low, hidden_pre=hidden_pre, activated=activated, normed2=normed2, inv2=inv2)

    g_w_in = jnp.zeros((width, hidden), jnp.float32)
    g_w_out_t = jnp.zeros((width, hidden), jnp.float32)
    g_b_in = jnp.zeros((hidden,), jnp.float32)
    g_vec = [jnp.zeros((width,), jnp.float32) for _ in range(8)]
    for s in range(seqs):
        f = fwd[s]
        row_valid = (row_positions < f["length"]).astype(jnp.float32)
        upstream = cotangent[s].astype(jnp.float32) * row_valid[:, None]
        d_second, d_g2, d_s2 = ln_backward(upstream, f["normed2"], f["inv2"], g2)
        d_ffn = d_second.astype(jnp.bfloat16)
        g_w_out_t = g_w_out_t + mm_tn(d_ffn, f["activated"])
        d_act = mm(d_ffn, w_out_t)
        _, gelu_pull = jax.vjp(exact_gelu, f["hidden_pre"])
        d_hidden = gelu_pull(d_act)[0].astype(jnp.bfloat16)
        g_w_in = g_w_in + mm_tn(f["first_low"], d_hidden)
        g_b_in = g_b_in + jnp.sum(d_hidden.astype(jnp.float32), axis=0)
        d_first = d_second + mm_nt(d_hidden, w_in_f)
        d_first_in, d_g1, d_s1 = ln_backward(d_first, f["normed1"], f["inv1"], g1)
        g_vec[5] = g_vec[5] + d_g2
        g_vec[6] = g_vec[6] + d_s2
        g_vec[7] = g_vec[7] + jnp.sum(d_second, axis=0)
        g_vec[3] = g_vec[3] + d_g1
        g_vec[4] = g_vec[4] + d_s1
        g_vec[2] = g_vec[2] + jnp.sum(d_first_in, axis=0)
        f.update(d_first_in=d_first_in)

    ffn_rep = jnp.concatenate([jnp.stack([g_vec[5], g_vec[6], g_vec[7]], axis=1), g_b_in.reshape(width, -1)], axis=1)

    g_wq = jnp.zeros((width, width), jnp.float32)
    g_wk = jnp.zeros((width, width), jnp.float32)
    g_wv = jnp.zeros((width, width), jnp.float32)
    g_wo_t = jnp.zeros((width, width), jnp.float32)
    grad_tokens = []
    dx_gate = []
    for s in range(seqs):
        f = fwd[s]
        d_branch = f["d_first_in"].astype(jnp.bfloat16)
        g_wo_t = g_wo_t + mm_tn(d_branch, f["attended"])
        d_att = mm(d_branch, wo_t).astype(jnp.bfloat16)
        if dx_gate:
            d_att = d_att + (prev_half[0, 0] * 0).astype(d_att.dtype)
        dq, dk, dv = attention_bwd(f["length"], f["q"], f["k"], f["v"], d_att, f["lse"], scale)
        g_wq = g_wq + mm_tn(tokens[s], dq)
        g_wk = g_wk + mm_tn(f["x_all"], dk)
        g_wv = g_wv + mm_tn(f["x_all"], dv)
        g_vec[0] = g_vec[0] + jnp.sum(dq.astype(jnp.float32), axis=0)
        g_vec[1] = g_vec[1] + jnp.sum(dv.astype(jnp.float32), axis=0)
        dx_kv = (mm_nt(dk, wk) + mm_nt(dv, wv)).reshape(2, seq_len // 2, width)
        dx_mine = lax.dynamic_index_in_dim(dx_kv, ctx_rank, axis=0, keepdims=False)
        dx_theirs = lax.dynamic_index_in_dim(dx_kv, 1 - ctx_rank, axis=0, keepdims=False).astype(jnp.bfloat16)
        dx_half = (dx_mine + ctx_swap(dx_theirs).astype(jnp.float32)).astype(jnp.bfloat16)
        dx_kv_own = lax.psum_scatter(dx_half, "tensor", scatter_dimension=0, tiled=True).astype(jnp.float32)
        dx_gate.append(dx_kv_own[0:1, 0:1])
        prev_half = dx_half
        d_tok = f["d_first_in"] + mm_nt(dq, wq) + dx_kv_own
        grad_tokens.append(d_tok.astype(jnp.bfloat16))

    attn_rep = jnp.stack(g_vec[0:5], axis=1)
    grad_w_in, grad_w_out_t, grad_wq, grad_wk, grad_wv, grad_wo_t, rep_out = reduce_rows(
        [g_w_in, g_w_out_t, g_wq, g_wk, g_wv, g_wo_t],
        jnp.concatenate([ffn_rep, attn_rep], axis=1),
        nt,
        gate=sum(dx_gate),
    )
    ffn_rep_out = rep_out[:, : ffn_rep.shape[1]]
    attn_rep_out = rep_out[:, ffn_rep.shape[1] :]

    return (
        jnp.stack(outputs),
        jnp.stack(grad_tokens),
        grad_wq,
        grad_wk,
        grad_wv,
        grad_wo_t.T,
        grad_w_in,
        grad_w_out_t.T,
        attn_rep_out[:, 0],
        attn_rep_out[:, 1],
        attn_rep_out[:, 2],
        attn_rep_out[:, 3],
        attn_rep_out[:, 4],
        ffn_rep_out[:, 0],
        ffn_rep_out[:, 1],
        ffn_rep_out[:, 2],
        ffn_rep_out[:, 3:].reshape(-1),
    )


def solution(mesh):
    row_spec = P("dp", ("ctx", "tensor"), None)
    w_rc = P(("dp", "ctx"), "tensor")
    w_cr = P("tensor", ("dp", "ctx"))
    vec = P(("dp", "ctx"))
    return jax.shard_map(
        body,
        mesh=mesh,
        in_specs=(row_spec, row_spec, P("dp"), w_rc, w_rc, w_rc, w_cr, w_rc, w_cr) + (vec,) * 9,
        out_specs=(row_spec, row_spec, w_rc, w_rc, w_rc, w_cr, w_rc, w_cr) + (vec,) * 9,
        check_vma=False,
    )
```

```python
import functools

import jax
import jax.numpy as jnp
from jax import lax
from jax.experimental import pallas as pl
from jax.experimental.pallas import tpu as pltpu
from jax.sharding import PartitionSpec as P

HD = 64
epsilon = 1e-05
masked_value = -1e30
ALL = ("dp", "ctx", "tensor")
SEQ_AXES = ("ctx", "tensor")


def exact_gelu(value):
    return jax.nn.gelu(value, approximate=False)


def mm(left, right):
    return jnp.dot(left, right, preferred_element_type=jnp.float32)


def mm_tn(left, right):
    return lax.dot_general(left, right, (((0,), (0,)), ((), ())), preferred_element_type=jnp.float32)


def mm_nt(left, right):
    return lax.dot_general(left, right, (((1,), (1,)), ((), ())), preferred_element_type=jnp.float32)


def ln_forward(hidden, gain, shift):
    mean = jnp.mean(hidden, axis=-1, keepdims=True)
    centre = hidden - mean
    var = jnp.mean(centre * centre, axis=-1, keepdims=True)
    inv = lax.rsqrt(var + epsilon)
    normed = centre * inv
    return normed * gain + shift, normed, inv


def ln_backward(grad_out, normed, inv, gain):
    d_normed = grad_out * gain
    width = normed.shape[-1]
    mean_d = jnp.sum(d_normed, axis=-1, keepdims=True) / width
    mean_dn = jnp.sum(d_normed * normed, axis=-1, keepdims=True) / width
    d_in = inv * (d_normed - mean_d - normed * mean_dn)
    d_gain = jnp.sum(grad_out * normed, axis=0)
    d_shift = jnp.sum(grad_out, axis=0)
    return d_in, d_gain, d_shift


KEY_BLOCK = 512


def _lane_masks(shape):
    lane = lax.broadcasted_iota(jnp.int32, shape, 1)
    return lane < HD, lane >= HD


def _nt(a, b):
    return lax.dot_general(a, b, (((1,), (1,)), ((), ())), preferred_element_type=jnp.float32)


def _tn(a, b):
    return lax.dot_general(a, b, (((0,), (0,)), ((), ())), preferred_element_type=jnp.float32)


def _attn_fwd_kernel(len_ref, q_ref, k_ref, v_ref, o_ref, lse_ref, s_buf, *, scale):
    length = len_ref[0]
    n_blocks = (length + KEY_BLOCK - 1) // KEY_BLOCK
    q = q_ref[...]
    rows = q.shape[0]
    in_a, in_b = _lane_masks(q.shape)
    zero = jnp.zeros_like(q)
    q_heads = (jnp.where(in_a, q, zero), jnp.where(in_b, q, zero))

    def pass_max(b, ms):
        start = pl.multiple_of(b * KEY_BLOCK, KEY_BLOCK)
        k_blk = k_ref[pl.ds(start, KEY_BLOCK), :]
        out = []
        for j in range(2):
            s = _nt(q_heads[j], k_blk) * scale
            pos = start + lax.broadcasted_iota(jnp.int32, s.shape, 1)
            s = jnp.where(pos < length, s, masked_value)
            s_buf[j, :, pl.ds(start, KEY_BLOCK)] = s
            out.append(jnp.maximum(ms[j], jnp.max(s, axis=1, keepdims=True)))
        return tuple(out)

    init = jnp.full((rows, 1), -jnp.inf, jnp.float32)
    ms = lax.fori_loop(0, n_blocks, pass_max, (init, init))

    def pass_sum(b, ls):
        start = pl.multiple_of(b * KEY_BLOCK, KEY_BLOCK)
        out = []
        for j in range(2):
            e = jnp.exp(s_buf[j, :, pl.ds(start, KEY_BLOCK)] - ms[j])
            s_buf[j, :, pl.ds(start, KEY_BLOCK)] = e
            out.append(ls[j] + jnp.sum(e, axis=1, keepdims=True))
        return tuple(out)

    zeros1 = jnp.zeros((rows, 1), jnp.float32)
    ls = lax.fori_loop(0, n_blocks, pass_sum, (zeros1, zeros1))

    def pass_out(b, acc):
        start = pl.multiple_of(b * KEY_BLOCK, KEY_BLOCK)
        v_blk = v_ref[pl.ds(start, KEY_BLOCK), :]
        vz = jnp.zeros_like(v_blk)
        in_a_v, in_b_v = _lane_masks(v_blk.shape)
        v_heads = (jnp.where(in_a_v, v_blk, vz), jnp.where(in_b_v, v_blk, vz))
        for j in range(2):
            probs = (s_buf[j, :, pl.ds(start, KEY_BLOCK)] / ls[j]).astype(jnp.bfloat16)
            acc = acc + jnp.dot(probs, v_heads[j], preferred_element_type=jnp.float32)
        return acc

    acc = lax.fori_loop(0, n_blocks, pass_out, jnp.zeros(q.shape, jnp.float32))
    o_ref[...] = acc.astype(o_ref.dtype)
    for j in range(2):
        lse_ref[0, j] = ms[j] + jnp.log(ls[j])


def attention_fwd(length, q, k, v, scale):
    rows, width = q.shape
    seq_len = k.shape[0]
    pairs = width // (2 * HD)
    kernel = functools.partial(_attn_fwd_kernel, scale=scale)
    return pl.pallas_call(
        kernel,
        out_shape=(
            jax.ShapeDtypeStruct((rows, width), jnp.bfloat16),
            jax.ShapeDtypeStruct((pairs, 2, rows, 1), jnp.float32),
        ),
        grid_spec=pltpu.PrefetchScalarGridSpec(
            num_scalar_prefetch=1,
            grid=(pairs,),
            in_specs=[
                pl.BlockSpec((rows, 2 * HD), lambda h, n: (0, h)),
                pl.BlockSpec((seq_len, 2 * HD), lambda h, n: (0, h)),
                pl.BlockSpec((seq_len, 2 * HD), lambda h, n: (0, h)),
            ],
            out_specs=[
                pl.BlockSpec((rows, 2 * HD), lambda h, n: (0, h)),
                pl.BlockSpec((1, 2, rows, 1), lambda h, n: (h, 0, 0, 0)),
            ],
            scratch_shapes=[pltpu.VMEM((2, rows, seq_len), jnp.float32)],
        ),
        cost_estimate=pl.CostEstimate(
            flops=8 * pairs * rows * seq_len * 2 * HD,
            transcendentals=2 * pairs * rows * seq_len,
            bytes_accessed=2 * (2 * q.size + k.size + v.size),
        ),
    )(length.reshape(1), q, k, v)


def _attn_bwd_kernel(len_ref, q_ref, k_ref, v_ref, do_ref, lse_ref, dq_ref, dk_ref, dv_ref, p_buf, dp_buf, *, scale):
    length = len_ref[0]
    n_blocks = (length + KEY_BLOCK - 1) // KEY_BLOCK
    total_blocks = k_ref.shape[0] // KEY_BLOCK
    q = q_ref[...]
    do = do_ref[...]
    rows = q.shape[0]
    in_a, in_b = _lane_masks(q.shape)
    zero = jnp.zeros_like(q)
    q_heads = (jnp.where(in_a, q, zero), jnp.where(in_b, q, zero))
    do_heads = (jnp.where(in_a, do, zero), jnp.where(in_b, do, zero))
    lses = (lse_ref[0, 0], lse_ref[0, 1])

    def pass_one(b, centres):
        start = pl.multiple_of(b * KEY_BLOCK, KEY_BLOCK)
        k_blk = k_ref[pl.ds(start, KEY_BLOCK), :]
        v_blk = v_ref[pl.ds(start, KEY_BLOCK), :]
        out = []
        for j in range(2):
            s = _nt(q_heads[j], k_blk) * scale
            pos = start + lax.broadcasted_iota(jnp.int32, s.shape, 1)
            s = jnp.where(pos < length, s, masked_value)
            p = jnp.exp(s - lses[j])
            dp = _nt(do_heads[j], v_blk)
            p_buf[j, :, pl.ds(start, KEY_BLOCK)] = p
            dp_buf[j, :, pl.ds(start, KEY_BLOCK)] = dp
            out.append(centres[j] + jnp.sum(p * dp, axis=1, keepdims=True))
        return tuple(out)

    zeros1 = jnp.zeros((rows, 1), jnp.float32)
    centres = lax.fori_loop(0, n_blocks, pass_one, (zeros1, zeros1))

    def pass_two(b, dq):
        start = pl.multiple_of(b * KEY_BLOCK, KEY_BLOCK)
        k_blk = k_ref[pl.ds(start, KEY_BLOCK), :]
        kz = jnp.zeros_like(k_blk)
        in_a_k, in_b_k = _lane_masks(k_blk.shape)
        k_heads = (jnp.where(in_a_k, k_blk, kz), jnp.where(in_b_k, k_blk, kz))
        dk = jnp.zeros(k_blk.shape, jnp.float32)
        dv = jnp.zeros(k_blk.shape, jnp.float32)
        for j in range(2):
            p = p_buf[j, :, pl.ds(start, KEY_BLOCK)]
            dp = dp_buf[j, :, pl.ds(start, KEY_BLOCK)]
            pos = start + lax.broadcasted_iota(jnp.int32, p.shape, 1)
            ds = jnp.where(pos < length, p * (dp - centres[j]), 0.0).astype(jnp.bfloat16)
            dk = dk + _tn(ds, q_heads[j])
            dv = dv + _tn(p.astype(jnp.bfloat16), do_heads[j])
            dq = dq + jnp.dot(ds, k_heads[j], preferred_element_type=jnp.float32)
        dk_ref[pl.ds(start, KEY_BLOCK), :] = (dk * scale).astype(dk_ref.dtype)
        dv_ref[pl.ds(start, KEY_BLOCK), :] = dv.astype(dv_ref.dtype)
        return dq

    dq = lax.fori_loop(0, n_blocks, pass_two, jnp.zeros(q.shape, jnp.float32))
    dq_ref[...] = (dq * scale).astype(dq_ref.dtype)

    def pass_zero(b, carry):
        start = pl.multiple_of(b * KEY_BLOCK, KEY_BLOCK)
        dk_ref[pl.ds(start, KEY_BLOCK), :] = jnp.zeros((KEY_BLOCK, q.shape[1]), dk_ref.dtype)
        dv_ref[pl.ds(start, KEY_BLOCK), :] = jnp.zeros((KEY_BLOCK, q.shape[1]), dv_ref.dtype)
        return carry

    lax.fori_loop(n_blocks, total_blocks, pass_zero, 0)


def attention_bwd(length, q, k, v, do, lse, scale):
    rows, width = q.shape
    seq_len = k.shape[0]
    pairs = width // (2 * HD)
    kernel = functools.partial(_attn_bwd_kernel, scale=scale)
    return pl.pallas_call(
        kernel,
        out_shape=(
            jax.ShapeDtypeStruct((rows, width), jnp.bfloat16),
            jax.ShapeDtypeStruct((seq_len, width), jnp.bfloat16),
            jax.ShapeDtypeStruct((seq_len, width), jnp.bfloat16),
        ),
        grid_spec=pltpu.PrefetchScalarGridSpec(
            num_scalar_prefetch=1,
            grid=(pairs,),
            in_specs=[
                pl.BlockSpec((rows, 2 * HD), lambda h, n: (0, h)),
                pl.BlockSpec((seq_len, 2 * HD), lambda h, n: (0, h)),
                pl.BlockSpec((seq_len, 2 * HD), lambda h, n: (0, h)),
                pl.BlockSpec((rows, 2 * HD), lambda h, n: (0, h)),
                pl.BlockSpec((1, 2, rows, 1), lambda h, n: (h, 0, 0, 0)),
            ],
            out_specs=[
                pl.BlockSpec((rows, 2 * HD), lambda h, n: (0, h)),
                pl.BlockSpec((seq_len, 2 * HD), lambda h, n: (0, h)),
                pl.BlockSpec((seq_len, 2 * HD), lambda h, n: (0, h)),
            ],
            scratch_shapes=[pltpu.VMEM((2, rows, seq_len), jnp.float32), pltpu.VMEM((2, rows, seq_len), jnp.float32)],
        ),
        cost_estimate=pl.CostEstimate(
            flops=20 * pairs * rows * seq_len * 2 * HD,
            transcendentals=2 * pairs * rows * seq_len,
            bytes_accessed=2 * (3 * q.size + 4 * k.size),
        ),
    )(length.reshape(1), q, k, v, do, lse)


def ctx_swap(x):
    return lax.ppermute(x, "ctx", [(0, 1), (1, 0)])


def pad_cols(x, multiple):
    cols = x.shape[1]
    padded = -(-cols // multiple) * multiple
    return jnp.pad(x, ((0, 0), (0, padded - cols)))


def gather_rows(pieces, replicated, nt):
    local = jnp.concatenate(pieces + [replicated], axis=1)
    width = local.shape[1]
    staged = lax.all_gather(local, "tensor", axis=1, tiled=True).reshape(local.shape[0], nt, width)
    parts, at = [], 0
    for p in pieces:
        parts.append(staged[:, :, at : at + p.shape[1]].reshape(local.shape[0], nt * p.shape[1]))
        at += p.shape[1]
    parts.append(staged[:, 0, at:])
    joined = jnp.concatenate(parts, axis=1)
    full = lax.all_gather(joined, ("dp", "ctx"), axis=0, tiled=True)
    out, at = [], 0
    for p in pieces:
        out.append(full[:, at : at + nt * p.shape[1]])
        at += nt * p.shape[1]
    out.append(full[:, at:])
    return out


def reduce_rows(pieces, replicated, nt, gate=None):
    if gate is not None:
        replicated = replicated + gate[0, 0] * 0
    local = jnp.concatenate(pieces + [replicated], axis=1).astype(jnp.bfloat16)
    width = local.shape[1]
    local = pad_cols(local, 128)
    staged = lax.psum_scatter(local, ("dp", "ctx"), scatter_dimension=0, tiled=True)
    rb = staged.shape[0]
    parts, at = [], 0
    for p in pieces:
        c = p.shape[1] // nt
        parts.append(staged[:, at : at + p.shape[1]].reshape(rb, nt, c))
        at += p.shape[1]
    rep = staged[:, at:width]
    parts.append(jnp.broadcast_to(rep[:, None, :], (rb, nt, rep.shape[1])))
    slots = jnp.concatenate(parts, axis=2)
    slot_width = slots.shape[2]
    padded = -(-slot_width // 128) * 128
    slots = jnp.pad(slots, ((0, 0), (0, 0), (0, padded - slot_width))).transpose(1, 0, 2)
    own = lax.psum_scatter(slots, "tensor", scatter_dimension=0, tiled=True)[0].astype(jnp.float32)
    out, at = [], 0
    for p in pieces:
        c = p.shape[1] // nt
        out.append(own[:, at : at + c])
        at += c
    out.append(own[:, at : at + rep.shape[1]])
    return out


def body(
    tokens,
    cotangent,
    lengths,
    w_query,
    w_key,
    w_value,
    w_output,
    w_in,
    w_out,
    bias_query,
    bias_value,
    bias_output,
    gain_first,
    shift_first,
    gain_second,
    shift_second,
    bias_out,
    bias_in,
):
    seqs, local_rows, width = tokens.shape
    ctx_rank = lax.axis_index("ctx")
    tensor_rank = lax.axis_index("tensor")
    nt = lax.axis_size("tensor")
    chunk = ctx_rank * nt + tensor_rank
    seq_len = local_rows * lax.axis_size("ctx") * nt
    scale = HD ** (-0.5)
    rb = w_query.shape[0]
    hidden = w_in.shape[1] * nt

    attn_vec = jnp.stack([bias_query, bias_value, bias_output, gain_first, shift_first], axis=1)
    wq, wk, wv, wo_t, attn_vec = gather_rows([w_query, w_key, w_value, w_output.T], attn_vec, nt)
    ffn_vec = jnp.concatenate(
        [jnp.stack([gain_second, shift_second, bias_out], axis=1), bias_in.reshape(rb, -1)], axis=1
    )
    w_in_f, w_out_t, ffn_vec = gather_rows([w_in, w_out.T], ffn_vec, nt)
    attn_vec = attn_vec.astype(jnp.float32)
    ffn_vec = ffn_vec.astype(jnp.float32)
    b_q, b_v, b_o, g1, s1 = [attn_vec[:, i] for i in range(5)]
    g2, s2, b_out = [ffn_vec[:, i] for i in range(3)]
    b_in = ffn_vec[:, 3:].reshape(hidden)

    row_positions = chunk * local_rows + jnp.arange(local_rows, dtype=jnp.int32)

    fwd = []
    for s in range(seqs):
        x_own = tokens[s]
        length = lengths[s]
        x_all = lax.all_gather(x_own, SEQ_AXES, axis=0, tiled=True)
        q = (mm(x_own, wq) + b_q).astype(jnp.bfloat16)
        k = mm(x_all, wk).astype(jnp.bfloat16)
        v = (mm(x_all, wv) + b_v).astype(jnp.bfloat16)
        attended, lse = attention_fwd(length, q, k, v, scale)
        first_in = x_own.astype(jnp.float32) + (mm_nt(attended, wo_t) + b_o)
        first, normed1, inv1 = ln_forward(first_in, g1, s1)
        fwd.append(dict(x_all=x_all, q=q, k=k, v=v, lse=lse, attended=attended, first=first,
                        normed1=normed1, inv1=inv1, length=length))

    outputs = []
    for s in range(seqs):
        f = fwd[s]
        first_low = f["first"].astype(jnp.bfloat16)
        hidden_pre = mm(first_low, w_in_f) + b_in
        activated = exact_gelu(hidden_pre).astype(jnp.bfloat16)
        second_in = f["first"] + mm_nt(activated, w_out_t) + b_out
        result, normed2, inv2 = ln_forward(second_in, g2, s2)
        outputs.append(result.astype(jnp.bfloat16))
        f.update(first_low=first_low, hidden_pre=hidden_pre, activated=activated, normed2=normed2, inv2=inv2)

    g_w_in = jnp.zeros((width, hidden), jnp.float32)
    g_w_out_t = jnp.zeros((width, hidden), jnp.float32)
    g_b_in = jnp.zeros((hidden,), jnp.float32)
    g_vec = [jnp.zeros((width,), jnp.float32) for _ in range(8)]
    g_wq = jnp.zeros((width, width), jnp.float32)
    g_wk = jnp.zeros((width, width), jnp.float32)
    g_wv = jnp.zeros((width, width), jnp.float32)
    g_wo_t = jnp.zeros((width, width), jnp.float32)
    grad_tokens = []
    dx_gate = []
    firsts = {}

    def ffn_backward(s):
        nonlocal g_w_in, g_w_out_t, g_b_in
        f = fwd[s]
        row_valid = (row_positions < f["length"]).astype(jnp.float32)
        upstream = cotangent[s].astype(jnp.float32) * row_valid[:, None]
        if dx_gate:
            upstream = upstream + (prev_half[0, 0] * 0).astype(upstream.dtype)
        d_second, d_g2, d_s2 = ln_backward(upstream, f["normed2"], f["inv2"], g2)
        d_ffn = d_second.astype(jnp.bfloat16)
        g_w_out_t = g_w_out_t + mm_tn(d_ffn, f["activated"])
        d_act = mm(d_ffn, w_out_t)
        _, gelu_pull = jax.vjp(exact_gelu, f["hidden_pre"])
        d_hidden = gelu_pull(d_act)[0].astype(jnp.bfloat16)
        g_w_in = g_w_in + mm_tn(f["first_low"], d_hidden)
        g_b_in = g_b_in + jnp.sum(d_hidden.astype(jnp.float32), axis=0)
        d_first = d_second + mm_nt(d_hidden, w_in_f)
        d_first_in, d_g1, d_s1 = ln_backward(d_first, f["normed1"], f["inv1"], g1)
        g_vec[5] = g_vec[5] + d_g2
        g_vec[6] = g_vec[6] + d_s2
        g_vec[7] = g_vec[7] + jnp.sum(d_second, axis=0)
        g_vec[3] = g_vec[3] + d_g1
        g_vec[4] = g_vec[4] + d_s1
        g_vec[2] = g_vec[2] + jnp.sum(d_first_in, axis=0)
        firsts[s] = d_first_in

    def attention_backward(s):
        nonlocal g_wo_t, g_wq, g_wk, g_wv, prev_half
        f = fwd[s]
        d_first_in = firsts[s]
        d_branch = d_first_in.astype(jnp.bfloat16)
        if dx_gate:
            d_branch = d_branch + (prev_half[0, 0] * 0).astype(d_branch.dtype)
        g_wo_t = g_wo_t + mm_tn(d_branch, f["attended"])
        d_att = mm(d_branch, wo_t).astype(jnp.bfloat16)
        dq, dk, dv = attention_bwd(f["length"], f["q"], f["k"], f["v"], d_att, f["lse"], scale)
        g_wq = g_wq + mm_tn(tokens[s], dq)
        g_wk = g_wk + mm_tn(f["x_all"], dk)
        g_wv = g_wv + mm_tn(f["x_all"], dv)
        g_vec[0] = g_vec[0] + jnp.sum(dq.astype(jnp.float32), axis=0)
        g_vec[1] = g_vec[1] + jnp.sum(dv.astype(jnp.float32), axis=0)
        dx_kv = (mm_nt(dk, wk) + mm_nt(dv, wv)).reshape(2, seq_len // 2, width)
        dx_mine = lax.dynamic_index_in_dim(dx_kv, ctx_rank, axis=0, keepdims=False)
        dx_theirs = lax.dynamic_index_in_dim(dx_kv, 1 - ctx_rank, axis=0, keepdims=False).astype(jnp.bfloat16)
        dx_half = (dx_mine + ctx_swap(dx_theirs).astype(jnp.float32)).astype(jnp.bfloat16)
        dx_kv_own = lax.psum_scatter(dx_half, "tensor", scatter_dimension=0, tiled=True).astype(jnp.float32)
        dx_gate.append(dx_kv_own[0:1, 0:1])
        prev_half = dx_half
        d_tok = d_first_in + mm_nt(dq, wq) + dx_kv_own
        grad_tokens.append(d_tok.astype(jnp.bfloat16))


    prev_half = None
    for s in [0]:
        ffn_backward(s)
        attention_backward(s)
    for s in range(1, seqs):
        ffn_backward(s)
    for s in range(1, seqs):
        attention_backward(s)

    ffn_rep = jnp.concatenate([jnp.stack([g_vec[5], g_vec[6], g_vec[7]], axis=1), g_b_in.reshape(width, -1)], axis=1)
    attn_rep = jnp.stack(g_vec[0:5], axis=1)
    grad_w_in, grad_w_out_t, grad_wq, grad_wk, grad_wv, grad_wo_t, rep_out = reduce_rows(
        [g_w_in, g_w_out_t, g_wq, g_wk, g_wv, g_wo_t],
        jnp.concatenate([ffn_rep, attn_rep], axis=1),
        nt,
        gate=sum(dx_gate),
    )
    ffn_rep_out = rep_out[:, : ffn_rep.shape[1]]
    attn_rep_out = rep_out[:, ffn_rep.shape[1] :]

    return (
        jnp.stack(outputs),
        jnp.stack(grad_tokens),
        grad_wq,
        grad_wk,
        grad_wv,
        grad_wo_t.T,
        grad_w_in,
        grad_w_out_t.T,
        attn_rep_out[:, 0],
        attn_rep_out[:, 1],
        attn_rep_out[:, 2],
        attn_rep_out[:, 3],
        attn_rep_out[:, 4],
        ffn_rep_out[:, 0],
        ffn_rep_out[:, 1],
        ffn_rep_out[:, 2],
        ffn_rep_out[:, 3:].reshape(-1),
    )


def solution(mesh):
    row_spec = P("dp", ("ctx", "tensor"), None)
    w_rc = P(("dp", "ctx"), "tensor")
    w_cr = P("tensor", ("dp", "ctx"))
    vec = P(("dp", "ctx"))
    return jax.shard_map(
        body,
        mesh=mesh,
        in_specs=(row_spec, row_spec, P("dp"), w_rc, w_rc, w_rc, w_cr, w_rc, w_cr) + (vec,) * 9,
        out_specs=(row_spec, row_spec, w_rc, w_rc, w_rc, w_cr, w_rc, w_cr) + (vec,) * 9,
        check_vma=False,
    )
```

```python
import functools

import jax
import jax.numpy as jnp
from jax import lax
from jax.experimental import pallas as pl
from jax.experimental.pallas import tpu as pltpu
from jax.sharding import PartitionSpec as P

HD = 64
epsilon = 1e-05
masked_value = -1e30
ALL = ("dp", "ctx", "tensor")
SEQ_AXES = ("ctx", "tensor")


def exact_gelu(value):
    return jax.nn.gelu(value, approximate=False)


def mm(left, right):
    return jnp.dot(left, right, preferred_element_type=jnp.float32)


def mm_tn(left, right):
    return lax.dot_general(left, right, (((0,), (0,)), ((), ())), preferred_element_type=jnp.float32)


def mm_nt(left, right):
    return lax.dot_general(left, right, (((1,), (1,)), ((), ())), preferred_element_type=jnp.float32)


def ln_forward(hidden, gain, shift):
    mean = jnp.mean(hidden, axis=-1, keepdims=True)
    centre = hidden - mean
    var = jnp.mean(centre * centre, axis=-1, keepdims=True)
    inv = lax.rsqrt(var + epsilon)
    normed = centre * inv
    return normed * gain + shift, normed, inv


def ln_backward(grad_out, normed, inv, gain):
    d_normed = grad_out * gain
    width = normed.shape[-1]
    mean_d = jnp.sum(d_normed, axis=-1, keepdims=True) / width
    mean_dn = jnp.sum(d_normed * normed, axis=-1, keepdims=True) / width
    d_in = inv * (d_normed - mean_d - normed * mean_dn)
    d_gain = jnp.sum(grad_out * normed, axis=0)
    d_shift = jnp.sum(grad_out, axis=0)
    return d_in, d_gain, d_shift


KEY_BLOCK = 512


def _lane_masks(shape):
    lane = lax.broadcasted_iota(jnp.int32, shape, 1)
    return lane < HD, lane >= HD


def _nt(a, b):
    return lax.dot_general(a, b, (((1,), (1,)), ((), ())), preferred_element_type=jnp.float32)


def _tn(a, b):
    return lax.dot_general(a, b, (((0,), (0,)), ((), ())), preferred_element_type=jnp.float32)


def _attn_fwd_kernel(len_ref, q_ref, k_ref, v_ref, o_ref, lse_ref, s_buf, *, scale):
    length = len_ref[0]
    n_blocks = (length + KEY_BLOCK - 1) // KEY_BLOCK
    q = q_ref[...]
    rows = q.shape[0]
    in_a, in_b = _lane_masks(q.shape)
    zero = jnp.zeros_like(q)
    q_heads = (jnp.where(in_a, q, zero), jnp.where(in_b, q, zero))

    def pass_max(b, ms):
        start = pl.multiple_of(b * KEY_BLOCK, KEY_BLOCK)
        k_blk = k_ref[pl.ds(start, KEY_BLOCK), :]
        out = []
        for j in range(2):
            s = _nt(q_heads[j], k_blk) * scale
            pos = start + lax.broadcasted_iota(jnp.int32, s.shape, 1)
            s = jnp.where(pos < length, s, masked_value)
            s_buf[j, :, pl.ds(start, KEY_BLOCK)] = s
            out.append(jnp.maximum(ms[j], jnp.max(s, axis=1, keepdims=True)))
        return tuple(out)

    init = jnp.full((rows, 1), -jnp.inf, jnp.float32)
    ms = lax.fori_loop(0, n_blocks, pass_max, (init, init))

    def pass_sum(b, ls):
        start = pl.multiple_of(b * KEY_BLOCK, KEY_BLOCK)
        out = []
        for j in range(2):
            e = jnp.exp(s_buf[j, :, pl.ds(start, KEY_BLOCK)] - ms[j])
            s_buf[j, :, pl.ds(start, KEY_BLOCK)] = e
            out.append(ls[j] + jnp.sum(e, axis=1, keepdims=True))
        return tuple(out)

    zeros1 = jnp.zeros((rows, 1), jnp.float32)
    ls = lax.fori_loop(0, n_blocks, pass_sum, (zeros1, zeros1))

    def pass_out(b, acc):
        start = pl.multiple_of(b * KEY_BLOCK, KEY_BLOCK)
        v_blk = v_ref[pl.ds(start, KEY_BLOCK), :]
        vz = jnp.zeros_like(v_blk)
        in_a_v, in_b_v = _lane_masks(v_blk.shape)
        v_heads = (jnp.where(in_a_v, v_blk, vz), jnp.where(in_b_v, v_blk, vz))
        for j in range(2):
            probs = (s_buf[j, :, pl.ds(start, KEY_BLOCK)] / ls[j]).astype(jnp.bfloat16)
            acc = acc + jnp.dot(probs, v_heads[j], preferred_element_type=jnp.float32)
        return acc

    acc = lax.fori_loop(0, n_blocks, pass_out, jnp.zeros(q.shape, jnp.float32))
    o_ref[...] = acc.astype(o_ref.dtype)
    for j in range(2):
        lse_ref[0, j] = ms[j] + jnp.log(ls[j])


def attention_fwd(length, q, k, v, scale):
    rows, width = q.shape
    seq_len = k.shape[0]
    pairs = width // (2 * HD)
    kernel = functools.partial(_attn_fwd_kernel, scale=scale)
    return pl.pallas_call(
        kernel,
        out_shape=(
            jax.ShapeDtypeStruct((rows, width), jnp.bfloat16),
            jax.ShapeDtypeStruct((pairs, 2, rows, 1), jnp.float32),
        ),
        grid_spec=pltpu.PrefetchScalarGridSpec(
            num_scalar_prefetch=1,
            grid=(pairs,),
            in_specs=[
                pl.BlockSpec((rows, 2 * HD), lambda h, n: (0, h)),
                pl.BlockSpec((seq_len, 2 * HD), lambda h, n: (0, h)),
                pl.BlockSpec((seq_len, 2 * HD), lambda h, n: (0, h)),
            ],
            out_specs=[
                pl.BlockSpec((rows, 2 * HD), lambda h, n: (0, h)),
                pl.BlockSpec((1, 2, rows, 1), lambda h, n: (h, 0, 0, 0)),
            ],
            scratch_shapes=[pltpu.VMEM((2, rows, seq_len), jnp.float32)],
        ),
        cost_estimate=pl.CostEstimate(
            flops=8 * pairs * rows * seq_len * 2 * HD,
            transcendentals=2 * pairs * rows * seq_len,
            bytes_accessed=2 * (2 * q.size + k.size + v.size),
        ),
    )(length.reshape(1), q, k, v)


def _attn_bwd_kernel(len_ref, q_ref, k_ref, v_ref, do_ref, lse_ref, dq_ref, dk_ref, dv_ref, p_buf, dp_buf, *, scale):
    length = len_ref[0]
    n_blocks = (length + KEY_BLOCK - 1) // KEY_BLOCK
    total_blocks = k_ref.shape[0] // KEY_BLOCK
    q = q_ref[...]
    do = do_ref[...]
    rows = q.shape[0]
    in_a, in_b = _lane_masks(q.shape)
    zero = jnp.zeros_like(q)
    q_heads = (jnp.where(in_a, q, zero), jnp.where(in_b, q, zero))
    do_heads = (jnp.where(in_a, do, zero), jnp.where(in_b, do, zero))
    lses = (lse_ref[0, 0], lse_ref[0, 1])

    def pass_one(b, centres):
        start = pl.multiple_of(b * KEY_BLOCK, KEY_BLOCK)
        k_blk = k_ref[pl.ds(start, KEY_BLOCK), :]
        v_blk = v_ref[pl.ds(start, KEY_BLOCK), :]
        out = []
        for j in range(2):
            s = _nt(q_heads[j], k_blk) * scale
            pos = start + lax.broadcasted_iota(jnp.int32, s.shape, 1)
            s = jnp.where(pos < length, s, masked_value)
            p = jnp.exp(s - lses[j])
            dp = _nt(do_heads[j], v_blk)
            p_buf[j, :, pl.ds(start, KEY_BLOCK)] = p
            dp_buf[j, :, pl.ds(start, KEY_BLOCK)] = dp
            out.append(centres[j] + jnp.sum(p * dp, axis=1, keepdims=True))
        return tuple(out)

    zeros1 = jnp.zeros((rows, 1), jnp.float32)
    centres = lax.fori_loop(0, n_blocks, pass_one, (zeros1, zeros1))

    def pass_two(b, dq):
        start = pl.multiple_of(b * KEY_BLOCK, KEY_BLOCK)
        k_blk = k_ref[pl.ds(start, KEY_BLOCK), :]
        kz = jnp.zeros_like(k_blk)
        in_a_k, in_b_k = _lane_masks(k_blk.shape)
        k_heads = (jnp.where(in_a_k, k_blk, kz), jnp.where(in_b_k, k_blk, kz))
        dk = jnp.zeros(k_blk.shape, jnp.float32)
        dv = jnp.zeros(k_blk.shape, jnp.float32)
        for j in range(2):
            p = p_buf[j, :, pl.ds(start, KEY_BLOCK)]
            dp = dp_buf[j, :, pl.ds(start, KEY_BLOCK)]
            pos = start + lax.broadcasted_iota(jnp.int32, p.shape, 1)
            ds = jnp.where(pos < length, p * (dp - centres[j]), 0.0).astype(jnp.bfloat16)
            dk = dk + _tn(ds, q_heads[j])
            dv = dv + _tn(p.astype(jnp.bfloat16), do_heads[j])
            dq = dq + jnp.dot(ds, k_heads[j], preferred_element_type=jnp.float32)
        dk_ref[pl.ds(start, KEY_BLOCK), :] = (dk * scale).astype(dk_ref.dtype)
        dv_ref[pl.ds(start, KEY_BLOCK), :] = dv.astype(dv_ref.dtype)
        return dq

    dq = lax.fori_loop(0, n_blocks, pass_two, jnp.zeros(q.shape, jnp.float32))
    dq_ref[...] = (dq * scale).astype(dq_ref.dtype)

    def pass_zero(b, carry):
        start = pl.multiple_of(b * KEY_BLOCK, KEY_BLOCK)
        dk_ref[pl.ds(start, KEY_BLOCK), :] = jnp.zeros((KEY_BLOCK, q.shape[1]), dk_ref.dtype)
        dv_ref[pl.ds(start, KEY_BLOCK), :] = jnp.zeros((KEY_BLOCK, q.shape[1]), dv_ref.dtype)
        return carry

    lax.fori_loop(n_blocks, total_blocks, pass_zero, 0)


def attention_bwd(length, q, k, v, do, lse, scale):
    rows, width = q.shape
    seq_len = k.shape[0]
    pairs = width // (2 * HD)
    kernel = functools.partial(_attn_bwd_kernel, scale=scale)
    return pl.pallas_call(
        kernel,
        out_shape=(
            jax.ShapeDtypeStruct((rows, width), jnp.bfloat16),
            jax.ShapeDtypeStruct((seq_len, width), jnp.bfloat16),
            jax.ShapeDtypeStruct((seq_len, width), jnp.bfloat16),
        ),
        grid_spec=pltpu.PrefetchScalarGridSpec(
            num_scalar_prefetch=1,
            grid=(pairs,),
            in_specs=[
                pl.BlockSpec((rows, 2 * HD), lambda h, n: (0, h)),
                pl.BlockSpec((seq_len, 2 * HD), lambda h, n: (0, h)),
                pl.BlockSpec((seq_len, 2 * HD), lambda h, n: (0, h)),
                pl.BlockSpec((rows, 2 * HD), lambda h, n: (0, h)),
                pl.BlockSpec((1, 2, rows, 1), lambda h, n: (h, 0, 0, 0)),
            ],
            out_specs=[
                pl.BlockSpec((rows, 2 * HD), lambda h, n: (0, h)),
                pl.BlockSpec((seq_len, 2 * HD), lambda h, n: (0, h)),
                pl.BlockSpec((seq_len, 2 * HD), lambda h, n: (0, h)),
            ],
            scratch_shapes=[pltpu.VMEM((2, rows, seq_len), jnp.float32), pltpu.VMEM((2, rows, seq_len), jnp.float32)],
        ),
        cost_estimate=pl.CostEstimate(
            flops=20 * pairs * rows * seq_len * 2 * HD,
            transcendentals=2 * pairs * rows * seq_len,
            bytes_accessed=2 * (3 * q.size + 4 * k.size),
        ),
    )(length.reshape(1), q, k, v, do, lse)


def ctx_swap(x):
    return lax.ppermute(x, "ctx", [(0, 1), (1, 0)])


def gather_sequence(x_own, ctx_rank, tensor_rank, nt):
    received = [x_own] + [
        lax.ppermute(x_own, "tensor", [(j, (j + k) % nt) for j in range(nt)]) for k in range(1, nt)
    ]
    stacked = jnp.stack(received)
    order = (tensor_rank - jnp.arange(nt, dtype=jnp.int32)) % nt
    half = jnp.take(stacked, order, axis=0).reshape(nt * x_own.shape[0], x_own.shape[1])
    other = ctx_swap(half)
    return jnp.where(ctx_rank == 0, jnp.concatenate([half, other]), jnp.concatenate([other, half]))


def pad_cols(x, multiple):
    cols = x.shape[1]
    padded = -(-cols // multiple) * multiple
    return jnp.pad(x, ((0, 0), (0, padded - cols)))


def gather_rows(pieces, replicated, nt):
    local = jnp.concatenate(pieces + [replicated], axis=1)
    width = local.shape[1]
    staged = lax.all_gather(local, "tensor", axis=1, tiled=True).reshape(local.shape[0], nt, width)
    parts, at = [], 0
    for p in pieces:
        parts.append(staged[:, :, at : at + p.shape[1]].reshape(local.shape[0], nt * p.shape[1]))
        at += p.shape[1]
    parts.append(staged[:, 0, at:])
    joined = jnp.concatenate(parts, axis=1)
    full = lax.all_gather(joined, ("dp", "ctx"), axis=0, tiled=True)
    out, at = [], 0
    for p in pieces:
        out.append(full[:, at : at + nt * p.shape[1]])
        at += nt * p.shape[1]
    out.append(full[:, at:])
    return out


def reduce_rows(pieces, replicated, nt, gate=None):
    if gate is not None:
        replicated = replicated + gate[0, 0] * 0
    local = jnp.concatenate(pieces + [replicated], axis=1).astype(jnp.bfloat16)
    width = local.shape[1]
    local = pad_cols(local, 128)
    staged = lax.psum_scatter(local, ("dp", "ctx"), scatter_dimension=0, tiled=True)
    rb = staged.shape[0]
    parts, at = [], 0
    for p in pieces:
        c = p.shape[1] // nt
        parts.append(staged[:, at : at + p.shape[1]].reshape(rb, nt, c))
        at += p.shape[1]
    rep = staged[:, at:width]
    parts.append(jnp.broadcast_to(rep[:, None, :], (rb, nt, rep.shape[1])))
    slots = jnp.concatenate(parts, axis=2)
    slot_width = slots.shape[2]
    padded = -(-slot_width // 128) * 128
    slots = jnp.pad(slots, ((0, 0), (0, 0), (0, padded - slot_width))).transpose(1, 0, 2)
    own = lax.psum_scatter(slots, "tensor", scatter_dimension=0, tiled=True)[0].astype(jnp.float32)
    out, at = [], 0
    for p in pieces:
        c = p.shape[1] // nt
        out.append(own[:, at : at + c])
        at += c
    out.append(own[:, at : at + rep.shape[1]])
    return out


def body(
    tokens,
    cotangent,
    lengths,
    w_query,
    w_key,
    w_value,
    w_output,
    w_in,
    w_out,
    bias_query,
    bias_value,
    bias_output,
    gain_first,
    shift_first,
    gain_second,
    shift_second,
    bias_out,
    bias_in,
):
    seqs, local_rows, width = tokens.shape
    ctx_rank = lax.axis_index("ctx")
    tensor_rank = lax.axis_index("tensor")
    nt = lax.axis_size("tensor")
    chunk = ctx_rank * nt + tensor_rank
    seq_len = local_rows * lax.axis_size("ctx") * nt
    scale = HD ** (-0.5)
    rb = w_query.shape[0]
    hidden = w_in.shape[1] * nt

    attn_vec = jnp.stack([bias_query, bias_value, bias_output, gain_first, shift_first], axis=1)
    wq, wk, wv, wo_t, attn_vec = gather_rows([w_query, w_key, w_value, w_output.T], attn_vec, nt)
    ffn_vec = jnp.concatenate(
        [jnp.stack([gain_second, shift_second, bias_out], axis=1), bias_in.reshape(rb, -1)], axis=1
    )
    w_in_f, w_out_t, ffn_vec = gather_rows([w_in, w_out.T], ffn_vec, nt)
    attn_vec = attn_vec.astype(jnp.float32)
    ffn_vec = ffn_vec.astype(jnp.float32)
    b_q, b_v, b_o, g1, s1 = [attn_vec[:, i] for i in range(5)]
    g2, s2, b_out = [ffn_vec[:, i] for i in range(3)]
    b_in = ffn_vec[:, 3:].reshape(hidden)

    row_positions = chunk * local_rows + jnp.arange(local_rows, dtype=jnp.int32)

    fwd = []
    for s in range(seqs):
        x_own = tokens[s]
        length = lengths[s]
        x_all = gather_sequence(x_own, ctx_rank, tensor_rank, nt)
        q = (mm(x_own, wq) + b_q).astype(jnp.bfloat16)
        k = mm(x_all, wk).astype(jnp.bfloat16)
        v = (mm(x_all, wv) + b_v).astype(jnp.bfloat16)
        attended, lse = attention_fwd(length, q, k, v, scale)
        first_in = x_own.astype(jnp.float32) + (mm_nt(attended, wo_t) + b_o)
        first, normed1, inv1 = ln_forward(first_in, g1, s1)
        fwd.append(dict(x_all=x_all, q=q, k=k, v=v, lse=lse, attended=attended, first=first,
                        normed1=normed1, inv1=inv1, length=length))

    outputs = []
    for s in range(seqs):
        f = fwd[s]
        first_low = f["first"].astype(jnp.bfloat16)
        hidden_pre = mm(first_low, w_in_f) + b_in
        activated = exact_gelu(hidden_pre).astype(jnp.bfloat16)
        second_in = f["first"] + mm_nt(activated, w_out_t) + b_out
        result, normed2, inv2 = ln_forward(second_in, g2, s2)
        outputs.append(result.astype(jnp.bfloat16))
        f.update(first_low=first_low, hidden_pre=hidden_pre, activated=activated, normed2=normed2, inv2=inv2)

    g_w_in = jnp.zeros((width, hidden), jnp.float32)
    g_w_out_t = jnp.zeros((width, hidden), jnp.float32)
    g_b_in = jnp.zeros((hidden,), jnp.float32)
    g_vec = [jnp.zeros((width,), jnp.float32) for _ in range(8)]
    g_wq = jnp.zeros((width, width), jnp.float32)
    g_wk = jnp.zeros((width, width), jnp.float32)
    g_wv = jnp.zeros((width, width), jnp.float32)
    g_wo_t = jnp.zeros((width, width), jnp.float32)
    grad_tokens = []
    dx_gate = []
    firsts = {}

    def ffn_backward(s):
        nonlocal g_w_in, g_w_out_t, g_b_in
        f = fwd[s]
        row_valid = (row_positions < f["length"]).astype(jnp.float32)
        upstream = cotangent[s].astype(jnp.float32) * row_valid[:, None]
        if dx_gate:
            upstream = upstream + (prev_half[0, 0] * 0).astype(upstream.dtype)
        d_second, d_g2, d_s2 = ln_backward(upstream, f["normed2"], f["inv2"], g2)
        d_ffn = d_second.astype(jnp.bfloat16)
        g_w_out_t = g_w_out_t + mm_tn(d_ffn, f["activated"])
        d_act = mm(d_ffn, w_out_t)
        _, gelu_pull = jax.vjp(exact_gelu, f["hidden_pre"])
        d_hidden = gelu_pull(d_act)[0].astype(jnp.bfloat16)
        g_w_in = g_w_in + mm_tn(f["first_low"], d_hidden)
        g_b_in = g_b_in + jnp.sum(d_hidden.astype(jnp.float32), axis=0)
        d_first = d_second + mm_nt(d_hidden, w_in_f)
        d_first_in, d_g1, d_s1 = ln_backward(d_first, f["normed1"], f["inv1"], g1)
        g_vec[5] = g_vec[5] + d_g2
        g_vec[6] = g_vec[6] + d_s2
        g_vec[7] = g_vec[7] + jnp.sum(d_second, axis=0)
        g_vec[3] = g_vec[3] + d_g1
        g_vec[4] = g_vec[4] + d_s1
        g_vec[2] = g_vec[2] + jnp.sum(d_first_in, axis=0)
        firsts[s] = d_first_in

    def attention_backward(s):
        nonlocal g_wo_t, g_wq, g_wk, g_wv, prev_half
        f = fwd[s]
        d_first_in = firsts[s]
        d_branch = d_first_in.astype(jnp.bfloat16)
        if dx_gate:
            d_branch = d_branch + (prev_half[0, 0] * 0).astype(d_branch.dtype)
        g_wo_t = g_wo_t + mm_tn(d_branch, f["attended"])
        d_att = mm(d_branch, wo_t).astype(jnp.bfloat16)
        dq, dk, dv = attention_bwd(f["length"], f["q"], f["k"], f["v"], d_att, f["lse"], scale)
        g_wq = g_wq + mm_tn(tokens[s], dq)
        g_wk = g_wk + mm_tn(f["x_all"], dk)
        g_wv = g_wv + mm_tn(f["x_all"], dv)
        g_vec[0] = g_vec[0] + jnp.sum(dq.astype(jnp.float32), axis=0)
        g_vec[1] = g_vec[1] + jnp.sum(dv.astype(jnp.float32), axis=0)
        dx_kv = (mm_nt(dk, wk) + mm_nt(dv, wv)).reshape(2, seq_len // 2, width)
        dx_mine = lax.dynamic_index_in_dim(dx_kv, ctx_rank, axis=0, keepdims=False)
        dx_theirs = lax.dynamic_index_in_dim(dx_kv, 1 - ctx_rank, axis=0, keepdims=False).astype(jnp.bfloat16)
        dx_half = (dx_mine + ctx_swap(dx_theirs).astype(jnp.float32)).astype(jnp.bfloat16)
        dx_kv_own = lax.psum_scatter(dx_half, "tensor", scatter_dimension=0, tiled=True).astype(jnp.float32)
        dx_gate.append(dx_kv_own[0:1, 0:1])
        prev_half = dx_half
        d_tok = d_first_in + mm_nt(dq, wq) + dx_kv_own
        grad_tokens.append(d_tok.astype(jnp.bfloat16))


    prev_half = None
    for s in [0]:
        ffn_backward(s)
        attention_backward(s)
    for s in range(1, seqs):
        ffn_backward(s)
    for s in range(1, seqs):
        attention_backward(s)

    ffn_rep = jnp.concatenate([jnp.stack([g_vec[5], g_vec[6], g_vec[7]], axis=1), g_b_in.reshape(width, -1)], axis=1)
    attn_rep = jnp.stack(g_vec[0:5], axis=1)
    grad_w_in, grad_w_out_t, grad_wq, grad_wk, grad_wv, grad_wo_t, rep_out = reduce_rows(
        [g_w_in, g_w_out_t, g_wq, g_wk, g_wv, g_wo_t],
        jnp.concatenate([ffn_rep, attn_rep], axis=1),
        nt,
        gate=sum(dx_gate),
    )
    ffn_rep_out = rep_out[:, : ffn_rep.shape[1]]
    attn_rep_out = rep_out[:, ffn_rep.shape[1] :]

    return (
        jnp.stack(outputs),
        jnp.stack(grad_tokens),
        grad_wq,
        grad_wk,
        grad_wv,
        grad_wo_t.T,
        grad_w_in,
        grad_w_out_t.T,
        attn_rep_out[:, 0],
        attn_rep_out[:, 1],
        attn_rep_out[:, 2],
        attn_rep_out[:, 3],
        attn_rep_out[:, 4],
        ffn_rep_out[:, 0],
        ffn_rep_out[:, 1],
        ffn_rep_out[:, 2],
        ffn_rep_out[:, 3:].reshape(-1),
    )


def solution(mesh):
    row_spec = P("dp", ("ctx", "tensor"), None)
    w_rc = P(("dp", "ctx"), "tensor")
    w_cr = P("tensor", ("dp", "ctx"))
    vec = P(("dp", "ctx"))
    return jax.shard_map(
        body,
        mesh=mesh,
        in_specs=(row_spec, row_spec, P("dp"), w_rc, w_rc, w_rc, w_cr, w_rc, w_cr) + (vec,) * 9,
        out_specs=(row_spec, row_spec, w_rc, w_rc, w_rc, w_cr, w_rc, w_cr) + (vec,) * 9,
        check_vma=False,
    )
```

```python
import functools

import jax
import jax.numpy as jnp
from jax import lax
from jax.experimental import pallas as pl
from jax.experimental.pallas import tpu as pltpu
from jax.sharding import PartitionSpec as P

HD = 64
epsilon = 1e-05
masked_value = -1e30
ALL = ("dp", "ctx", "tensor")
SEQ_AXES = ("ctx", "tensor")


def exact_gelu(value):
    return jax.nn.gelu(value, approximate=False)


def mm(left, right):
    return jnp.dot(left, right, preferred_element_type=jnp.float32)


def mm_tn(left, right):
    return lax.dot_general(left, right, (((0,), (0,)), ((), ())), preferred_element_type=jnp.float32)


def mm_nt(left, right):
    return lax.dot_general(left, right, (((1,), (1,)), ((), ())), preferred_element_type=jnp.float32)


def ln_forward(hidden, gain, shift):
    mean = jnp.mean(hidden, axis=-1, keepdims=True)
    centre = hidden - mean
    var = jnp.mean(centre * centre, axis=-1, keepdims=True)
    inv = lax.rsqrt(var + epsilon)
    normed = centre * inv
    return normed * gain + shift, normed, inv


def ln_backward(grad_out, normed, inv, gain):
    d_normed = grad_out * gain
    width = normed.shape[-1]
    mean_d = jnp.sum(d_normed, axis=-1, keepdims=True) / width
    mean_dn = jnp.sum(d_normed * normed, axis=-1, keepdims=True) / width
    d_in = inv * (d_normed - mean_d - normed * mean_dn)
    d_gain = jnp.sum(grad_out * normed, axis=0)
    d_shift = jnp.sum(grad_out, axis=0)
    return d_in, d_gain, d_shift


KEY_BLOCK = 512


def _lane_masks(shape):
    lane = lax.broadcasted_iota(jnp.int32, shape, 1)
    return lane < HD, lane >= HD


def _nt(a, b):
    return lax.dot_general(a, b, (((1,), (1,)), ((), ())), preferred_element_type=jnp.float32)


def _tn(a, b):
    return lax.dot_general(a, b, (((0,), (0,)), ((), ())), preferred_element_type=jnp.float32)


def _attn_fwd_kernel(len_ref, q_ref, k_ref, v_ref, o_ref, lse_ref, s_buf, *, scale):
    length = len_ref[0]
    n_blocks = (length + KEY_BLOCK - 1) // KEY_BLOCK
    q = q_ref[...]
    rows = q.shape[0]
    in_a, in_b = _lane_masks(q.shape)
    zero = jnp.zeros_like(q)
    q_heads = (jnp.where(in_a, q, zero), jnp.where(in_b, q, zero))

    def pass_max(b, ms):
        start = pl.multiple_of(b * KEY_BLOCK, KEY_BLOCK)
        k_blk = k_ref[pl.ds(start, KEY_BLOCK), :]
        out = []
        for j in range(2):
            s = _nt(q_heads[j], k_blk) * scale
            pos = start + lax.broadcasted_iota(jnp.int32, s.shape, 1)
            s = jnp.where(pos < length, s, masked_value)
            s_buf[j, :, pl.ds(start, KEY_BLOCK)] = s
            out.append(jnp.maximum(ms[j], jnp.max(s, axis=1, keepdims=True)))
        return tuple(out)

    init = jnp.full((rows, 1), -jnp.inf, jnp.float32)
    ms = lax.fori_loop(0, n_blocks, pass_max, (init, init))

    def pass_sum(b, ls):
        start = pl.multiple_of(b * KEY_BLOCK, KEY_BLOCK)
        out = []
        for j in range(2):
            e = jnp.exp(s_buf[j, :, pl.ds(start, KEY_BLOCK)] - ms[j])
            s_buf[j, :, pl.ds(start, KEY_BLOCK)] = e
            out.append(ls[j] + jnp.sum(e, axis=1, keepdims=True))
        return tuple(out)

    zeros1 = jnp.zeros((rows, 1), jnp.float32)
    ls = lax.fori_loop(0, n_blocks, pass_sum, (zeros1, zeros1))

    def pass_out(b, acc):
        start = pl.multiple_of(b * KEY_BLOCK, KEY_BLOCK)
        v_blk = v_ref[pl.ds(start, KEY_BLOCK), :]
        vz = jnp.zeros_like(v_blk)
        in_a_v, in_b_v = _lane_masks(v_blk.shape)
        v_heads = (jnp.where(in_a_v, v_blk, vz), jnp.where(in_b_v, v_blk, vz))
        for j in range(2):
            probs = (s_buf[j, :, pl.ds(start, KEY_BLOCK)] / ls[j]).astype(jnp.bfloat16)
            acc = acc + jnp.dot(probs, v_heads[j], preferred_element_type=jnp.float32)
        return acc

    acc = lax.fori_loop(0, n_blocks, pass_out, jnp.zeros(q.shape, jnp.float32))
    o_ref[...] = acc.astype(o_ref.dtype)
    for j in range(2):
        lse_ref[0, j] = ms[j] + jnp.log(ls[j])


def attention_fwd(length, q, k, v, scale):
    rows, width = q.shape
    seq_len = k.shape[0]
    pairs = width // (2 * HD)
    kernel = functools.partial(_attn_fwd_kernel, scale=scale)
    return pl.pallas_call(
        kernel,
        out_shape=(
            jax.ShapeDtypeStruct((rows, width), jnp.bfloat16),
            jax.ShapeDtypeStruct((pairs, 2, rows, 1), jnp.float32),
        ),
        grid_spec=pltpu.PrefetchScalarGridSpec(
            num_scalar_prefetch=1,
            grid=(pairs,),
            in_specs=[
                pl.BlockSpec((rows, 2 * HD), lambda h, n: (0, h)),
                pl.BlockSpec((seq_len, 2 * HD), lambda h, n: (0, h)),
                pl.BlockSpec((seq_len, 2 * HD), lambda h, n: (0, h)),
            ],
            out_specs=[
                pl.BlockSpec((rows, 2 * HD), lambda h, n: (0, h)),
                pl.BlockSpec((1, 2, rows, 1), lambda h, n: (h, 0, 0, 0)),
            ],
            scratch_shapes=[pltpu.VMEM((2, rows, seq_len), jnp.float32)],
        ),
        cost_estimate=pl.CostEstimate(
            flops=8 * pairs * rows * seq_len * 2 * HD,
            transcendentals=2 * pairs * rows * seq_len,
            bytes_accessed=2 * (2 * q.size + k.size + v.size),
        ),
    )(length.reshape(1), q, k, v)


def _attn_bwd_kernel(len_ref, q_ref, k_ref, v_ref, do_ref, lse_ref, dq_ref, dk_ref, dv_ref, p_buf, dp_buf, *, scale):
    length = len_ref[0]
    n_blocks = (length + KEY_BLOCK - 1) // KEY_BLOCK
    total_blocks = k_ref.shape[0] // KEY_BLOCK
    q = q_ref[...]
    do = do_ref[...]
    rows = q.shape[0]
    in_a, in_b = _lane_masks(q.shape)
    zero = jnp.zeros_like(q)
    q_heads = (jnp.where(in_a, q, zero), jnp.where(in_b, q, zero))
    do_heads = (jnp.where(in_a, do, zero), jnp.where(in_b, do, zero))
    lses = (lse_ref[0, 0], lse_ref[0, 1])

    def pass_one(b, centres):
        start = pl.multiple_of(b * KEY_BLOCK, KEY_BLOCK)
        k_blk = k_ref[pl.ds(start, KEY_BLOCK), :]
        v_blk = v_ref[pl.ds(start, KEY_BLOCK), :]
        out = []
        for j in range(2):
            s = _nt(q_heads[j], k_blk) * scale
            pos = start + lax.broadcasted_iota(jnp.int32, s.shape, 1)
            s = jnp.where(pos < length, s, masked_value)
            p = jnp.exp(s - lses[j])
            dp = _nt(do_heads[j], v_blk)
            p_buf[j, :, pl.ds(start, KEY_BLOCK)] = p
            dp_buf[j, :, pl.ds(start, KEY_BLOCK)] = dp
            out.append(centres[j] + jnp.sum(p * dp, axis=1, keepdims=True))
        return tuple(out)

    zeros1 = jnp.zeros((rows, 1), jnp.float32)
    centres = lax.fori_loop(0, n_blocks, pass_one, (zeros1, zeros1))

    def pass_two(b, dq):
        start = pl.multiple_of(b * KEY_BLOCK, KEY_BLOCK)
        k_blk = k_ref[pl.ds(start, KEY_BLOCK), :]
        kz = jnp.zeros_like(k_blk)
        in_a_k, in_b_k = _lane_masks(k_blk.shape)
        k_heads = (jnp.where(in_a_k, k_blk, kz), jnp.where(in_b_k, k_blk, kz))
        dk = jnp.zeros(k_blk.shape, jnp.float32)
        dv = jnp.zeros(k_blk.shape, jnp.float32)
        for j in range(2):
            p = p_buf[j, :, pl.ds(start, KEY_BLOCK)]
            dp = dp_buf[j, :, pl.ds(start, KEY_BLOCK)]
            pos = start + lax.broadcasted_iota(jnp.int32, p.shape, 1)
            ds = jnp.where(pos < length, p * (dp - centres[j]), 0.0).astype(jnp.bfloat16)
            dk = dk + _tn(ds, q_heads[j])
            dv = dv + _tn(p.astype(jnp.bfloat16), do_heads[j])
            dq = dq + jnp.dot(ds, k_heads[j], preferred_element_type=jnp.float32)
        dk_ref[pl.ds(start, KEY_BLOCK), :] = (dk * scale).astype(dk_ref.dtype)
        dv_ref[pl.ds(start, KEY_BLOCK), :] = dv.astype(dv_ref.dtype)
        return dq

    dq = lax.fori_loop(0, n_blocks, pass_two, jnp.zeros(q.shape, jnp.float32))
    dq_ref[...] = (dq * scale).astype(dq_ref.dtype)

    def pass_zero(b, carry):
        start = pl.multiple_of(b * KEY_BLOCK, KEY_BLOCK)
        dk_ref[pl.ds(start, KEY_BLOCK), :] = jnp.zeros((KEY_BLOCK, q.shape[1]), dk_ref.dtype)
        dv_ref[pl.ds(start, KEY_BLOCK), :] = jnp.zeros((KEY_BLOCK, q.shape[1]), dv_ref.dtype)
        return carry

    lax.fori_loop(n_blocks, total_blocks, pass_zero, 0)


def attention_bwd(length, q, k, v, do, lse, scale):
    rows, width = q.shape
    seq_len = k.shape[0]
    pairs = width // (2 * HD)
    kernel = functools.partial(_attn_bwd_kernel, scale=scale)
    return pl.pallas_call(
        kernel,
        out_shape=(
            jax.ShapeDtypeStruct((rows, width), jnp.bfloat16),
            jax.ShapeDtypeStruct((seq_len, width), jnp.bfloat16),
            jax.ShapeDtypeStruct((seq_len, width), jnp.bfloat16),
        ),
        grid_spec=pltpu.PrefetchScalarGridSpec(
            num_scalar_prefetch=1,
            grid=(pairs,),
            in_specs=[
                pl.BlockSpec((rows, 2 * HD), lambda h, n: (0, h)),
                pl.BlockSpec((seq_len, 2 * HD), lambda h, n: (0, h)),
                pl.BlockSpec((seq_len, 2 * HD), lambda h, n: (0, h)),
                pl.BlockSpec((rows, 2 * HD), lambda h, n: (0, h)),
                pl.BlockSpec((1, 2, rows, 1), lambda h, n: (h, 0, 0, 0)),
            ],
            out_specs=[
                pl.BlockSpec((rows, 2 * HD), lambda h, n: (0, h)),
                pl.BlockSpec((seq_len, 2 * HD), lambda h, n: (0, h)),
                pl.BlockSpec((seq_len, 2 * HD), lambda h, n: (0, h)),
            ],
            scratch_shapes=[pltpu.VMEM((2, rows, seq_len), jnp.float32), pltpu.VMEM((2, rows, seq_len), jnp.float32)],
        ),
        cost_estimate=pl.CostEstimate(
            flops=20 * pairs * rows * seq_len * 2 * HD,
            transcendentals=2 * pairs * rows * seq_len,
            bytes_accessed=2 * (3 * q.size + 4 * k.size),
        ),
    )(length.reshape(1), q, k, v, do, lse)


def ctx_swap(x):
    return lax.ppermute(x, "ctx", [(0, 1), (1, 0)])


def pad_cols(x, multiple):
    cols = x.shape[1]
    padded = -(-cols // multiple) * multiple
    return jnp.pad(x, ((0, 0), (0, padded - cols)))


def gather_rows(pieces, replicated, nt):
    local = jnp.concatenate(pieces + [replicated], axis=1)
    width = local.shape[1]
    staged = lax.all_gather(local, "tensor", axis=1, tiled=True).reshape(local.shape[0], nt, width)
    parts, at = [], 0
    for p in pieces:
        parts.append(staged[:, :, at : at + p.shape[1]].reshape(local.shape[0], nt * p.shape[1]))
        at += p.shape[1]
    parts.append(staged[:, 0, at:])
    joined = jnp.concatenate(parts, axis=1)
    full = lax.all_gather(joined, ("dp", "ctx"), axis=0, tiled=True)
    out, at = [], 0
    for p in pieces:
        out.append(full[:, at : at + nt * p.shape[1]])
        at += nt * p.shape[1]
    out.append(full[:, at:])
    return out


def reduce_rows(pieces, replicated, nt, gate=None):
    if gate is not None:
        replicated = replicated + gate[0, 0] * 0
    width = sum(p.shape[1] for p in pieces) + replicated.shape[1]
    fill = jnp.zeros((replicated.shape[0], -(-width // 128) * 128 - width), replicated.dtype)
    local = jnp.concatenate(pieces + [replicated, fill], axis=1).astype(jnp.bfloat16)
    staged = lax.psum_scatter(local, ("dp", "ctx"), scatter_dimension=0, tiled=True)
    rb = staged.shape[0]
    parts, at = [], 0
    for p in pieces:
        c = p.shape[1] // nt
        parts.append(staged[:, at : at + p.shape[1]].reshape(rb, nt, c))
        at += p.shape[1]
    rep = staged[:, at:width]
    parts.append(jnp.broadcast_to(rep[:, None, :], (rb, nt, rep.shape[1])))
    slots = jnp.concatenate(parts, axis=2)
    slot_width = slots.shape[2]
    padded = -(-slot_width // 128) * 128
    slots = jnp.pad(slots, ((0, 0), (0, 0), (0, padded - slot_width))).transpose(1, 0, 2)
    own = lax.psum_scatter(slots, "tensor", scatter_dimension=0, tiled=True)[0].astype(jnp.float32)
    out, at = [], 0
    for p in pieces:
        c = p.shape[1] // nt
        out.append(own[:, at : at + c])
        at += c
    out.append(own[:, at : at + rep.shape[1]])
    return out


def body(
    tokens,
    cotangent,
    lengths,
    w_query,
    w_key,
    w_value,
    w_output,
    w_in,
    w_out,
    bias_query,
    bias_value,
    bias_output,
    gain_first,
    shift_first,
    gain_second,
    shift_second,
    bias_out,
    bias_in,
):
    seqs, local_rows, width = tokens.shape
    ctx_rank = lax.axis_index("ctx")
    tensor_rank = lax.axis_index("tensor")
    nt = lax.axis_size("tensor")
    chunk = ctx_rank * nt + tensor_rank
    seq_len = local_rows * lax.axis_size("ctx") * nt
    scale = HD ** (-0.5)
    rb = w_query.shape[0]
    hidden = w_in.shape[1] * nt

    attn_vec = jnp.stack([bias_query, bias_value, bias_output, gain_first, shift_first], axis=1)
    wq, wk, wv, wo_t, attn_vec = gather_rows([w_query, w_key, w_value, w_output.T], attn_vec, nt)
    ffn_vec = jnp.concatenate(
        [jnp.stack([gain_second, shift_second, bias_out], axis=1), bias_in.reshape(rb, -1)], axis=1
    )
    w_in_f, w_out_t, ffn_vec = gather_rows([w_in, w_out.T], ffn_vec, nt)
    attn_vec = attn_vec.astype(jnp.float32)
    ffn_vec = ffn_vec.astype(jnp.float32)
    b_q, b_v, b_o, g1, s1 = [attn_vec[:, i] for i in range(5)]
    g2, s2, b_out = [ffn_vec[:, i] for i in range(3)]
    b_in = ffn_vec[:, 3:].reshape(hidden)

    row_positions = chunk * local_rows + jnp.arange(local_rows, dtype=jnp.int32)

    fwd = []
    for s in range(seqs):
        x_own = tokens[s]
        length = lengths[s]
        x_all = lax.all_gather(x_own, SEQ_AXES, axis=0, tiled=True)
        q = (mm(x_own, wq) + b_q).astype(jnp.bfloat16)
        k = mm(x_all, wk).astype(jnp.bfloat16)
        v = (mm(x_all, wv) + b_v).astype(jnp.bfloat16)
        attended, lse = attention_fwd(length, q, k, v, scale)
        first_in = x_own.astype(jnp.float32) + (mm_nt(attended, wo_t) + b_o)
        first, normed1, inv1 = ln_forward(first_in, g1, s1)
        fwd.append(dict(x_all=x_all, q=q, k=k, v=v, lse=lse, attended=attended, first=first,
                        normed1=normed1, inv1=inv1, length=length))

    outputs = []
    for s in range(seqs):
        f = fwd[s]
        first_low = f["first"].astype(jnp.bfloat16)
        hidden_pre = mm(first_low, w_in_f) + b_in
        activated = exact_gelu(hidden_pre).astype(jnp.bfloat16)
        second_in = f["first"] + mm_nt(activated, w_out_t) + b_out
        result, normed2, inv2 = ln_forward(second_in, g2, s2)
        outputs.append(result.astype(jnp.bfloat16))
        f.update(first_low=first_low, hidden_pre=hidden_pre, activated=activated, normed2=normed2, inv2=inv2)

    g_w_in = jnp.zeros((width, hidden), jnp.float32)
    g_w_out_t = jnp.zeros((width, hidden), jnp.float32)
    g_b_in = jnp.zeros((hidden,), jnp.float32)
    g_vec = [jnp.zeros((width,), jnp.float32) for _ in range(8)]
    g_wq = jnp.zeros((width, width), jnp.float32)
    g_wk = jnp.zeros((width, width), jnp.float32)
    g_wv = jnp.zeros((width, width), jnp.float32)
    g_wo_t = jnp.zeros((width, width), jnp.float32)
    grad_tokens = []
    dx_gate = []
    firsts = {}

    def ffn_backward(s):
        nonlocal g_w_in, g_w_out_t, g_b_in
        f = fwd[s]
        row_valid = (row_positions < f["length"]).astype(jnp.float32)
        upstream = cotangent[s].astype(jnp.float32) * row_valid[:, None]
        if dx_gate:
            upstream = upstream + (prev_half[0, 0] * 0).astype(upstream.dtype)
        d_second, d_g2, d_s2 = ln_backward(upstream, f["normed2"], f["inv2"], g2)
        d_ffn = d_second.astype(jnp.bfloat16)
        g_w_out_t = g_w_out_t + mm_tn(d_ffn, f["activated"])
        d_act = mm(d_ffn, w_out_t)
        _, gelu_pull = jax.vjp(exact_gelu, f["hidden_pre"])
        d_hidden = gelu_pull(d_act)[0].astype(jnp.bfloat16)
        g_w_in = g_w_in + mm_tn(f["first_low"], d_hidden)
        g_b_in = g_b_in + jnp.sum(d_hidden.astype(jnp.float32), axis=0)
        d_first = d_second + mm_nt(d_hidden, w_in_f)
        d_first_in, d_g1, d_s1 = ln_backward(d_first, f["normed1"], f["inv1"], g1)
        g_vec[5] = g_vec[5] + d_g2
        g_vec[6] = g_vec[6] + d_s2
        g_vec[7] = g_vec[7] + jnp.sum(d_second, axis=0)
        g_vec[3] = g_vec[3] + d_g1
        g_vec[4] = g_vec[4] + d_s1
        g_vec[2] = g_vec[2] + jnp.sum(d_first_in, axis=0)
        firsts[s] = d_first_in

    def attention_backward(s):
        nonlocal g_wo_t, g_wq, g_wk, g_wv, prev_half
        f = fwd[s]
        d_first_in = firsts[s]
        d_branch = d_first_in.astype(jnp.bfloat16)
        if dx_gate:
            d_branch = d_branch + (prev_half[0, 0] * 0).astype(d_branch.dtype)
        g_wo_t = g_wo_t + mm_tn(d_branch, f["attended"])
        d_att = mm(d_branch, wo_t).astype(jnp.bfloat16)
        dq, dk, dv = attention_bwd(f["length"], f["q"], f["k"], f["v"], d_att, f["lse"], scale)
        g_wq = g_wq + mm_tn(tokens[s], dq)
        g_wk = g_wk + mm_tn(f["x_all"], dk)
        g_wv = g_wv + mm_tn(f["x_all"], dv)
        g_vec[0] = g_vec[0] + jnp.sum(dq.astype(jnp.float32), axis=0)
        g_vec[1] = g_vec[1] + jnp.sum(dv.astype(jnp.float32), axis=0)
        dx_kv = (mm_nt(dk, wk) + mm_nt(dv, wv)).reshape(2, seq_len // 2, width)
        dx_mine = lax.dynamic_index_in_dim(dx_kv, ctx_rank, axis=0, keepdims=False)
        dx_theirs = lax.dynamic_index_in_dim(dx_kv, 1 - ctx_rank, axis=0, keepdims=False).astype(jnp.bfloat16)
        dx_half = (dx_mine + ctx_swap(dx_theirs).astype(jnp.float32)).astype(jnp.bfloat16)
        dx_kv_own = lax.psum_scatter(dx_half, "tensor", scatter_dimension=0, tiled=True).astype(jnp.float32)
        dx_gate.append(dx_kv_own[0:1, 0:1])
        prev_half = dx_half
        d_tok = d_first_in + mm_nt(dq, wq) + dx_kv_own
        grad_tokens.append(d_tok.astype(jnp.bfloat16))


    prev_half = None
    for s in [0]:
        ffn_backward(s)
        attention_backward(s)
    for s in range(1, seqs):
        ffn_backward(s)
    for s in range(1, seqs):
        attention_backward(s)

    ffn_rep = jnp.concatenate([jnp.stack([g_vec[5], g_vec[6], g_vec[7]], axis=1), g_b_in.reshape(width, -1)], axis=1)
    attn_rep = jnp.stack(g_vec[0:5], axis=1)
    grad_w_in, grad_w_out_t, grad_wq, grad_wk, grad_wv, grad_wo_t, rep_out = reduce_rows(
        [g_w_in, g_w_out_t, g_wq, g_wk, g_wv, g_wo_t],
        jnp.concatenate([ffn_rep, attn_rep], axis=1),
        nt,
        gate=sum(dx_gate),
    )
    ffn_rep_out = rep_out[:, : ffn_rep.shape[1]]
    attn_rep_out = rep_out[:, ffn_rep.shape[1] :]

    return (
        jnp.stack(outputs),
        jnp.stack(grad_tokens),
        grad_wq,
        grad_wk,
        grad_wv,
        grad_wo_t.T,
        grad_w_in,
        grad_w_out_t.T,
        attn_rep_out[:, 0],
        attn_rep_out[:, 1],
        attn_rep_out[:, 2],
        attn_rep_out[:, 3],
        attn_rep_out[:, 4],
        ffn_rep_out[:, 0],
        ffn_rep_out[:, 1],
        ffn_rep_out[:, 2],
        ffn_rep_out[:, 3:].reshape(-1),
    )


def solution(mesh):
    row_spec = P("dp", ("ctx", "tensor"), None)
    w_rc = P(("dp", "ctx"), "tensor")
    w_cr = P("tensor", ("dp", "ctx"))
    vec = P(("dp", "ctx"))
    return jax.shard_map(
        body,
        mesh=mesh,
        in_specs=(row_spec, row_spec, P("dp"), w_rc, w_rc, w_rc, w_cr, w_rc, w_cr) + (vec,) * 9,
        out_specs=(row_spec, row_spec, w_rc, w_rc, w_rc, w_cr, w_rc, w_cr) + (vec,) * 9,
        check_vma=False,
    )
```

```python
import functools

import jax
import jax.numpy as jnp
from jax import lax
from jax.experimental import pallas as pl
from jax.experimental.pallas import tpu as pltpu
from jax.sharding import PartitionSpec as P

HD = 64
epsilon = 1e-05
masked_value = -1e30
ALL = ("dp", "ctx", "tensor")
SEQ_AXES = ("ctx", "tensor")


def exact_gelu(value):
    return jax.nn.gelu(value, approximate=False)


def mm(left, right):
    return jnp.dot(left, right, preferred_element_type=jnp.float32)


def mm_tn(left, right):
    return lax.dot_general(left, right, (((0,), (0,)), ((), ())), preferred_element_type=jnp.float32)


def mm_nt(left, right):
    return lax.dot_general(left, right, (((1,), (1,)), ((), ())), preferred_element_type=jnp.float32)


def ln_forward(hidden, gain, shift):
    mean = jnp.mean(hidden, axis=-1, keepdims=True)
    centre = hidden - mean
    var = jnp.mean(centre * centre, axis=-1, keepdims=True)
    inv = lax.rsqrt(var + epsilon)
    normed = centre * inv
    return normed * gain + shift, normed, inv


def ln_backward(grad_out, normed, inv, gain):
    d_normed = grad_out * gain
    width = normed.shape[-1]
    mean_d = jnp.sum(d_normed, axis=-1, keepdims=True) / width
    mean_dn = jnp.sum(d_normed * normed, axis=-1, keepdims=True) / width
    d_in = inv * (d_normed - mean_d - normed * mean_dn)
    d_gain = jnp.sum(grad_out * normed, axis=0)
    d_shift = jnp.sum(grad_out, axis=0)
    return d_in, d_gain, d_shift


KEY_BLOCK = 512


def _lane_masks(shape):
    lane = lax.broadcasted_iota(jnp.int32, shape, 1)
    return lane < HD, lane >= HD


def _nt(a, b):
    return lax.dot_general(a, b, (((1,), (1,)), ((), ())), preferred_element_type=jnp.float32)


def _tn(a, b):
    return lax.dot_general(a, b, (((0,), (0,)), ((), ())), preferred_element_type=jnp.float32)


def _attn_fwd_kernel(len_ref, q_ref, k_ref, v_ref, o_ref, lse_ref, s_buf, *, scale):
    length = len_ref[0]
    n_blocks = (length + KEY_BLOCK - 1) // KEY_BLOCK
    q = q_ref[...]
    rows = q.shape[0]
    in_a, in_b = _lane_masks(q.shape)
    zero = jnp.zeros_like(q)
    q_heads = (jnp.where(in_a, q, zero), jnp.where(in_b, q, zero))

    def pass_max(b, ms):
        start = pl.multiple_of(b * KEY_BLOCK, KEY_BLOCK)
        k_blk = k_ref[pl.ds(start, KEY_BLOCK), :]
        out = []
        for j in range(2):
            s = _nt(q_heads[j], k_blk) * scale
            pos = start + lax.broadcasted_iota(jnp.int32, s.shape, 1)
            s = jnp.where(pos < length, s, masked_value)
            s_buf[j, :, pl.ds(start, KEY_BLOCK)] = s
            out.append(jnp.maximum(ms[j], jnp.max(s, axis=1, keepdims=True)))
        return tuple(out)

    init = jnp.full((rows, 1), -jnp.inf, jnp.float32)
    ms = lax.fori_loop(0, n_blocks, pass_max, (init, init))

    def pass_sum(b, ls):
        start = pl.multiple_of(b * KEY_BLOCK, KEY_BLOCK)
        out = []
        for j in range(2):
            e = jnp.exp(s_buf[j, :, pl.ds(start, KEY_BLOCK)] - ms[j])
            s_buf[j, :, pl.ds(start, KEY_BLOCK)] = e
            out.append(ls[j] + jnp.sum(e, axis=1, keepdims=True))
        return tuple(out)

    zeros1 = jnp.zeros((rows, 1), jnp.float32)
    ls = lax.fori_loop(0, n_blocks, pass_sum, (zeros1, zeros1))

    def pass_out(b, acc):
        start = pl.multiple_of(b * KEY_BLOCK, KEY_BLOCK)
        v_blk = v_ref[pl.ds(start, KEY_BLOCK), :]
        vz = jnp.zeros_like(v_blk)
        in_a_v, in_b_v = _lane_masks(v_blk.shape)
        v_heads = (jnp.where(in_a_v, v_blk, vz), jnp.where(in_b_v, v_blk, vz))
        for j in range(2):
            probs = (s_buf[j, :, pl.ds(start, KEY_BLOCK)] / ls[j]).astype(jnp.bfloat16)
            acc = acc + jnp.dot(probs, v_heads[j], preferred_element_type=jnp.float32)
        return acc

    acc = lax.fori_loop(0, n_blocks, pass_out, jnp.zeros(q.shape, jnp.float32))
    o_ref[...] = acc.astype(o_ref.dtype)
    for j in range(2):
        lse_ref[0, j] = ms[j] + jnp.log(ls[j])


def attention_fwd(length, q, k, v, scale):
    rows, width = q.shape
    seq_len = k.shape[0]
    pairs = width // (2 * HD)
    kernel = functools.partial(_attn_fwd_kernel, scale=scale)
    return pl.pallas_call(
        kernel,
        out_shape=(
            jax.ShapeDtypeStruct((rows, width), jnp.bfloat16),
            jax.ShapeDtypeStruct((pairs, 2, rows, 1), jnp.float32),
        ),
        grid_spec=pltpu.PrefetchScalarGridSpec(
            num_scalar_prefetch=1,
            grid=(pairs,),
            in_specs=[
                pl.BlockSpec((rows, 2 * HD), lambda h, n: (0, h)),
                pl.BlockSpec((seq_len, 2 * HD), lambda h, n: (0, h)),
                pl.BlockSpec((seq_len, 2 * HD), lambda h, n: (0, h)),
            ],
            out_specs=[
                pl.BlockSpec((rows, 2 * HD), lambda h, n: (0, h)),
                pl.BlockSpec((1, 2, rows, 1), lambda h, n: (h, 0, 0, 0)),
            ],
            scratch_shapes=[pltpu.VMEM((2, rows, seq_len), jnp.float32)],
        ),
        cost_estimate=pl.CostEstimate(
            flops=8 * pairs * rows * seq_len * 2 * HD,
            transcendentals=2 * pairs * rows * seq_len,
            bytes_accessed=2 * (2 * q.size + k.size + v.size),
        ),
    )(length.reshape(1), q, k, v)


def _attn_bwd_kernel(len_ref, q_ref, k_ref, v_ref, do_ref, lse_ref, dq_ref, dk_ref, dv_ref, p_buf, dp_buf, *, scale):
    length = len_ref[0]
    n_blocks = (length + KEY_BLOCK - 1) // KEY_BLOCK
    total_blocks = k_ref.shape[0] // KEY_BLOCK
    q = q_ref[...]
    do = do_ref[...]
    rows = q.shape[0]
    in_a, in_b = _lane_masks(q.shape)
    zero = jnp.zeros_like(q)
    q_heads = (jnp.where(in_a, q, zero), jnp.where(in_b, q, zero))
    do_heads = (jnp.where(in_a, do, zero), jnp.where(in_b, do, zero))
    lses = (lse_ref[0, 0], lse_ref[0, 1])

    def pass_one(b, centres):
        start = pl.multiple_of(b * KEY_BLOCK, KEY_BLOCK)
        k_blk = k_ref[pl.ds(start, KEY_BLOCK), :]
        v_blk = v_ref[pl.ds(start, KEY_BLOCK), :]
        out = []
        for j in range(2):
            s = _nt(q_heads[j], k_blk) * scale
            pos = start + lax.broadcasted_iota(jnp.int32, s.shape, 1)
            s = jnp.where(pos < length, s, masked_value)
            p = jnp.exp(s - lses[j])
            dp = _nt(do_heads[j], v_blk)
            p_buf[j, :, pl.ds(start, KEY_BLOCK)] = p
            dp_buf[j, :, pl.ds(start, KEY_BLOCK)] = dp
            out.append(centres[j] + jnp.sum(p * dp, axis=1, keepdims=True))
        return tuple(out)

    zeros1 = jnp.zeros((rows, 1), jnp.float32)
    centres = lax.fori_loop(0, n_blocks, pass_one, (zeros1, zeros1))

    def pass_two(b, dq):
        start = pl.multiple_of(b * KEY_BLOCK, KEY_BLOCK)
        k_blk = k_ref[pl.ds(start, KEY_BLOCK), :]
        kz = jnp.zeros_like(k_blk)
        in_a_k, in_b_k = _lane_masks(k_blk.shape)
        k_heads = (jnp.where(in_a_k, k_blk, kz), jnp.where(in_b_k, k_blk, kz))
        dk = jnp.zeros(k_blk.shape, jnp.float32)
        dv = jnp.zeros(k_blk.shape, jnp.float32)
        for j in range(2):
            p = p_buf[j, :, pl.ds(start, KEY_BLOCK)]
            dp = dp_buf[j, :, pl.ds(start, KEY_BLOCK)]
            pos = start + lax.broadcasted_iota(jnp.int32, p.shape, 1)
            ds = jnp.where(pos < length, p * (dp - centres[j]), 0.0).astype(jnp.bfloat16)
            dk = dk + _tn(ds, q_heads[j])
            dv = dv + _tn(p.astype(jnp.bfloat16), do_heads[j])
            dq = dq + jnp.dot(ds, k_heads[j], preferred_element_type=jnp.float32)
        dk_ref[pl.ds(start, KEY_BLOCK), :] = (dk * scale).astype(dk_ref.dtype)
        dv_ref[pl.ds(start, KEY_BLOCK), :] = dv.astype(dv_ref.dtype)
        return dq

    dq = lax.fori_loop(0, n_blocks, pass_two, jnp.zeros(q.shape, jnp.float32))
    dq_ref[...] = (dq * scale).astype(dq_ref.dtype)

    def pass_zero(b, carry):
        start = pl.multiple_of(b * KEY_BLOCK, KEY_BLOCK)
        dk_ref[pl.ds(start, KEY_BLOCK), :] = jnp.zeros((KEY_BLOCK, q.shape[1]), dk_ref.dtype)
        dv_ref[pl.ds(start, KEY_BLOCK), :] = jnp.zeros((KEY_BLOCK, q.shape[1]), dv_ref.dtype)
        return carry

    lax.fori_loop(n_blocks, total_blocks, pass_zero, 0)


def attention_bwd(length, q, k, v, do, lse, scale):
    rows, width = q.shape
    seq_len = k.shape[0]
    pairs = width // (2 * HD)
    kernel = functools.partial(_attn_bwd_kernel, scale=scale)
    return pl.pallas_call(
        kernel,
        out_shape=(
            jax.ShapeDtypeStruct((rows, width), jnp.bfloat16),
            jax.ShapeDtypeStruct((seq_len, width), jnp.bfloat16),
            jax.ShapeDtypeStruct((seq_len, width), jnp.bfloat16),
        ),
        grid_spec=pltpu.PrefetchScalarGridSpec(
            num_scalar_prefetch=1,
            grid=(pairs,),
            in_specs=[
                pl.BlockSpec((rows, 2 * HD), lambda h, n: (0, h)),
                pl.BlockSpec((seq_len, 2 * HD), lambda h, n: (0, h)),
                pl.BlockSpec((seq_len, 2 * HD), lambda h, n: (0, h)),
                pl.BlockSpec((rows, 2 * HD), lambda h, n: (0, h)),
                pl.BlockSpec((1, 2, rows, 1), lambda h, n: (h, 0, 0, 0)),
            ],
            out_specs=[
                pl.BlockSpec((rows, 2 * HD), lambda h, n: (0, h)),
                pl.BlockSpec((seq_len, 2 * HD), lambda h, n: (0, h)),
                pl.BlockSpec((seq_len, 2 * HD), lambda h, n: (0, h)),
            ],
            scratch_shapes=[pltpu.VMEM((2, rows, seq_len), jnp.float32), pltpu.VMEM((2, rows, seq_len), jnp.float32)],
        ),
        cost_estimate=pl.CostEstimate(
            flops=20 * pairs * rows * seq_len * 2 * HD,
            transcendentals=2 * pairs * rows * seq_len,
            bytes_accessed=2 * (3 * q.size + 4 * k.size),
        ),
    )(length.reshape(1), q, k, v, do, lse)


def ctx_swap(x):
    return lax.ppermute(x, "ctx", [(0, 1), (1, 0)])


def pad_cols(x, multiple):
    cols = x.shape[1]
    padded = -(-cols // multiple) * multiple
    return jnp.pad(x, ((0, 0), (0, padded - cols)))


def gather_rows(pieces, replicated, nt):
    local = jnp.concatenate(pieces + [replicated], axis=1)
    width = local.shape[1]
    staged = lax.all_gather(local, "tensor", axis=1, tiled=True).reshape(local.shape[0], nt, width)
    parts, at = [], 0
    for p in pieces:
        parts.append(staged[:, :, at : at + p.shape[1]].reshape(local.shape[0], nt * p.shape[1]))
        at += p.shape[1]
    parts.append(staged[:, 0, at:])
    joined = jnp.concatenate(parts, axis=1)
    full = lax.all_gather(joined, ("dp", "ctx"), axis=0, tiled=True)
    out, at = [], 0
    for p in pieces:
        out.append(full[:, at : at + nt * p.shape[1]])
        at += nt * p.shape[1]
    out.append(full[:, at:])
    return out


def reduce_rows(pieces, replicated, nt, gate=None):
    width = sum(p.shape[1] for p in pieces) + replicated.shape[1]
    fill = jnp.zeros((replicated.shape[0], -(-width // 128) * 128 - width), replicated.dtype)
    local = jnp.concatenate(pieces + [replicated, fill], axis=1).astype(jnp.bfloat16)
    if gate is not None:
        local = local.at[0, width].add((gate[0, 0] * 0).astype(local.dtype))
    staged = lax.psum_scatter(local, ("dp", "ctx"), scatter_dimension=0, tiled=True)
    rb = staged.shape[0]
    parts, at = [], 0
    for p in pieces:
        c = p.shape[1] // nt
        parts.append(staged[:, at : at + p.shape[1]].reshape(rb, nt, c))
        at += p.shape[1]
    rep = staged[:, at:width]
    parts.append(jnp.broadcast_to(rep[:, None, :], (rb, nt, rep.shape[1])))
    slots = jnp.concatenate(parts, axis=2)
    slot_width = slots.shape[2]
    padded = -(-slot_width // 128) * 128
    slots = jnp.pad(slots, ((0, 0), (0, 0), (0, padded - slot_width))).transpose(1, 0, 2)
    own = lax.psum_scatter(slots, "tensor", scatter_dimension=0, tiled=True)[0].astype(jnp.float32)
    out, at = [], 0
    for p in pieces:
        c = p.shape[1] // nt
        out.append(own[:, at : at + c])
        at += c
    out.append(own[:, at : at + rep.shape[1]])
    return out


def body(
    tokens,
    cotangent,
    lengths,
    w_query,
    w_key,
    w_value,
    w_output,
    w_in,
    w_out,
    bias_query,
    bias_value,
    bias_output,
    gain_first,
    shift_first,
    gain_second,
    shift_second,
    bias_out,
    bias_in,
):
    seqs, local_rows, width = tokens.shape
    ctx_rank = lax.axis_index("ctx")
    tensor_rank = lax.axis_index("tensor")
    nt = lax.axis_size("tensor")
    chunk = ctx_rank * nt + tensor_rank
    seq_len = local_rows * lax.axis_size("ctx") * nt
    scale = HD ** (-0.5)
    rb = w_query.shape[0]
    hidden = w_in.shape[1] * nt

    attn_vec = jnp.stack([bias_query, bias_value, bias_output, gain_first, shift_first], axis=1)
    wq, wk, wv, wo_t, attn_vec = gather_rows([w_query, w_key, w_value, w_output.T], attn_vec, nt)
    ffn_vec = jnp.concatenate(
        [jnp.stack([gain_second, shift_second, bias_out], axis=1), bias_in.reshape(rb, -1)], axis=1
    )
    w_in_f, w_out_t, ffn_vec = gather_rows([w_in, w_out.T], ffn_vec, nt)
    attn_vec = attn_vec.astype(jnp.float32)
    ffn_vec = ffn_vec.astype(jnp.float32)
    b_q, b_v, b_o, g1, s1 = [attn_vec[:, i] for i in range(5)]
    g2, s2, b_out = [ffn_vec[:, i] for i in range(3)]
    b_in = ffn_vec[:, 3:].reshape(hidden)

    row_positions = chunk * local_rows + jnp.arange(local_rows, dtype=jnp.int32)

    fwd = []
    for s in range(seqs):
        x_own = tokens[s]
        length = lengths[s]
        x_all = lax.all_gather(x_own, SEQ_AXES, axis=0, tiled=True)
        q = (mm(x_own, wq) + b_q).astype(jnp.bfloat16)
        k = mm(x_all, wk).astype(jnp.bfloat16)
        v = (mm(x_all, wv) + b_v).astype(jnp.bfloat16)
        attended, lse = attention_fwd(length, q, k, v, scale)
        first_in = x_own.astype(jnp.float32) + (mm_nt(attended, wo_t) + b_o)
        first, normed1, inv1 = ln_forward(first_in, g1, s1)
        fwd.append(dict(x_all=x_all, q=q, k=k, v=v, lse=lse, attended=attended, first=first,
                        normed1=normed1, inv1=inv1, length=length))

    outputs = []
    for s in range(seqs):
        f = fwd[s]
        first_low = f["first"].astype(jnp.bfloat16)
        hidden_pre = mm(first_low, w_in_f) + b_in
        activated = exact_gelu(hidden_pre).astype(jnp.bfloat16)
        second_in = f["first"] + mm_nt(activated, w_out_t) + b_out
        result, normed2, inv2 = ln_forward(second_in, g2, s2)
        outputs.append(result.astype(jnp.bfloat16))
        f.update(first_low=first_low, hidden_pre=hidden_pre, activated=activated, normed2=normed2, inv2=inv2)

    g_w_in = jnp.zeros((width, hidden), jnp.float32)
    g_w_out_t = jnp.zeros((width, hidden), jnp.float32)
    g_b_in = jnp.zeros((hidden,), jnp.float32)
    g_vec = [jnp.zeros((width,), jnp.float32) for _ in range(8)]
    g_wq = jnp.zeros((width, width), jnp.float32)
    g_wk = jnp.zeros((width, width), jnp.float32)
    g_wv = jnp.zeros((width, width), jnp.float32)
    g_wo_t = jnp.zeros((width, width), jnp.float32)
    grad_tokens = []
    dx_gate = []
    firsts = {}

    def ffn_backward(s):
        nonlocal g_w_in, g_w_out_t, g_b_in
        f = fwd[s]
        row_valid = (row_positions < f["length"]).astype(jnp.float32)
        upstream = cotangent[s].astype(jnp.float32) * row_valid[:, None]
        if dx_gate:
            upstream = upstream + (prev_half[0, 0] * 0).astype(upstream.dtype)
        d_second, d_g2, d_s2 = ln_backward(upstream, f["normed2"], f["inv2"], g2)
        d_ffn = d_second.astype(jnp.bfloat16)
        g_w_out_t = g_w_out_t + mm_tn(d_ffn, f["activated"])
        d_act = mm(d_ffn, w_out_t)
        _, gelu_pull = jax.vjp(exact_gelu, f["hidden_pre"])
        d_hidden = gelu_pull(d_act)[0].astype(jnp.bfloat16)
        g_w_in = g_w_in + mm_tn(f["first_low"], d_hidden)
        g_b_in = g_b_in + jnp.sum(d_hidden.astype(jnp.float32), axis=0)
        d_first = d_second + mm_nt(d_hidden, w_in_f)
        d_first_in, d_g1, d_s1 = ln_backward(d_first, f["normed1"], f["inv1"], g1)
        g_vec[5] = g_vec[5] + d_g2
        g_vec[6] = g_vec[6] + d_s2
        g_vec[7] = g_vec[7] + jnp.sum(d_second, axis=0)
        g_vec[3] = g_vec[3] + d_g1
        g_vec[4] = g_vec[4] + d_s1
        g_vec[2] = g_vec[2] + jnp.sum(d_first_in, axis=0)
        firsts[s] = d_first_in

    def attention_backward(s):
        nonlocal g_wo_t, g_wq, g_wk, g_wv, prev_half
        f = fwd[s]
        d_first_in = firsts[s]
        d_branch = d_first_in.astype(jnp.bfloat16)
        if dx_gate:
            d_branch = d_branch + (prev_half[0, 0] * 0).astype(d_branch.dtype)
        g_wo_t = g_wo_t + mm_tn(d_branch, f["attended"])
        d_att = mm(d_branch, wo_t).astype(jnp.bfloat16)
        dq, dk, dv = attention_bwd(f["length"], f["q"], f["k"], f["v"], d_att, f["lse"], scale)
        g_wq = g_wq + mm_tn(tokens[s], dq)
        g_wk = g_wk + mm_tn(f["x_all"], dk)
        g_wv = g_wv + mm_tn(f["x_all"], dv)
        g_vec[0] = g_vec[0] + jnp.sum(dq.astype(jnp.float32), axis=0)
        g_vec[1] = g_vec[1] + jnp.sum(dv.astype(jnp.float32), axis=0)
        dx_kv = (mm_nt(dk, wk) + mm_nt(dv, wv)).reshape(2, seq_len // 2, width)
        dx_mine = lax.dynamic_index_in_dim(dx_kv, ctx_rank, axis=0, keepdims=False)
        dx_theirs = lax.dynamic_index_in_dim(dx_kv, 1 - ctx_rank, axis=0, keepdims=False).astype(jnp.bfloat16)
        dx_half = (dx_mine + ctx_swap(dx_theirs).astype(jnp.float32)).astype(jnp.bfloat16)
        dx_kv_own = lax.psum_scatter(dx_half, "tensor", scatter_dimension=0, tiled=True).astype(jnp.float32)
        dx_gate.append(dx_kv_own[0:1, 0:1])
        prev_half = dx_half
        d_tok = d_first_in + mm_nt(dq, wq) + dx_kv_own
        grad_tokens.append(d_tok.astype(jnp.bfloat16))


    prev_half = None
    for s in [0]:
        ffn_backward(s)
        attention_backward(s)
    for s in range(1, seqs):
        ffn_backward(s)
    for s in range(1, seqs):
        attention_backward(s)

    ffn_rep = jnp.concatenate([jnp.stack([g_vec[5], g_vec[6], g_vec[7]], axis=1), g_b_in.reshape(width, -1)], axis=1)
    attn_rep = jnp.stack(g_vec[0:5], axis=1)
    grad_w_in, grad_w_out_t, grad_wq, grad_wk, grad_wv, grad_wo_t, rep_out = reduce_rows(
        [g_w_in, g_w_out_t, g_wq, g_wk, g_wv, g_wo_t],
        jnp.concatenate([ffn_rep, attn_rep], axis=1),
        nt,
        gate=sum(dx_gate),
    )
    ffn_rep_out = rep_out[:, : ffn_rep.shape[1]]
    attn_rep_out = rep_out[:, ffn_rep.shape[1] :]

    return (
        jnp.stack(outputs),
        jnp.stack(grad_tokens),
        grad_wq,
        grad_wk,
        grad_wv,
        grad_wo_t.T,
        grad_w_in,
        grad_w_out_t.T,
        attn_rep_out[:, 0],
        attn_rep_out[:, 1],
        attn_rep_out[:, 2],
        attn_rep_out[:, 3],
        attn_rep_out[:, 4],
        ffn_rep_out[:, 0],
        ffn_rep_out[:, 1],
        ffn_rep_out[:, 2],
        ffn_rep_out[:, 3:].reshape(-1),
    )


def solution(mesh):
    row_spec = P("dp", ("ctx", "tensor"), None)
    w_rc = P(("dp", "ctx"), "tensor")
    w_cr = P("tensor", ("dp", "ctx"))
    vec = P(("dp", "ctx"))
    return jax.shard_map(
        body,
        mesh=mesh,
        in_specs=(row_spec, row_spec, P("dp"), w_rc, w_rc, w_rc, w_cr, w_rc, w_cr) + (vec,) * 9,
        out_specs=(row_spec, row_spec, w_rc, w_rc, w_rc, w_cr, w_rc, w_cr) + (vec,) * 9,
        check_vma=False,
    )
```

```python
import functools

import jax
import jax.numpy as jnp
from jax import lax
from jax.experimental import pallas as pl
from jax.experimental.pallas import tpu as pltpu
from jax.sharding import PartitionSpec as P

HD = 64
epsilon = 1e-05
masked_value = -1e30
ALL = ("dp", "ctx", "tensor")
SEQ_AXES = ("ctx", "tensor")


def exact_gelu(value):
    return jax.nn.gelu(value, approximate=False)


def mm(left, right):
    return jnp.dot(left, right, preferred_element_type=jnp.float32)


def mm_tn(left, right):
    return lax.dot_general(left, right, (((0,), (0,)), ((), ())), preferred_element_type=jnp.float32)


def mm_nt(left, right):
    return lax.dot_general(left, right, (((1,), (1,)), ((), ())), preferred_element_type=jnp.float32)


def ln_forward(hidden, gain, shift):
    mean = jnp.mean(hidden, axis=-1, keepdims=True)
    centre = hidden - mean
    var = jnp.mean(centre * centre, axis=-1, keepdims=True)
    inv = lax.rsqrt(var + epsilon)
    normed = centre * inv
    return normed * gain + shift, normed, inv


def ln_backward(grad_out, normed, inv, gain):
    d_normed = grad_out * gain
    width = normed.shape[-1]
    mean_d = jnp.sum(d_normed, axis=-1, keepdims=True) / width
    mean_dn = jnp.sum(d_normed * normed, axis=-1, keepdims=True) / width
    d_in = inv * (d_normed - mean_d - normed * mean_dn)
    d_gain = jnp.sum(grad_out * normed, axis=0)
    d_shift = jnp.sum(grad_out, axis=0)
    return d_in, d_gain, d_shift


KEY_BLOCK = 512


def _lane_masks(shape):
    lane = lax.broadcasted_iota(jnp.int32, shape, 1)
    return lane < HD, lane >= HD


def _nt(a, b):
    return lax.dot_general(a, b, (((1,), (1,)), ((), ())), preferred_element_type=jnp.float32)


def _tn(a, b):
    return lax.dot_general(a, b, (((0,), (0,)), ((), ())), preferred_element_type=jnp.float32)


def _attn_fwd_kernel(len_ref, q_ref, k_ref, v_ref, o_ref, lse_ref, s_buf, *, scale):
    length = len_ref[0]
    n_blocks = (length + KEY_BLOCK - 1) // KEY_BLOCK
    q = q_ref[...]
    rows = q.shape[0]
    in_a, in_b = _lane_masks(q.shape)
    zero = jnp.zeros_like(q)
    q_heads = (jnp.where(in_a, q, zero), jnp.where(in_b, q, zero))

    def pass_max(b, ms):
        start = pl.multiple_of(b * KEY_BLOCK, KEY_BLOCK)
        k_blk = k_ref[pl.ds(start, KEY_BLOCK), :]
        out = []
        for j in range(2):
            s = _nt(q_heads[j], k_blk) * scale
            pos = start + lax.broadcasted_iota(jnp.int32, s.shape, 1)
            s = jnp.where(pos < length, s, masked_value)
            s_buf[j, :, pl.ds(start, KEY_BLOCK)] = s
            out.append(jnp.maximum(ms[j], jnp.max(s, axis=1, keepdims=True)))
        return tuple(out)

    init = jnp.full((rows, 1), -jnp.inf, jnp.float32)
    ms = lax.fori_loop(0, n_blocks, pass_max, (init, init))

    def pass_sum(b, ls):
        start = pl.multiple_of(b * KEY_BLOCK, KEY_BLOCK)
        out = []
        for j in range(2):
            e = jnp.exp(s_buf[j, :, pl.ds(start, KEY_BLOCK)] - ms[j])
            s_buf[j, :, pl.ds(start, KEY_BLOCK)] = e
            out.append(ls[j] + jnp.sum(e, axis=1, keepdims=True))
        return tuple(out)

    zeros1 = jnp.zeros((rows, 1), jnp.float32)
    ls = lax.fori_loop(0, n_blocks, pass_sum, (zeros1, zeros1))

    def pass_out(b, acc):
        start = pl.multiple_of(b * KEY_BLOCK, KEY_BLOCK)
        v_blk = v_ref[pl.ds(start, KEY_BLOCK), :]
        vz = jnp.zeros_like(v_blk)
        in_a_v, in_b_v = _lane_masks(v_blk.shape)
        v_heads = (jnp.where(in_a_v, v_blk, vz), jnp.where(in_b_v, v_blk, vz))
        for j in range(2):
            probs = (s_buf[j, :, pl.ds(start, KEY_BLOCK)] / ls[j]).astype(jnp.bfloat16)
            acc = acc + jnp.dot(probs, v_heads[j], preferred_element_type=jnp.float32)
        return acc

    acc = lax.fori_loop(0, n_blocks, pass_out, jnp.zeros(q.shape, jnp.float32))
    o_ref[...] = acc.astype(o_ref.dtype)
    for j in range(2):
        lse_ref[0, j] = ms[j] + jnp.log(ls[j])


def attention_fwd(length, q, k, v, scale):
    rows, width = q.shape
    seq_len = k.shape[0]
    pairs = width // (2 * HD)
    kernel = functools.partial(_attn_fwd_kernel, scale=scale)
    return pl.pallas_call(
        kernel,
        out_shape=(
            jax.ShapeDtypeStruct((rows, width), jnp.bfloat16),
            jax.ShapeDtypeStruct((pairs, 2, rows, 1), jnp.float32),
        ),
        grid_spec=pltpu.PrefetchScalarGridSpec(
            num_scalar_prefetch=1,
            grid=(pairs,),
            in_specs=[
                pl.BlockSpec((rows, 2 * HD), lambda h, n: (0, h)),
                pl.BlockSpec((seq_len, 2 * HD), lambda h, n: (0, h)),
                pl.BlockSpec((seq_len, 2 * HD), lambda h, n: (0, h)),
            ],
            out_specs=[
                pl.BlockSpec((rows, 2 * HD), lambda h, n: (0, h)),
                pl.BlockSpec((1, 2, rows, 1), lambda h, n: (h, 0, 0, 0)),
            ],
            scratch_shapes=[pltpu.VMEM((2, rows, seq_len), jnp.float32)],
        ),
        cost_estimate=pl.CostEstimate(
            flops=8 * pairs * rows * seq_len * 2 * HD,
            transcendentals=2 * pairs * rows * seq_len,
            bytes_accessed=2 * (2 * q.size + k.size + v.size),
        ),
    )(length.reshape(1), q, k, v)


def _attn_bwd_kernel(len_ref, q_ref, k_ref, v_ref, do_ref, lse_ref, dq_ref, dk_ref, dv_ref, p_buf, dp_buf, *, scale):
    length = len_ref[0]
    n_blocks = (length + KEY_BLOCK - 1) // KEY_BLOCK
    total_blocks = k_ref.shape[0] // KEY_BLOCK
    q = q_ref[...]
    do = do_ref[...]
    rows = q.shape[0]
    in_a, in_b = _lane_masks(q.shape)
    zero = jnp.zeros_like(q)
    q_heads = (jnp.where(in_a, q, zero), jnp.where(in_b, q, zero))
    do_heads = (jnp.where(in_a, do, zero), jnp.where(in_b, do, zero))
    lses = (lse_ref[0, 0], lse_ref[0, 1])

    def pass_one(b, centres):
        start = pl.multiple_of(b * KEY_BLOCK, KEY_BLOCK)
        k_blk = k_ref[pl.ds(start, KEY_BLOCK), :]
        v_blk = v_ref[pl.ds(start, KEY_BLOCK), :]
        out = []
        for j in range(2):
            s = _nt(q_heads[j], k_blk) * scale
            pos = start + lax.broadcasted_iota(jnp.int32, s.shape, 1)
            s = jnp.where(pos < length, s, masked_value)
            p = jnp.exp(s - lses[j])
            dp = _nt(do_heads[j], v_blk)
            p_buf[j, :, pl.ds(start, KEY_BLOCK)] = p
            dp_buf[j, :, pl.ds(start, KEY_BLOCK)] = dp
            out.append(centres[j] + jnp.sum(p * dp, axis=1, keepdims=True))
        return tuple(out)

    zeros1 = jnp.zeros((rows, 1), jnp.float32)
    centres = lax.fori_loop(0, n_blocks, pass_one, (zeros1, zeros1))

    def pass_two(b, dq):
        start = pl.multiple_of(b * KEY_BLOCK, KEY_BLOCK)
        k_blk = k_ref[pl.ds(start, KEY_BLOCK), :]
        kz = jnp.zeros_like(k_blk)
        in_a_k, in_b_k = _lane_masks(k_blk.shape)
        k_heads = (jnp.where(in_a_k, k_blk, kz), jnp.where(in_b_k, k_blk, kz))
        dk = jnp.zeros(k_blk.shape, jnp.float32)
        dv = jnp.zeros(k_blk.shape, jnp.float32)
        for j in range(2):
            p = p_buf[j, :, pl.ds(start, KEY_BLOCK)]
            dp = dp_buf[j, :, pl.ds(start, KEY_BLOCK)]
            pos = start + lax.broadcasted_iota(jnp.int32, p.shape, 1)
            ds = jnp.where(pos < length, p * (dp - centres[j]), 0.0).astype(jnp.bfloat16)
            dk = dk + _tn(ds, q_heads[j])
            dv = dv + _tn(p.astype(jnp.bfloat16), do_heads[j])
            dq = dq + jnp.dot(ds, k_heads[j], preferred_element_type=jnp.float32)
        dk_ref[pl.ds(start, KEY_BLOCK), :] = (dk * scale).astype(dk_ref.dtype)
        dv_ref[pl.ds(start, KEY_BLOCK), :] = dv.astype(dv_ref.dtype)
        return dq

    dq = lax.fori_loop(0, n_blocks, pass_two, jnp.zeros(q.shape, jnp.float32))
    dq_ref[...] = (dq * scale).astype(dq_ref.dtype)

    def pass_zero(b, carry):
        start = pl.multiple_of(b * KEY_BLOCK, KEY_BLOCK)
        dk_ref[pl.ds(start, KEY_BLOCK), :] = jnp.zeros((KEY_BLOCK, q.shape[1]), dk_ref.dtype)
        dv_ref[pl.ds(start, KEY_BLOCK), :] = jnp.zeros((KEY_BLOCK, q.shape[1]), dv_ref.dtype)
        return carry

    lax.fori_loop(n_blocks, total_blocks, pass_zero, 0)


def attention_bwd(length, q, k, v, do, lse, scale):
    rows, width = q.shape
    seq_len = k.shape[0]
    pairs = width // (2 * HD)
    kernel = functools.partial(_attn_bwd_kernel, scale=scale)
    return pl.pallas_call(
        kernel,
        out_shape=(
            jax.ShapeDtypeStruct((rows, width), jnp.bfloat16),
            jax.ShapeDtypeStruct((seq_len, width), jnp.bfloat16),
            jax.ShapeDtypeStruct((seq_len, width), jnp.bfloat16),
        ),
        grid_spec=pltpu.PrefetchScalarGridSpec(
            num_scalar_prefetch=1,
            grid=(pairs,),
            in_specs=[
                pl.BlockSpec((rows, 2 * HD), lambda h, n: (0, h)),
                pl.BlockSpec((seq_len, 2 * HD), lambda h, n: (0, h)),
                pl.BlockSpec((seq_len, 2 * HD), lambda h, n: (0, h)),
                pl.BlockSpec((rows, 2 * HD), lambda h, n: (0, h)),
                pl.BlockSpec((1, 2, rows, 1), lambda h, n: (h, 0, 0, 0)),
            ],
            out_specs=[
                pl.BlockSpec((rows, 2 * HD), lambda h, n: (0, h)),
                pl.BlockSpec((seq_len, 2 * HD), lambda h, n: (0, h)),
                pl.BlockSpec((seq_len, 2 * HD), lambda h, n: (0, h)),
            ],
            scratch_shapes=[pltpu.VMEM((2, rows, seq_len), jnp.float32), pltpu.VMEM((2, rows, seq_len), jnp.float32)],
        ),
        cost_estimate=pl.CostEstimate(
            flops=20 * pairs * rows * seq_len * 2 * HD,
            transcendentals=2 * pairs * rows * seq_len,
            bytes_accessed=2 * (3 * q.size + 4 * k.size),
        ),
    )(length.reshape(1), q, k, v, do, lse)


def ctx_swap(x):
    return lax.ppermute(x, "ctx", [(0, 1), (1, 0)])


def pad_cols(x, multiple):
    cols = x.shape[1]
    padded = -(-cols // multiple) * multiple
    return jnp.pad(x, ((0, 0), (0, padded - cols)))


def gather_rows(pieces, replicated, nt):
    local = jnp.concatenate(pieces + [replicated], axis=1)
    width = local.shape[1]
    staged = lax.all_gather(local, "tensor", axis=1, tiled=True).reshape(local.shape[0], nt, width)
    parts, at = [], 0
    for p in pieces:
        parts.append(staged[:, :, at : at + p.shape[1]].reshape(local.shape[0], nt * p.shape[1]))
        at += p.shape[1]
    parts.append(staged[:, 0, at:])
    joined = jnp.concatenate(parts, axis=1)
    full = lax.all_gather(joined, ("dp", "ctx"), axis=0, tiled=True)
    out, at = [], 0
    for p in pieces:
        out.append(full[:, at : at + nt * p.shape[1]])
        at += nt * p.shape[1]
    out.append(full[:, at:])
    return out


def reduce_rows(pieces, replicated, nt, gate=None):
    if gate is not None:
        replicated = replicated + gate[0, 0] * 0
    local = jnp.concatenate(pieces + [replicated], axis=1).astype(jnp.bfloat16)
    width = local.shape[1]
    local = pad_cols(local, 128)
    staged = lax.psum_scatter(local, ("dp", "ctx"), scatter_dimension=0, tiled=True)
    rb = staged.shape[0]
    parts, at = [], 0
    for p in pieces:
        c = p.shape[1] // nt
        parts.append(staged[:, at : at + p.shape[1]].reshape(rb, nt, c))
        at += p.shape[1]
    rep = staged[:, at:width]
    parts.append(jnp.broadcast_to(rep[:, None, :], (rb, nt, rep.shape[1])))
    slots = jnp.concatenate(parts, axis=2)
    slot_width = slots.shape[2]
    padded = -(-slot_width // 128) * 128
    slots = jnp.pad(slots, ((0, 0), (0, 0), (0, padded - slot_width))).transpose(1, 0, 2)
    own = lax.psum_scatter(slots, "tensor", scatter_dimension=0, tiled=True)[0].astype(jnp.float32)
    out, at = [], 0
    for p in pieces:
        c = p.shape[1] // nt
        out.append(own[:, at : at + c])
        at += c
    out.append(own[:, at : at + rep.shape[1]])
    return out


def body(
    tokens,
    cotangent,
    lengths,
    w_query,
    w_key,
    w_value,
    w_output,
    w_in,
    w_out,
    bias_query,
    bias_value,
    bias_output,
    gain_first,
    shift_first,
    gain_second,
    shift_second,
    bias_out,
    bias_in,
):
    seqs, local_rows, width = tokens.shape
    ctx_rank = lax.axis_index("ctx")
    tensor_rank = lax.axis_index("tensor")
    nt = lax.axis_size("tensor")
    chunk = ctx_rank * nt + tensor_rank
    seq_len = local_rows * lax.axis_size("ctx") * nt
    scale = HD ** (-0.5)
    rb = w_query.shape[0]
    hidden = w_in.shape[1] * nt

    attn_vec = jnp.stack([bias_query, bias_value, bias_output, gain_first, shift_first], axis=1)
    wq, wk, wv, wo_t, attn_vec = gather_rows([w_query, w_key, w_value, w_output.T], attn_vec, nt)
    ffn_vec = jnp.concatenate(
        [jnp.stack([gain_second, shift_second, bias_out], axis=1), bias_in.reshape(rb, -1)], axis=1
    )
    w_in_f, w_out_t, ffn_vec = gather_rows([w_in, w_out.T], ffn_vec, nt)
    attn_vec = attn_vec.astype(jnp.float32)
    ffn_vec = ffn_vec.astype(jnp.float32)
    b_q, b_v, b_o, g1, s1 = [attn_vec[:, i] for i in range(5)]
    g2, s2, b_out = [ffn_vec[:, i] for i in range(3)]
    b_in = ffn_vec[:, 3:].reshape(hidden)

    row_positions = chunk * local_rows + jnp.arange(local_rows, dtype=jnp.int32)

    fwd = []
    gathered = [lax.all_gather(tokens[0], SEQ_AXES, axis=0, tiled=True)]
    if seqs > 1:
        rest = lax.all_gather(tokens[1:], SEQ_AXES, axis=1, tiled=True)
        gathered += [rest[i] for i in range(seqs - 1)]
    for s in range(seqs):
        x_own = tokens[s]
        length = lengths[s]
        x_all = gathered[s]
        q = (mm(x_own, wq) + b_q).astype(jnp.bfloat16)
        k = mm(x_all, wk).astype(jnp.bfloat16)
        v = (mm(x_all, wv) + b_v).astype(jnp.bfloat16)
        attended, lse = attention_fwd(length, q, k, v, scale)
        first_in = x_own.astype(jnp.float32) + (mm_nt(attended, wo_t) + b_o)
        first, normed1, inv1 = ln_forward(first_in, g1, s1)
        fwd.append(dict(x_all=x_all, q=q, k=k, v=v, lse=lse, attended=attended, first=first,
                        normed1=normed1, inv1=inv1, length=length))

    outputs = []
    for s in range(seqs):
        f = fwd[s]
        first_low = f["first"].astype(jnp.bfloat16)
        hidden_pre = mm(first_low, w_in_f) + b_in
        activated = exact_gelu(hidden_pre).astype(jnp.bfloat16)
        second_in = f["first"] + mm_nt(activated, w_out_t) + b_out
        result, normed2, inv2 = ln_forward(second_in, g2, s2)
        outputs.append(result.astype(jnp.bfloat16))
        f.update(first_low=first_low, hidden_pre=hidden_pre, activated=activated, normed2=normed2, inv2=inv2)

    g_w_in = jnp.zeros((width, hidden), jnp.float32)
    g_w_out_t = jnp.zeros((width, hidden), jnp.float32)
    g_b_in = jnp.zeros((hidden,), jnp.float32)
    g_vec = [jnp.zeros((width,), jnp.float32) for _ in range(8)]
    g_wq = jnp.zeros((width, width), jnp.float32)
    g_wk = jnp.zeros((width, width), jnp.float32)
    g_wv = jnp.zeros((width, width), jnp.float32)
    g_wo_t = jnp.zeros((width, width), jnp.float32)
    grad_tokens = []
    dx_gate = []
    firsts = {}

    def ffn_backward(s):
        nonlocal g_w_in, g_w_out_t, g_b_in
        f = fwd[s]
        row_valid = (row_positions < f["length"]).astype(jnp.float32)
        upstream = cotangent[s].astype(jnp.float32) * row_valid[:, None]
        if dx_gate:
            upstream = upstream + (prev_half[0, 0] * 0).astype(upstream.dtype)
        d_second, d_g2, d_s2 = ln_backward(upstream, f["normed2"], f["inv2"], g2)
        d_ffn = d_second.astype(jnp.bfloat16)
        g_w_out_t = g_w_out_t + mm_tn(d_ffn, f["activated"])
        d_act = mm(d_ffn, w_out_t)
        _, gelu_pull = jax.vjp(exact_gelu, f["hidden_pre"])
        d_hidden = gelu_pull(d_act)[0].astype(jnp.bfloat16)
        g_w_in = g_w_in + mm_tn(f["first_low"], d_hidden)
        g_b_in = g_b_in + jnp.sum(d_hidden.astype(jnp.float32), axis=0)
        d_first = d_second + mm_nt(d_hidden, w_in_f)
        d_first_in, d_g1, d_s1 = ln_backward(d_first, f["normed1"], f["inv1"], g1)
        g_vec[5] = g_vec[5] + d_g2
        g_vec[6] = g_vec[6] + d_s2
        g_vec[7] = g_vec[7] + jnp.sum(d_second, axis=0)
        g_vec[3] = g_vec[3] + d_g1
        g_vec[4] = g_vec[4] + d_s1
        g_vec[2] = g_vec[2] + jnp.sum(d_first_in, axis=0)
        firsts[s] = d_first_in

    def attention_backward(s):
        nonlocal g_wo_t, g_wq, g_wk, g_wv, prev_half
        f = fwd[s]
        d_first_in = firsts[s]
        d_branch = d_first_in.astype(jnp.bfloat16)
        if dx_gate:
            d_branch = d_branch + (prev_half[0, 0] * 0).astype(d_branch.dtype)
        g_wo_t = g_wo_t + mm_tn(d_branch, f["attended"])
        d_att = mm(d_branch, wo_t).astype(jnp.bfloat16)
        dq, dk, dv = attention_bwd(f["length"], f["q"], f["k"], f["v"], d_att, f["lse"], scale)
        g_wq = g_wq + mm_tn(tokens[s], dq)
        g_wk = g_wk + mm_tn(f["x_all"], dk)
        g_wv = g_wv + mm_tn(f["x_all"], dv)
        g_vec[0] = g_vec[0] + jnp.sum(dq.astype(jnp.float32), axis=0)
        g_vec[1] = g_vec[1] + jnp.sum(dv.astype(jnp.float32), axis=0)
        dx_kv = (mm_nt(dk, wk) + mm_nt(dv, wv)).reshape(2, seq_len // 2, width)
        dx_mine = lax.dynamic_index_in_dim(dx_kv, ctx_rank, axis=0, keepdims=False)
        dx_theirs = lax.dynamic_index_in_dim(dx_kv, 1 - ctx_rank, axis=0, keepdims=False).astype(jnp.bfloat16)
        dx_half = (dx_mine + ctx_swap(dx_theirs).astype(jnp.float32)).astype(jnp.bfloat16)
        dx_kv_own = lax.psum_scatter(dx_half, "tensor", scatter_dimension=0, tiled=True).astype(jnp.float32)
        dx_gate.append(dx_kv_own[0:1, 0:1])
        prev_half = dx_half
        d_tok = d_first_in + mm_nt(dq, wq) + dx_kv_own
        grad_tokens.append(d_tok.astype(jnp.bfloat16))


    prev_half = None
    for s in [0]:
        ffn_backward(s)
        attention_backward(s)
    for s in range(1, seqs):
        ffn_backward(s)
    for s in range(1, seqs):
        attention_backward(s)

    ffn_rep = jnp.concatenate([jnp.stack([g_vec[5], g_vec[6], g_vec[7]], axis=1), g_b_in.reshape(width, -1)], axis=1)
    attn_rep = jnp.stack(g_vec[0:5], axis=1)
    grad_w_in, grad_w_out_t, grad_wq, grad_wk, grad_wv, grad_wo_t, rep_out = reduce_rows(
        [g_w_in, g_w_out_t, g_wq, g_wk, g_wv, g_wo_t],
        jnp.concatenate([ffn_rep, attn_rep], axis=1),
        nt,
        gate=sum(dx_gate),
    )
    ffn_rep_out = rep_out[:, : ffn_rep.shape[1]]
    attn_rep_out = rep_out[:, ffn_rep.shape[1] :]

    return (
        jnp.stack(outputs),
        jnp.stack(grad_tokens),
        grad_wq,
        grad_wk,
        grad_wv,
        grad_wo_t.T,
        grad_w_in,
        grad_w_out_t.T,
        attn_rep_out[:, 0],
        attn_rep_out[:, 1],
        attn_rep_out[:, 2],
        attn_rep_out[:, 3],
        attn_rep_out[:, 4],
        ffn_rep_out[:, 0],
        ffn_rep_out[:, 1],
        ffn_rep_out[:, 2],
        ffn_rep_out[:, 3:].reshape(-1),
    )


def solution(mesh):
    row_spec = P("dp", ("ctx", "tensor"), None)
    w_rc = P(("dp", "ctx"), "tensor")
    w_cr = P("tensor", ("dp", "ctx"))
    vec = P(("dp", "ctx"))
    return jax.shard_map(
        body,
        mesh=mesh,
        in_specs=(row_spec, row_spec, P("dp"), w_rc, w_rc, w_rc, w_cr, w_rc, w_cr) + (vec,) * 9,
        out_specs=(row_spec, row_spec, w_rc, w_rc, w_rc, w_cr, w_rc, w_cr) + (vec,) * 9,
        check_vma=False,
    )
```

```python
import functools

import jax
import jax.numpy as jnp
from jax import lax
from jax.experimental import pallas as pl
from jax.experimental.pallas import tpu as pltpu
from jax.sharding import PartitionSpec as P

HD = 64
epsilon = 1e-05
masked_value = -1e30
ALL = ("dp", "ctx", "tensor")
SEQ_AXES = ("ctx", "tensor")


def exact_gelu(value):
    return jax.nn.gelu(value, approximate=False)


def mm(left, right):
    return jnp.dot(left, right, preferred_element_type=jnp.float32)


def mm_tn(left, right):
    return lax.dot_general(left, right, (((0,), (0,)), ((), ())), preferred_element_type=jnp.float32)


def mm_nt(left, right):
    return lax.dot_general(left, right, (((1,), (1,)), ((), ())), preferred_element_type=jnp.float32)


def ln_forward(hidden, gain, shift):
    mean = jnp.mean(hidden, axis=-1, keepdims=True)
    centre = hidden - mean
    var = jnp.mean(centre * centre, axis=-1, keepdims=True)
    inv = lax.rsqrt(var + epsilon)
    normed = centre * inv
    return normed * gain + shift, normed, inv


def ln_backward(grad_out, normed, inv, gain):
    d_normed = grad_out * gain
    width = normed.shape[-1]
    mean_d = jnp.sum(d_normed, axis=-1, keepdims=True) / width
    mean_dn = jnp.sum(d_normed * normed, axis=-1, keepdims=True) / width
    d_in = inv * (d_normed - mean_d - normed * mean_dn)
    d_gain = jnp.sum(grad_out * normed, axis=0)
    d_shift = jnp.sum(grad_out, axis=0)
    return d_in, d_gain, d_shift


KEY_BLOCK = 512


def _lane_masks(shape):
    lane = lax.broadcasted_iota(jnp.int32, shape, 1)
    return lane < HD, lane >= HD


def _nt(a, b):
    return lax.dot_general(a, b, (((1,), (1,)), ((), ())), preferred_element_type=jnp.float32)


def _tn(a, b):
    return lax.dot_general(a, b, (((0,), (0,)), ((), ())), preferred_element_type=jnp.float32)


def _attn_fwd_kernel(len_ref, q_ref, k_ref, v_ref, o_ref, lse_ref, s_buf, *, scale):
    length = len_ref[0]
    n_blocks = (length + KEY_BLOCK - 1) // KEY_BLOCK
    q = q_ref[...]
    rows = q.shape[0]
    in_a, in_b = _lane_masks(q.shape)
    zero = jnp.zeros_like(q)
    q_heads = (jnp.where(in_a, q, zero), jnp.where(in_b, q, zero))

    def pass_max(b, ms):
        start = pl.multiple_of(b * KEY_BLOCK, KEY_BLOCK)
        k_blk = k_ref[pl.ds(start, KEY_BLOCK), :]
        out = []
        for j in range(2):
            s = _nt(q_heads[j], k_blk) * scale
            pos = start + lax.broadcasted_iota(jnp.int32, s.shape, 1)
            s = jnp.where(pos < length, s, masked_value)
            s_buf[j, :, pl.ds(start, KEY_BLOCK)] = s
            out.append(jnp.maximum(ms[j], jnp.max(s, axis=1, keepdims=True)))
        return tuple(out)

    init = jnp.full((rows, 1), -jnp.inf, jnp.float32)
    ms = lax.fori_loop(0, n_blocks, pass_max, (init, init))

    def pass_sum(b, ls):
        start = pl.multiple_of(b * KEY_BLOCK, KEY_BLOCK)
        out = []
        for j in range(2):
            e = jnp.exp(s_buf[j, :, pl.ds(start, KEY_BLOCK)] - ms[j])
            s_buf[j, :, pl.ds(start, KEY_BLOCK)] = e
            out.append(ls[j] + jnp.sum(e, axis=1, keepdims=True))
        return tuple(out)

    zeros1 = jnp.zeros((rows, 1), jnp.float32)
    ls = lax.fori_loop(0, n_blocks, pass_sum, (zeros1, zeros1))

    def pass_out(b, acc):
        start = pl.multiple_of(b * KEY_BLOCK, KEY_BLOCK)
        v_blk = v_ref[pl.ds(start, KEY_BLOCK), :]
        vz = jnp.zeros_like(v_blk)
        in_a_v, in_b_v = _lane_masks(v_blk.shape)
        v_heads = (jnp.where(in_a_v, v_blk, vz), jnp.where(in_b_v, v_blk, vz))
        for j in range(2):
            probs = (s_buf[j, :, pl.ds(start, KEY_BLOCK)] / ls[j]).astype(jnp.bfloat16)
            acc = acc + jnp.dot(probs, v_heads[j], preferred_element_type=jnp.float32)
        return acc

    acc = lax.fori_loop(0, n_blocks, pass_out, jnp.zeros(q.shape, jnp.float32))
    o_ref[...] = acc.astype(o_ref.dtype)
    for j in range(2):
        lse_ref[0, j] = ms[j] + jnp.log(ls[j])


def attention_fwd(length, q, k, v, scale):
    rows, width = q.shape
    seq_len = k.shape[0]
    pairs = width // (2 * HD)
    kernel = functools.partial(_attn_fwd_kernel, scale=scale)
    return pl.pallas_call(
        kernel,
        out_shape=(
            jax.ShapeDtypeStruct((rows, width), jnp.bfloat16),
            jax.ShapeDtypeStruct((pairs, 2, rows, 1), jnp.float32),
        ),
        grid_spec=pltpu.PrefetchScalarGridSpec(
            num_scalar_prefetch=1,
            grid=(pairs,),
            in_specs=[
                pl.BlockSpec((rows, 2 * HD), lambda h, n: (0, h)),
                pl.BlockSpec((seq_len, 2 * HD), lambda h, n: (0, h)),
                pl.BlockSpec((seq_len, 2 * HD), lambda h, n: (0, h)),
            ],
            out_specs=[
                pl.BlockSpec((rows, 2 * HD), lambda h, n: (0, h)),
                pl.BlockSpec((1, 2, rows, 1), lambda h, n: (h, 0, 0, 0)),
            ],
            scratch_shapes=[pltpu.VMEM((2, rows, seq_len), jnp.float32)],
        ),
        cost_estimate=pl.CostEstimate(
            flops=8 * pairs * rows * seq_len * 2 * HD,
            transcendentals=2 * pairs * rows * seq_len,
            bytes_accessed=2 * (2 * q.size + k.size + v.size),
        ),
    )(length.reshape(1), q, k, v)


def _attn_bwd_kernel(len_ref, q_ref, k_ref, v_ref, do_ref, lse_ref, dq_ref, dk_ref, dv_ref, p_buf, dp_buf, *, scale):
    length = len_ref[0]
    n_blocks = (length + KEY_BLOCK - 1) // KEY_BLOCK
    total_blocks = k_ref.shape[0] // KEY_BLOCK
    q = q_ref[...]
    do = do_ref[...]
    rows = q.shape[0]
    in_a, in_b = _lane_masks(q.shape)
    zero = jnp.zeros_like(q)
    q_heads = (jnp.where(in_a, q, zero), jnp.where(in_b, q, zero))
    do_heads = (jnp.where(in_a, do, zero), jnp.where(in_b, do, zero))
    lses = (lse_ref[0, 0], lse_ref[0, 1])

    def pass_one(b, centres):
        start = pl.multiple_of(b * KEY_BLOCK, KEY_BLOCK)
        k_blk = k_ref[pl.ds(start, KEY_BLOCK), :]
        v_blk = v_ref[pl.ds(start, KEY_BLOCK), :]
        out = []
        for j in range(2):
            s = _nt(q_heads[j], k_blk) * scale
            pos = start + lax.broadcasted_iota(jnp.int32, s.shape, 1)
            s = jnp.where(pos < length, s, masked_value)
            p = jnp.exp(s - lses[j])
            dp = _nt(do_heads[j], v_blk)
            p_buf[j, :, pl.ds(start, KEY_BLOCK)] = p
            dp_buf[j, :, pl.ds(start, KEY_BLOCK)] = dp
            out.append(centres[j] + jnp.sum(p * dp, axis=1, keepdims=True))
        return tuple(out)

    zeros1 = jnp.zeros((rows, 1), jnp.float32)
    centres = lax.fori_loop(0, n_blocks, pass_one, (zeros1, zeros1))

    def pass_two(b, dq):
        start = pl.multiple_of(b * KEY_BLOCK, KEY_BLOCK)
        k_blk = k_ref[pl.ds(start, KEY_BLOCK), :]
        kz = jnp.zeros_like(k_blk)
        in_a_k, in_b_k = _lane_masks(k_blk.shape)
        k_heads = (jnp.where(in_a_k, k_blk, kz), jnp.where(in_b_k, k_blk, kz))
        dk = jnp.zeros(k_blk.shape, jnp.float32)
        dv = jnp.zeros(k_blk.shape, jnp.float32)
        for j in range(2):
            p = p_buf[j, :, pl.ds(start, KEY_BLOCK)]
            dp = dp_buf[j, :, pl.ds(start, KEY_BLOCK)]
            pos = start + lax.broadcasted_iota(jnp.int32, p.shape, 1)
            ds = jnp.where(pos < length, p * (dp - centres[j]), 0.0).astype(jnp.bfloat16)
            dk = dk + _tn(ds, q_heads[j])
            dv = dv + _tn(p.astype(jnp.bfloat16), do_heads[j])
            dq = dq + jnp.dot(ds, k_heads[j], preferred_element_type=jnp.float32)
        dk_ref[pl.ds(start, KEY_BLOCK), :] = (dk * scale).astype(dk_ref.dtype)
        dv_ref[pl.ds(start, KEY_BLOCK), :] = dv.astype(dv_ref.dtype)
        return dq

    dq = lax.fori_loop(0, n_blocks, pass_two, jnp.zeros(q.shape, jnp.float32))
    dq_ref[...] = (dq * scale).astype(dq_ref.dtype)

    def pass_zero(b, carry):
        start = pl.multiple_of(b * KEY_BLOCK, KEY_BLOCK)
        dk_ref[pl.ds(start, KEY_BLOCK), :] = jnp.zeros((KEY_BLOCK, q.shape[1]), dk_ref.dtype)
        dv_ref[pl.ds(start, KEY_BLOCK), :] = jnp.zeros((KEY_BLOCK, q.shape[1]), dv_ref.dtype)
        return carry

    lax.fori_loop(n_blocks, total_blocks, pass_zero, 0)


def attention_bwd(length, q, k, v, do, lse, scale):
    rows, width = q.shape
    seq_len = k.shape[0]
    pairs = width // (2 * HD)
    kernel = functools.partial(_attn_bwd_kernel, scale=scale)
    return pl.pallas_call(
        kernel,
        out_shape=(
            jax.ShapeDtypeStruct((rows, width), jnp.bfloat16),
            jax.ShapeDtypeStruct((seq_len, width), jnp.bfloat16),
            jax.ShapeDtypeStruct((seq_len, width), jnp.bfloat16),
        ),
        grid_spec=pltpu.PrefetchScalarGridSpec(
            num_scalar_prefetch=1,
            grid=(pairs,),
            in_specs=[
                pl.BlockSpec((rows, 2 * HD), lambda h, n: (0, h)),
                pl.BlockSpec((seq_len, 2 * HD), lambda h, n: (0, h)),
                pl.BlockSpec((seq_len, 2 * HD), lambda h, n: (0, h)),
                pl.BlockSpec((rows, 2 * HD), lambda h, n: (0, h)),
                pl.BlockSpec((1, 2, rows, 1), lambda h, n: (h, 0, 0, 0)),
            ],
            out_specs=[
                pl.BlockSpec((rows, 2 * HD), lambda h, n: (0, h)),
                pl.BlockSpec((seq_len, 2 * HD), lambda h, n: (0, h)),
                pl.BlockSpec((seq_len, 2 * HD), lambda h, n: (0, h)),
            ],
            scratch_shapes=[pltpu.VMEM((2, rows, seq_len), jnp.float32), pltpu.VMEM((2, rows, seq_len), jnp.float32)],
        ),
        cost_estimate=pl.CostEstimate(
            flops=20 * pairs * rows * seq_len * 2 * HD,
            transcendentals=2 * pairs * rows * seq_len,
            bytes_accessed=2 * (3 * q.size + 4 * k.size),
        ),
    )(length.reshape(1), q, k, v, do, lse)


def ctx_swap(x):
    return lax.ppermute(x, "ctx", [(0, 1), (1, 0)])


def pad_cols(x, multiple):
    cols = x.shape[1]
    padded = -(-cols // multiple) * multiple
    return jnp.pad(x, ((0, 0), (0, padded - cols)))


def gather_rows(pieces, replicated, nt):
    local = jnp.concatenate(pieces + [replicated], axis=1)
    width = local.shape[1]
    staged = lax.all_gather(local, "tensor", axis=1, tiled=True).reshape(local.shape[0], nt, width)
    parts, at = [], 0
    for p in pieces:
        parts.append(staged[:, :, at : at + p.shape[1]].reshape(local.shape[0], nt * p.shape[1]))
        at += p.shape[1]
    parts.append(staged[:, 0, at:])
    joined = jnp.concatenate(parts, axis=1)
    full = lax.all_gather(joined, ("dp", "ctx"), axis=0, tiled=True)
    out, at = [], 0
    for p in pieces:
        out.append(full[:, at : at + nt * p.shape[1]])
        at += nt * p.shape[1]
    out.append(full[:, at:])
    return out


def reduce_rows(pieces, replicated, nt, gate=None):
    if gate is not None:
        replicated = replicated + gate[0, 0] * 0
    local = jnp.concatenate(pieces + [replicated], axis=1).astype(jnp.bfloat16)
    width = local.shape[1]
    local = pad_cols(local, 128)
    staged = lax.psum_scatter(local, ("dp", "ctx"), scatter_dimension=0, tiled=True)
    rb = staged.shape[0]
    parts, at = [], 0
    for p in pieces:
        c = p.shape[1] // nt
        parts.append(staged[:, at : at + p.shape[1]].reshape(rb, nt, c))
        at += p.shape[1]
    rep = staged[:, at:width]
    parts.append(jnp.broadcast_to(rep[:, None, :], (rb, nt, rep.shape[1])))
    slots = jnp.concatenate(parts, axis=2)
    slot_width = slots.shape[2]
    padded = -(-slot_width // 128) * 128
    slots = jnp.pad(slots, ((0, 0), (0, 0), (0, padded - slot_width))).transpose(1, 0, 2)
    own = lax.psum_scatter(slots, "tensor", scatter_dimension=0, tiled=True)[0].astype(jnp.float32)
    out, at = [], 0
    for p in pieces:
        c = p.shape[1] // nt
        out.append(own[:, at : at + c])
        at += c
    out.append(own[:, at : at + rep.shape[1]])
    return out


def body(
    tokens,
    cotangent,
    lengths,
    w_query,
    w_key,
    w_value,
    w_output,
    w_in,
    w_out,
    bias_query,
    bias_value,
    bias_output,
    gain_first,
    shift_first,
    gain_second,
    shift_second,
    bias_out,
    bias_in,
):
    seqs, local_rows, width = tokens.shape
    ctx_rank = lax.axis_index("ctx")
    tensor_rank = lax.axis_index("tensor")
    nt = lax.axis_size("tensor")
    chunk = ctx_rank * nt + tensor_rank
    seq_len = local_rows * lax.axis_size("ctx") * nt
    scale = HD ** (-0.5)
    rb = w_query.shape[0]
    hidden = w_in.shape[1] * nt

    attn_vec = jnp.stack([bias_query, bias_value, bias_output, gain_first, shift_first], axis=1)
    wq, wk, wv, wo_t, attn_vec = gather_rows([w_query, w_key, w_value, w_output.T], attn_vec, nt)
    ffn_vec = jnp.concatenate(
        [jnp.stack([gain_second, shift_second, bias_out], axis=1), bias_in.reshape(rb, -1)], axis=1
    )
    w_in_f, w_out_t, ffn_vec = gather_rows([w_in, w_out.T], ffn_vec, nt)
    attn_vec = attn_vec.astype(jnp.float32)
    ffn_vec = ffn_vec.astype(jnp.float32)
    b_q, b_v, b_o, g1, s1 = [attn_vec[:, i] for i in range(5)]
    g2, s2, b_out = [ffn_vec[:, i] for i in range(3)]
    b_in = ffn_vec[:, 3:].reshape(hidden)

    row_positions = chunk * local_rows + jnp.arange(local_rows, dtype=jnp.int32)

    fwd = []
    for s in range(seqs):
        x_own = tokens[s]
        length = lengths[s]
        x_all = lax.all_gather(x_own, SEQ_AXES, axis=0, tiled=True)
        q = (mm(x_own, wq) + b_q).astype(jnp.bfloat16)
        k = mm(x_all, wk).astype(jnp.bfloat16)
        v = (mm(x_all, wv) + b_v).astype(jnp.bfloat16)
        attended, lse = attention_fwd(length, q, k, v, scale)
        first_in = x_own.astype(jnp.float32) + (mm_nt(attended, wo_t) + b_o)
        first, normed1, inv1 = ln_forward(first_in, g1, s1)
        fwd.append(dict(x_all=x_all, q=q, k=k, v=v, lse=lse, attended=attended, first=first,
                        normed1=normed1, inv1=inv1, length=length))

    outputs = [None] * seqs

    def ffn_forward(s, gate=None):
        f = fwd[s]
        first = f["first"]
        if gate is not None:
            first = first + (gate[0, 0] * 0).astype(first.dtype)
        first_low = first.astype(jnp.bfloat16)
        hidden_pre = mm(first_low, w_in_f) + b_in
        activated = exact_gelu(hidden_pre).astype(jnp.bfloat16)
        second_in = first + mm_nt(activated, w_out_t) + b_out
        result, normed2, inv2 = ln_forward(second_in, g2, s2)
        outputs[s] = result.astype(jnp.bfloat16)
        f.update(first_low=first_low, hidden_pre=hidden_pre, activated=activated, normed2=normed2, inv2=inv2)

    g_w_in = jnp.zeros((width, hidden), jnp.float32)
    g_w_out_t = jnp.zeros((width, hidden), jnp.float32)
    g_b_in = jnp.zeros((hidden,), jnp.float32)
    g_vec = [jnp.zeros((width,), jnp.float32) for _ in range(8)]
    g_wq = jnp.zeros((width, width), jnp.float32)
    g_wk = jnp.zeros((width, width), jnp.float32)
    g_wv = jnp.zeros((width, width), jnp.float32)
    g_wo_t = jnp.zeros((width, width), jnp.float32)
    grad_tokens = []
    dx_gate = []
    firsts = {}

    def ffn_backward(s):
        nonlocal g_w_in, g_w_out_t, g_b_in
        f = fwd[s]
        row_valid = (row_positions < f["length"]).astype(jnp.float32)
        upstream = cotangent[s].astype(jnp.float32) * row_valid[:, None]
        if dx_gate:
            upstream = upstream + (prev_half[0, 0] * 0).astype(upstream.dtype)
        d_second, d_g2, d_s2 = ln_backward(upstream, f["normed2"], f["inv2"], g2)
        d_ffn = d_second.astype(jnp.bfloat16)
        g_w_out_t = g_w_out_t + mm_tn(d_ffn, f["activated"])
        d_act = mm(d_ffn, w_out_t)
        _, gelu_pull = jax.vjp(exact_gelu, f["hidden_pre"])
        d_hidden = gelu_pull(d_act)[0].astype(jnp.bfloat16)
        g_w_in = g_w_in + mm_tn(f["first_low"], d_hidden)
        g_b_in = g_b_in + jnp.sum(d_hidden.astype(jnp.float32), axis=0)
        d_first = d_second + mm_nt(d_hidden, w_in_f)
        d_first_in, d_g1, d_s1 = ln_backward(d_first, f["normed1"], f["inv1"], g1)
        g_vec[5] = g_vec[5] + d_g2
        g_vec[6] = g_vec[6] + d_s2
        g_vec[7] = g_vec[7] + jnp.sum(d_second, axis=0)
        g_vec[3] = g_vec[3] + d_g1
        g_vec[4] = g_vec[4] + d_s1
        g_vec[2] = g_vec[2] + jnp.sum(d_first_in, axis=0)
        firsts[s] = d_first_in

    def attention_backward(s):
        nonlocal g_wo_t, g_wq, g_wk, g_wv, prev_half
        f = fwd[s]
        d_first_in = firsts[s]
        d_branch = d_first_in.astype(jnp.bfloat16)
        if dx_gate:
            d_branch = d_branch + (prev_half[0, 0] * 0).astype(d_branch.dtype)
        g_wo_t = g_wo_t + mm_tn(d_branch, f["attended"])
        d_att = mm(d_branch, wo_t).astype(jnp.bfloat16)
        dq, dk, dv = attention_bwd(f["length"], f["q"], f["k"], f["v"], d_att, f["lse"], scale)
        g_wq = g_wq + mm_tn(tokens[s], dq)
        g_wk = g_wk + mm_tn(f["x_all"], dk)
        g_wv = g_wv + mm_tn(f["x_all"], dv)
        g_vec[0] = g_vec[0] + jnp.sum(dq.astype(jnp.float32), axis=0)
        g_vec[1] = g_vec[1] + jnp.sum(dv.astype(jnp.float32), axis=0)
        dx_kv = (mm_nt(dk, wk) + mm_nt(dv, wv)).reshape(2, seq_len // 2, width)
        dx_mine = lax.dynamic_index_in_dim(dx_kv, ctx_rank, axis=0, keepdims=False)
        dx_theirs = lax.dynamic_index_in_dim(dx_kv, 1 - ctx_rank, axis=0, keepdims=False).astype(jnp.bfloat16)
        dx_half = (dx_mine + ctx_swap(dx_theirs).astype(jnp.float32)).astype(jnp.bfloat16)
        dx_kv_own = lax.psum_scatter(dx_half, "tensor", scatter_dimension=0, tiled=True).astype(jnp.float32)
        dx_gate.append(dx_kv_own[0:1, 0:1])
        prev_half = dx_half
        d_tok = d_first_in + mm_nt(dq, wq) + dx_kv_own
        grad_tokens.append(d_tok.astype(jnp.bfloat16))


    prev_half = None
    ffn_forward(0)
    ffn_backward(0)
    attention_backward(0)
    for s in range(1, seqs):
        ffn_forward(s, gate=prev_half)
    for s in range(1, seqs):
        ffn_backward(s)
    for s in range(1, seqs):
        attention_backward(s)

    ffn_rep = jnp.concatenate([jnp.stack([g_vec[5], g_vec[6], g_vec[7]], axis=1), g_b_in.reshape(width, -1)], axis=1)
    attn_rep = jnp.stack(g_vec[0:5], axis=1)
    grad_w_in, grad_w_out_t, grad_wq, grad_wk, grad_wv, grad_wo_t, rep_out = reduce_rows(
        [g_w_in, g_w_out_t, g_wq, g_wk, g_wv, g_wo_t],
        jnp.concatenate([ffn_rep, attn_rep], axis=1),
        nt,
        gate=sum(dx_gate),
    )
    ffn_rep_out = rep_out[:, : ffn_rep.shape[1]]
    attn_rep_out = rep_out[:, ffn_rep.shape[1] :]

    return (
        jnp.stack(outputs),
        jnp.stack(grad_tokens),
        grad_wq,
        grad_wk,
        grad_wv,
        grad_wo_t.T,
        grad_w_in,
        grad_w_out_t.T,
        attn_rep_out[:, 0],
        attn_rep_out[:, 1],
        attn_rep_out[:, 2],
        attn_rep_out[:, 3],
        attn_rep_out[:, 4],
        ffn_rep_out[:, 0],
        ffn_rep_out[:, 1],
        ffn_rep_out[:, 2],
        ffn_rep_out[:, 3:].reshape(-1),
    )


def solution(mesh):
    row_spec = P("dp", ("ctx", "tensor"), None)
    w_rc = P(("dp", "ctx"), "tensor")
    w_cr = P("tensor", ("dp", "ctx"))
    vec = P(("dp", "ctx"))
    return jax.shard_map(
        body,
        mesh=mesh,
        in_specs=(row_spec, row_spec, P("dp"), w_rc, w_rc, w_rc, w_cr, w_rc, w_cr) + (vec,) * 9,
        out_specs=(row_spec, row_spec, w_rc, w_rc, w_rc, w_cr, w_rc, w_cr) + (vec,) * 9,
        check_vma=False,
    )
```
